128 devices in a mesh: dp: 1, row: 16 (over z, y), col: 8 (over x, core).
Axes of the slice: x: 4, y: 4, z: 4, core: 2. Of those that a mesh axis runs over, the one named last changes fastest.
Arguments:
- pair_rep: bfloat16 [768, 768, 64], P(('dp', 'row'), 'col')
- res_mask: int32 [768], P('dp')
- ln_gamma: float32 [64], replicated
- ln_beta: float32 [64], replicated
- w_q: bfloat16 [64, 64], replicated
- w_k: bfloat16 [64, 64], replicated
- w_v: bfloat16 [64, 64], replicated
- w_b: bfloat16 [64, 4], replicated
- w_g: bfloat16 [64, 64], replicated
- w_o: bfloat16 [64, 64], replicated
Outputs:
- output: bfloat16 [768, 768, 64], P(('dp', 'row'), 'col')
All inputs are finite; a program needn't handle non-finite values.
Results may differ from the reference program's by a relative error of at most 0.00749946.
Values are sent between devices in bfloat16 or wider.
A program may use at most 1 GiB of HBM per device.

```python
import jax
import jax.numpy as jnp
from jax import lax

N = 768
C_Z = 64
HEADS = 4
HEAD = 16
LN_EPS = 1e-5


def layer_norm(pair_rep, ln_gamma, ln_beta):
    pair_f32 = pair_rep.astype(jnp.float32)
    mean_c = jnp.mean(pair_f32, axis=-1, keepdims=True)
    centered = pair_f32 - mean_c
    var_c = jnp.mean(jnp.square(centered), axis=-1, keepdims=True)
    return (centered * lax.rsqrt(var_c + LN_EPS) * ln_gamma + ln_beta).astype(jnp.bfloat16)


def setup_inputs(seed: int = 0, part: int = 0) -> dict:
    part_key = jax.random.fold_in(jax.random.key(seed), part)
    pair_key, len_key = jax.random.split(part_key)
    weight_keys = jax.random.split(jax.random.key(seed + 1), 8)
    proj_dim = HEADS * HEAD
    in_scale = C_Z ** -0.5
    pair_rep = jax.random.normal(pair_key, (N, N, C_Z), jnp.float32).astype(jnp.bfloat16)
    seq_len = jax.random.randint(len_key, (), N // 4, N - N // 8 + 1)
    res_mask = (jnp.arange(N) < seq_len).astype(jnp.int32)
    ln_gamma = 1.0 + 0.5 * jax.random.normal(weight_keys[0], (C_Z,), jnp.float32)
    ln_beta = 0.5 * jax.random.normal(weight_keys[1], (C_Z,), jnp.float32)
    w_q = (jax.random.normal(weight_keys[2], (C_Z, proj_dim), jnp.float32) * in_scale).astype(jnp.bfloat16)
    w_k = (jax.random.normal(weight_keys[3], (C_Z, proj_dim), jnp.float32) * in_scale).astype(jnp.bfloat16)
    w_v = (jax.random.normal(weight_keys[4], (C_Z, proj_dim), jnp.float32) * in_scale).astype(jnp.bfloat16)
    w_b = (jax.random.normal(weight_keys[5], (C_Z, HEADS), jnp.float32) * in_scale).astype(jnp.bfloat16)
    w_g = (jax.random.normal(weight_keys[6], (C_Z, proj_dim), jnp.float32) * in_scale).astype(jnp.bfloat16)
    w_o = (jax.random.normal(weight_keys[7], (proj_dim, C_Z), jnp.float32) * (4.0 * proj_dim ** -0.5)).astype(jnp.bfloat16)
    return {'pair_rep': pair_rep, 'res_mask': res_mask, 'ln_gamma': ln_gamma, 'ln_beta': ln_beta, 'w_q': w_q, 'w_k': w_k, 'w_v': w_v, 'w_b': w_b, 'w_g': w_g, 'w_o': w_o}


def reference(pair_rep, res_mask, ln_gamma, ln_beta, w_q, w_k, w_v, w_b, w_g, w_o):
    proj_dim = HEADS * HEAD
    normed = layer_norm(pair_rep, ln_gamma, ln_beta)
    pair_bias = jnp.dot(normed.reshape(N * N, C_Z), w_b, preferred_element_type=jnp.float32).astype(jnp.bfloat16)
    key_bias = jnp.where(res_mask > 0, 0.0, -1e9).astype(jnp.float32)
    full_bias = pair_bias.reshape(N, N, HEADS).astype(jnp.float32) + key_bias[None, :, None]

    def one_row(row_args):
        pair_row, normed_row = row_args
        queries = (jnp.dot(normed_row, w_q, preferred_element_type=jnp.float32) * HEAD ** -0.5).astype(jnp.bfloat16)
        key_row = jnp.dot(normed_row, w_k, preferred_element_type=jnp.float32).astype(jnp.bfloat16)
        val_row = jnp.dot(normed_row, w_v, preferred_element_type=jnp.float32).astype(jnp.bfloat16)
        gate_vals = jax.nn.sigmoid(jnp.dot(normed_row, w_g, preferred_element_type=jnp.float32))
        logits = jnp.einsum('jhd,khd->jkh', queries.reshape(N, HEADS, HEAD).astype(jnp.float32), key_row.reshape(N, HEADS, HEAD).astype(jnp.float32)) + full_bias
        weights = jax.nn.softmax(logits, axis=1)
        attended = jnp.einsum('jkh,khd->jhd', weights, val_row.reshape(N, HEADS, HEAD).astype(jnp.float32))
        gated_out = (gate_vals * attended.reshape(N, proj_dim)).astype(jnp.bfloat16)
        update = jnp.dot(gated_out, w_o, preferred_element_type=jnp.float32)
        return (pair_row.astype(jnp.float32) + update).astype(jnp.bfloat16)

    return lax.map(one_row, (pair_rep, normed))
```

```python
import functools

import jax
import jax.numpy as jnp
from jax import lax
from jax.experimental import pallas as pl
from jax.experimental.pallas import tpu as pltpu
from jax.sharding import PartitionSpec as P

LN_EPS = 1e-5
NEG = -1e9
MESH = pl.DeviceIdType.MESH
F32 = jnp.float32
BF16 = jnp.bfloat16

PAIRS, COLS, CH = 24, 96, 64
HEADS, HEAD = 4, 16
KEYS = 768
BLOCKS = 8


def dot(a, b, ca=1, cb=0):
    return lax.dot_general(a, b, (((ca,), (cb,)), ((), ())), preferred_element_type=F32)


def iota(shape, dim):
    return lax.broadcasted_iota(jnp.int32, shape, dim)


def column(row_ref, n):
    eye = iota((n, n), 0) == iota((n, n), 1)
    return jnp.sum(jnp.where(eye, jnp.broadcast_to(row_ref[...], (n, n)), 0.0), axis=1, keepdims=True)


def block_diag(w):
    zero = jnp.zeros_like(w)
    return jnp.concatenate(
        [jnp.concatenate([w, zero], axis=1), jnp.concatenate([zero, w], axis=1)], axis=0
    )


def norm_kernel(z_ref, gamma_ref, beta_ref, wbt_ref, a_ref, b_ref, bias_acc):
    gamma = column(gamma_ref, CH)
    beta = column(beta_ref, CH)
    pick = (iota((192, HEADS), 0) // 48 == iota((192, HEADS), 1)).astype(F32).astype(BF16)
    per_head = dot(pick, wbt_ref[...]).astype(BF16)
    wide = jnp.concatenate([per_head, per_head], axis=1)
    keep = iota((192, 128), 0) % 2 == iota((192, 128), 1) // CH
    wide = jnp.where(keep, wide.astype(F32), 0.0).astype(BF16)
    lane_pair = (iota((COLS, 192), 1) % 48) // 2

    def body(p, carry):
        halves = []
        for half in range(2):
            x = z_ref[2 * p + half].astype(F32)
            mean = jnp.sum(x, axis=0, keepdims=True) * (1.0 / CH)
            centered = x - mean
            var = jnp.sum(centered * centered, axis=0, keepdims=True) * (1.0 / CH)
            halves.append(centered * lax.rsqrt(var + LN_EPS) * gamma + beta)
        a_t = jnp.concatenate(halves, axis=0)
        a = jnp.transpose(a_t).astype(BF16)
        a_ref[p] = a
        bias = dot(a, wide, 1, 1)
        bias_acc[...] = jnp.where(lane_pair == p, bias, bias_acc[...])
        return carry

    lax.fori_loop(0, PAIRS, body, 0)
    bias = bias_acc[...]
    b_ref[0:96, :] = bias[:, 0:128].astype(BF16)
    tail = jnp.concatenate([bias[0:48, 128:192], bias[48:96, 128:192]], axis=1)
    b_ref[96:144, :] = tail.astype(BF16)


def norm_call(z_t, gamma, beta, wb_t):
    return pl.pallas_call(
        norm_kernel,
        out_shape=(
            jax.ShapeDtypeStruct((PAIRS, COLS, 2 * CH), BF16),
            jax.ShapeDtypeStruct((144, 128), BF16),
        ),
        in_specs=[pl.BlockSpec(memory_space=pltpu.VMEM)] * 4,
        out_specs=(pl.BlockSpec(memory_space=pltpu.VMEM),) * 2,
        scratch_shapes=[pltpu.VMEM((COLS, 192), F32)],
        cost_estimate=pl.CostEstimate(flops=10**8, bytes_accessed=2 * 10**6, transcendentals=4608),
        name="norm",
    )(z_t, gamma, beta, wb_t)


def exchange_kernel(
    a_ref, b_ref, all_a, all_b,
    send_b1, recv_b1, send_b2, recv_b2, send_a, recv_a, send_f, recv_f,
):
    row = lax.axis_index("row")
    col = lax.axis_index("col")
    z, y = row // 4, row % 4
    x, core = col // 2, col % 2
    half = PAIRS // 2

    right = {"row": row, "col": ((x + 1) % 4) * 2 + core}
    left = {"row": row, "col": ((x + 3) % 4) * 2 + core}
    partner = {"row": row, "col": x * 2 + (1 - core)}
    swap_row, swap_col = 4 * x + y, 2 * z + y // 2
    is_relay = core == y // 2
    swap_self = jnp.logical_and(z == x, is_relay)

    barrier = pltpu.get_barrier_semaphore()

    def hello(dev):
        pl.semaphore_signal(barrier, inc=1, device_id=dev, device_id_type=MESH)

    for step in range(1, 16):
        hello({"row": (row + step) % 16, "col": col})
    hello(right)
    hello(left)
    hello(partner)

    @pl.when(jnp.logical_not(swap_self))
    def _():
        hello({"row": swap_row, "col": swap_col})

    for c in range(2):
        @pl.when(jnp.logical_and(is_relay, jnp.logical_not(jnp.logical_and(z == x, core == c))))
        def _():
            hello({"row": 4 * x + y, "col": 2 * z + c})

    from_dest = jnp.where(swap_self, 0, 1)
    from_sources = jnp.where(is_relay, jnp.where(z == x, 1, 2), 0)
    pl.semaphore_wait(barrier, 18 + from_dest + from_sources)

    def bias1(c):
        return pltpu.make_async_remote_copy(
            src_ref=b_ref,
            dst_ref=all_b.at[y % 2, 2 * x + c],
            send_sem=send_b1,
            recv_sem=recv_b1.at[c],
            device_id={"row": swap_row, "col": swap_col},
            device_id_type=MESH,
        )

    for c in range(2):
        @pl.when(jnp.logical_and(core == c, jnp.logical_not(swap_self)))
        def _():
            bias1(c).start()

    @pl.when(swap_self)
    def _():
        all_b[y % 2, col] = b_ref[...]

    def slot(ref, hf, c):
        return ref.at[pl.ds(hf * half, half), pl.ds(pl.multiple_of(c * COLS, COLS), COLS)]

    def a_copy(src, hf, c, sem, dev):
        return pltpu.make_async_remote_copy(
            src_ref=src, dst_ref=slot(all_a, hf, c),
            send_sem=send_a.at[sem], recv_sem=recv_a.at[sem],
            device_id=dev, device_id_type=MESH,
        )

    def own(hf):
        return a_ref.at[pl.ds(hf * half, half)]

    a_copy(own(0), 0, col, 0, right).start()
    a_copy(own(1), 1, col, 3, left).start()
    a_copy(own(1), 1, col, 1, right).start()
    a_copy(own(0), 0, col, 2, left).start()

    def f_copy(src, hf, c, sem):
        return pltpu.make_async_remote_copy(
            src_ref=src, dst_ref=slot(all_a, hf, c),
            send_sem=send_f.at[sem], recv_sem=recv_f.at[sem],
            device_id=partner, device_id_type=MESH,
        )

    for hf in range(2):
        f_copy(own(hf), hf, col, 6 + hf).start()
    all_a[:, pl.ds(pl.multiple_of(col * COLS, COLS), COLS), :] = a_ref[...]

    par = y % 2

    def bias2(step, src_row):
        sz, sy = src_row // 4, src_row % 4
        ref = all_b.at[sy % 2, pl.ds(2 * sz, 2)]
        return pltpu.make_async_remote_copy(
            src_ref=ref, dst_ref=ref,
            send_sem=send_b2.at[step], recv_sem=recv_b2.at[sy % 2, sz],
            device_id={"row": (row + step) % 16, "col": col}, device_id_type=MESH,
        )

    @pl.when(is_relay)
    def _():
        for c in range(2):
            @pl.when(jnp.logical_not(jnp.logical_and(z == x, core == c)))
            def _():
                pltpu.make_async_remote_copy(
                    src_ref=b_ref, dst_ref=all_b.at[par, 2 * z + c],
                    send_sem=send_b1, recv_sem=recv_b1.at[c],
                    device_id={"row": swap_row, "col": swap_col}, device_id_type=MESH,
                ).wait_recv()
        for step in range(1, 16):
            bias2(step, row).start()

    cl, cr, co = ((x + 3) % 4) * 2 + core, ((x + 1) % 4) * 2 + core, ((x + 2) % 4) * 2 + core

    def arrived(hf, c, sem):
        a_copy(slot(all_a, hf, c), hf, c, sem, right).wait_recv()

    arrived(0, cl, 0)
    a_copy(slot(all_a, 0, cl), 0, cl, 4, right).start()
    f_copy(slot(all_a, 0, cl), 0, cl, 0).start()
    arrived(1, cr, 3)
    a_copy(slot(all_a, 1, cr), 1, cr, 5, left).start()
    f_copy(slot(all_a, 1, cr), 1, cr, 3).start()
    arrived(1, cl, 1)
    f_copy(slot(all_a, 1, cl), 1, cl, 1).start()
    arrived(0, cr, 2)
    f_copy(slot(all_a, 0, cr), 0, cr, 2).start()
    arrived(0, co, 4)
    f_copy(slot(all_a, 0, co), 0, co, 4).start()
    arrived(1, co, 5)
    f_copy(slot(all_a, 1, co), 1, co, 5).start()

    for sy in range(2):
        for sz in range(4):
            @pl.when(jnp.logical_not(row == sz * 4 + 2 * core + sy))
            def _():
                ref = all_b.at[sy, pl.ds(2 * sz, 2)]
                pltpu.make_async_remote_copy(
                    src_ref=ref, dst_ref=ref, send_sem=send_b2.at[1], recv_sem=recv_b2.at[sy, sz],
                    device_id=partner, device_id_type=MESH,
                ).wait_recv()

    def from_partner(hf, c, sem):
        f_copy(slot(all_a, hf, c), hf, c, sem).wait_recv()

    other = 1 - core
    pl_, pr_, po_ = ((x + 3) % 4) * 2 + other, ((x + 1) % 4) * 2 + other, ((x + 2) % 4) * 2 + other
    from_partner(0, 2 * x + other, 6)
    from_partner(1, 2 * x + other, 7)
    from_partner(0, pl_, 0)
    from_partner(1, pr_, 3)
    from_partner(1, pl_, 1)
    from_partner(0, pr_, 2)
    from_partner(0, po_, 4)
    from_partner(1, po_, 5)

    for c in range(2):
        @pl.when(jnp.logical_and(core == c, jnp.logical_not(swap_self)))
        def _():
            bias1(c).wait_send()

    @pl.when(is_relay)
    def _():
        for step in range(1, 16):
            bias2(step, row).wait_send()

    for sem in range(6):
        a_copy(own(0), 0, col, sem, right).wait_send()
    for sem in range(8):
        f_copy(own(0), 0, col, sem).wait_send()


def exchange_call(a, b):
    dma = pltpu.SemaphoreType.DMA
    return pl.pallas_call(
        exchange_kernel,
        out_shape=(
            jax.ShapeDtypeStruct((PAIRS, KEYS, 2 * CH), BF16),
            jax.ShapeDtypeStruct((2, 8, 144, 128), BF16),
        ),
        in_specs=[pl.BlockSpec(memory_space=pltpu.VMEM)] * 2,
        out_specs=(pl.BlockSpec(memory_space=pltpu.VMEM),) * 2,
        scratch_shapes=[
            dma(()), dma((2,)), dma((16,)), dma((2, 4)), dma((6,)), dma((6,)), dma((8,)), dma((8,)),
        ],
        compiler_params=pltpu.CompilerParams(collective_id=0, has_side_effects=True),
        cost_estimate=pl.CostEstimate(flops=10**9, bytes_accessed=5 * 10**6, transcendentals=0),
        name="exchange",
    )(a, b)


TILE_ROWS = ((0, 48), (32, 96), (80, 128))


def attention_kernel(
    a_ref, own_ref, z_ref, b_ref, mask_ref, gamma_ref, beta_ref, wb_ref,
    wq_ref, wk_ref, wv_ref, wg_ref, wo_ref, a_hbm,
    out_ref,
    bias_s, w_s, kk_s, vt_s, qm_s, p_s, l_s, bad_s, nk_s, a_s, dma_sem,
):
    pid = pl.program_id(0)

    @pl.when(pid == 0)
    def _():
        length = jnp.sum((mask_ref[...] > 0).astype(F32)).astype(jnp.int32)
        def top(ref):
            return jnp.max(jnp.abs(ref[...].astype(F32)))

        norm_max = 8.1 * top(gamma_ref) + 1.1 * top(beta_ref)
        q_max = CH * norm_max * top(wq_ref)
        k_max = CH * norm_max * top(wk_ref)
        limit = 4.2 * q_max * k_max + 1.1 * CH * norm_max * top(wb_ref)
        nk_s[0] = jnp.where(limit < 2e8, (length + 127) // 128, 6)
        bad_s[...] = jnp.zeros_like(bad_s)
        w_s[0] = block_diag(wk_ref[...])
        w_s[1] = jnp.transpose(block_diag(wv_ref[...]).astype(F32)).astype(BF16)
        w_s[2] = block_diag(wq_ref[...])
        w_s[3] = jnp.transpose(block_diag(wg_ref[...]).astype(F32)).astype(BF16)
        w_s[4] = jnp.transpose(block_diag(wo_ref[...]).astype(F32)).astype(BF16)
        for c in range(8):
            tiles = []
            for par in range(2):
                t = b_ref[par, c].astype(F32)
                tail = t[96:144]
                tiles.append(jnp.concatenate(
                    [t[0:96], jnp.concatenate([tail[:, 0:64], tail[:, 64:128]], axis=0)], axis=1))
            full = jnp.concatenate(
                [tiles[par][:, 48 * h:48 * h + 48] for h in range(HEADS) for par in range(2)], axis=1)
            key = iota((COLS, 384), 0) + c * COLS
            bias_s[c * COLS:(c + 1) * COLS, :] = full + jnp.where(key < length, 0.0, NEG)

    def project(a, a_own):
        kk_s[...] = dot(a, w_s[0]).astype(BF16)
        vt_s[...] = dot(w_s[1], a, 1, 1).astype(BF16)
        q = (dot(a_own, w_s[2]) * HEAD ** -0.5)
        block = iota((COLS, 128), 1) // HEAD
        for b in range(BLOCKS):
            qm_s[b * COLS:(b + 1) * COLS, :] = jnp.where(block == b, q, 0.0).astype(BF16)
        return jax.nn.sigmoid(dot(w_s[3], a_own, 1, 1))

    def bias_of(t, k0, nk):
        lo = (2 * t) % 3
        if lo < 2:
            return bias_s[k0:k0 + nk, lo * 128:lo * 128 + 256]
        return jnp.concatenate([bias_s[k0:k0 + nk, 256:384], bias_s[k0:k0 + nk, 0:128]], axis=1)

    def finish(p, gate, o_tiles):
        parts = []
        for b in range(BLOCKS):
            pieces = []
            for t in range(3):
                lo, hi = max(b * 96, t * 256), min(b * 96 + 96, t * 256 + 256)
                if lo < hi:
                    r = b * HEAD - TILE_ROWS[t][0]
                    pieces.append(o_tiles[t][r:r + HEAD, lo - t * 256:hi - t * 256])
            parts.append(pieces[0] if len(pieces) == 1 else jnp.concatenate(pieces, axis=1))
        o = jnp.concatenate(parts, axis=0)
        gated = (gate * o).astype(BF16)
        update = dot(w_s[4], gated)
        for hf in range(2):
            res = z_ref[2 * p + hf].astype(F32) + update[hf * CH:(hf + 1) * CH]
            out_ref[2 * p + hf] = res.astype(BF16)

    def fast(p, n_chunks):
        nk = n_chunks * 128
        gate = project(a_ref[0], own_ref[p])
        outs = []
        for t in range(3):
            lanes = slice(t * 256, t * 256 + 256)
            qm = qm_s[lanes, :]
            total = jnp.zeros((8, 256), F32)
            for kc in range(n_chunks):
                keys = slice(kc * 128, kc * 128 + 128)
                e = jnp.exp(dot(kk_s[keys, :], qm, 1, 1) + bias_of(t, kc * 128, 128))
                total = total + jnp.sum(e.reshape(16, 8, 256), axis=0)
                p_s[keys, lanes] = e.astype(BF16)
            r0, r1 = TILE_ROWS[t]
            o = dot(vt_s[r0:r1, 0:nk], p_s[0:nk, lanes])
            total = jnp.sum(total, axis=0, keepdims=True)
            o_max = jnp.max(jnp.abs(o), axis=0, keepdims=True)
            good = (total > 1e-12) & (total < 1e25) & (o_max < 1e35)
            bad_s[0:1, lanes] = jnp.maximum(bad_s[0:1, lanes], jnp.where(good, 0.0, 1.0))
            outs.append(o * (1.0 / total))
        finish(p, gate, outs)

    for n_chunks in range(2, 7):
        @pl.when(nk_s[0] == n_chunks)
        def _():
            fast(pid, n_chunks)

    @pl.when(pid == PAIRS - 1)
    def _():
        @pl.when(jnp.max(bad_s[...]) > 0.0)
        def _():
            def body(p, carry):
                cp = pltpu.make_async_copy(a_hbm.at[p], a_s, dma_sem)
                cp.start()
                cp.wait()
                gate = project(a_s[...], own_ref[p])
                outs = []
                for t in range(3):
                    lanes = slice(t * 256, t * 256 + 256)
                    qm = qm_s[lanes, :]
                    top = jnp.full((1, 256), -jnp.inf, F32)
                    for kc in range(6):
                        keys = slice(kc * 128, kc * 128 + 128)
                        s = dot(kk_s[keys, :], qm, 1, 1) + bias_of(t, kc * 128, 128)
                        l_s[keys, :] = s
                        top = jnp.maximum(top, jnp.max(s, axis=0, keepdims=True))
                    total = jnp.zeros((1, 256), F32)
                    for kc in range(6):
                        keys = slice(kc * 128, kc * 128 + 128)
                        e = jnp.exp(l_s[keys, :] - top)
                        total = total + jnp.sum(e, axis=0, keepdims=True)
                        p_s[keys, lanes] = e.astype(BF16)
                    r0, r1 = TILE_ROWS[t]
                    outs.append(dot(vt_s[r0:r1, :], p_s[:, lanes]) * (1.0 / total))
                finish(p, gate, outs)
                return carry

            lax.fori_loop(0, PAIRS, body, 0)


def attention_call(all_a, a, z_t, all_b, mask, gamma, beta, wb_t, wq, wk, wv, wg, wo):
    pairs = all_a.shape[0]

    def whole(arr):
        nd = arr.ndim
        return pl.BlockSpec(arr.shape, lambda i: (0,) * nd)

    small = (a, z_t, all_b, mask, gamma, beta, wb_t, wq, wk, wv, wg, wo)
    return pl.pallas_call(
        attention_kernel,
        grid=(pairs,),
        out_shape=jax.ShapeDtypeStruct(z_t.shape, BF16),
        in_specs=[pl.BlockSpec((1, KEYS, 2 * CH), lambda i: (i, 0, 0))]
        + [whole(s) for s in small]
        + [pl.BlockSpec(memory_space=pl.ANY)],
        out_specs=whole(z_t),
        scratch_shapes=[
            pltpu.VMEM((KEYS, 384), F32),
            pltpu.VMEM((5, 128, 128), BF16),
            pltpu.VMEM((KEYS, 128), BF16),
            pltpu.VMEM((128, KEYS), BF16),
            pltpu.VMEM((KEYS, 128), BF16),
            pltpu.VMEM((KEYS, KEYS), BF16),
            pltpu.VMEM((KEYS, 256), F32),
            pltpu.VMEM((8, KEYS), F32),
            pltpu.SMEM((1,), jnp.int32),
            pltpu.VMEM((KEYS, 128), BF16),
            pltpu.SemaphoreType.DMA(()),
        ],
        compiler_params=pltpu.CompilerParams(dimension_semantics=("arbitrary",)),
        cost_estimate=pl.CostEstimate(flops=10**10, bytes_accessed=8 * 10**6, transcendentals=14 * 10**6),
        name="attention",
    )(all_a, *small, all_a)


def solution(mesh):
    tile_spec = P(("dp", "row"), "col", None)

    def per_device(pair_tile, res_mask, ln_gamma, ln_beta, w_q, w_k, w_v, w_b, w_g, w_o):
        z_t = jnp.transpose(pair_tile, (0, 2, 1))
        gamma = ln_gamma.reshape(1, CH)
        beta = ln_beta.reshape(1, CH)
        wb_t = jnp.transpose(w_b)
        a, b = norm_call(z_t, gamma, beta, wb_t)
        all_a, all_b = exchange_call(a, b)
        out_t = attention_call(
            all_a, a, z_t, all_b, res_mask.reshape(6, 128), gamma, beta, wb_t, w_q, w_k, w_v, w_g, w_o
        )
        return jnp.transpose(out_t, (0, 2, 1))

    return jax.shard_map(
        per_device, mesh=mesh,
        in_specs=(tile_spec, P("dp"), P(), P(), P(), P(), P(), P(), P(), P()),
        out_specs=tile_spec, check_vma=False,
    )
```

```python
import functools

import jax
import jax.numpy as jnp
from jax import lax
from jax.experimental import pallas as pl
from jax.experimental.pallas import tpu as pltpu
from jax.sharding import PartitionSpec as P

LN_EPS = 1e-5
NEG = -1e9
MESH = pl.DeviceIdType.MESH
F32 = jnp.float32
BF16 = jnp.bfloat16

PAIRS, COLS, CH = 24, 96, 64
HEADS, HEAD = 4, 16
KEYS = 768
BLOCKS = 8


def dot(a, b, ca=1, cb=0):
    return lax.dot_general(a, b, (((ca,), (cb,)), ((), ())), preferred_element_type=F32)


def iota(shape, dim):
    return lax.broadcasted_iota(jnp.int32, shape, dim)


def column(row_ref, n):
    eye = iota((n, n), 0) == iota((n, n), 1)
    return jnp.sum(jnp.where(eye, jnp.broadcast_to(row_ref[...], (n, n)), 0.0), axis=1, keepdims=True)


def block_diag(w):
    zero = jnp.zeros_like(w)
    return jnp.concatenate(
        [jnp.concatenate([w, zero], axis=1), jnp.concatenate([zero, w], axis=1)], axis=0
    )


def load(pairs, sems):
    copies = [pltpu.make_async_copy(src, dst, sems.at[i]) for i, (src, dst) in enumerate(pairs)]
    for copy in copies:
        copy.start()
    return copies


def norm_kernel(
    z_hbm, gamma_hbm, beta_hbm, wbt_hbm, a_ref, b_ref, z_ref, gamma_ref, beta_ref, wbt_ref, bias_acc, sems
):
    copies = load(
        [(gamma_hbm, gamma_ref), (beta_hbm, beta_ref), (wbt_hbm, wbt_ref)]
        + [(z_hbm.at[pl.ds(12 * n, 12)], z_ref.at[pl.ds(12 * n, 12)]) for n in range(4)], sems)
    for copy in copies[:3]:
        copy.wait()
    gamma = column(gamma_ref, CH)
    beta = column(beta_ref, CH)
    pick = (iota((192, HEADS), 0) // 48 == iota((192, HEADS), 1)).astype(F32).astype(BF16)
    per_head = dot(pick, wbt_ref[...]).astype(BF16)
    wide = jnp.concatenate([per_head, per_head], axis=1)
    keep = iota((192, 128), 0) % 2 == iota((192, 128), 1) // CH
    wide = jnp.where(keep, wide.astype(F32), 0.0).astype(BF16)
    lane_pair = (iota((COLS, 192), 1) % 48) // 2

    def body(p, carry):
        halves = []
        for half in range(2):
            x = z_ref[2 * p + half].astype(F32)
            mean = jnp.sum(x, axis=0, keepdims=True) * (1.0 / CH)
            centered = x - mean
            var = jnp.sum(centered * centered, axis=0, keepdims=True) * (1.0 / CH)
            halves.append(centered * lax.rsqrt(var + LN_EPS) * gamma + beta)
        a_t = jnp.concatenate(halves, axis=0)
        a = jnp.transpose(a_t).astype(BF16)
        a_ref[p] = a
        bias = dot(a, wide, 1, 1)
        bias_acc[...] = jnp.where(lane_pair == p, bias, bias_acc[...])
        return carry

    for n in range(4):
        copies[3 + n].wait()
        lax.fori_loop(6 * n, 6 * n + 6, body, 0, unroll=6)
    bias = bias_acc[...]
    b_ref[0:96, :] = bias[:, 0:128].astype(BF16)
    tail = jnp.concatenate([bias[0:48, 128:192], bias[48:96, 128:192]], axis=1)
    b_ref[96:144, :] = tail.astype(BF16)


def norm_call(z_t, gamma, beta, wb_t):
    return pl.pallas_call(
        norm_kernel,
        out_shape=(
            jax.ShapeDtypeStruct((PAIRS, COLS, 2 * CH), BF16),
            jax.ShapeDtypeStruct((144, 128), BF16),
        ),
        in_specs=[pl.BlockSpec(memory_space=pltpu.HBM)] * 4,
        out_specs=(pl.BlockSpec(memory_space=pltpu.VMEM),) * 2,
        scratch_shapes=[
            pltpu.VMEM(z_t.shape, BF16), pltpu.VMEM((1, CH), F32), pltpu.VMEM((1, CH), F32),
            pltpu.VMEM((HEADS, CH), BF16), pltpu.VMEM((COLS, 192), F32), pltpu.SemaphoreType.DMA((7,)),
        ],
        compiler_params=pltpu.CompilerParams(vmem_limit_bytes=8 * 2**20),
        cost_estimate=pl.CostEstimate(flops=10**8, bytes_accessed=2 * 10**6, transcendentals=4608),
        name="norm",
    )(z_t, gamma, beta, wb_t)


def exchange_kernel(
    a_ref, b_ref, all_a, all_b,
    send_b1, recv_b1, send_b2, recv_b2, send_a, recv_a, send_f, recv_f,
):
    row = lax.axis_index("row")
    col = lax.axis_index("col")
    z, y = row // 4, row % 4
    x, core = col // 2, col % 2
    half = PAIRS // 2

    right = {"row": row, "col": ((x + 1) % 4) * 2 + core}
    left = {"row": row, "col": ((x + 3) % 4) * 2 + core}
    partner = {"row": row, "col": x * 2 + (1 - core)}
    swap_row, swap_col = 4 * x + y, 2 * z + y // 2
    is_relay = core == y // 2
    swap_self = jnp.logical_and(z == x, is_relay)

    barrier = pltpu.get_barrier_semaphore()

    def hello(dev):
        pl.semaphore_signal(barrier, inc=1, device_id=dev, device_id_type=MESH)

    for step in range(1, 16):
        hello({"row": (row + step) % 16, "col": col})
    hello(right)
    hello(left)
    hello(partner)

    @pl.when(jnp.logical_not(swap_self))
    def _():
        hello({"row": swap_row, "col": swap_col})

    for c in range(2):
        @pl.when(jnp.logical_and(is_relay, jnp.logical_not(jnp.logical_and(z == x, core == c))))
        def _():
            hello({"row": 4 * x + y, "col": 2 * z + c})

    from_dest = jnp.where(swap_self, 0, 1)
    from_sources = jnp.where(is_relay, jnp.where(z == x, 1, 2), 0)
    pl.semaphore_wait(barrier, 18 + from_dest + from_sources)

    def bias1(c):
        return pltpu.make_async_remote_copy(
            src_ref=b_ref,
            dst_ref=all_b.at[y % 2, 2 * x + c],
            send_sem=send_b1,
            recv_sem=recv_b1.at[c],
            device_id={"row": swap_row, "col": swap_col},
            device_id_type=MESH,
        )

    for c in range(2):
        @pl.when(jnp.logical_and(core == c, jnp.logical_not(swap_self)))
        def _():
            bias1(c).start()

    @pl.when(swap_self)
    def _():
        all_b[y % 2, col] = b_ref[...]

    def slot(ref, hf, c):
        return ref.at[pl.ds(hf * half, half), pl.ds(pl.multiple_of(c * COLS, COLS), COLS)]

    def a_copy(src, hf, c, sem, dev):
        return pltpu.make_async_remote_copy(
            src_ref=src, dst_ref=slot(all_a, hf, c),
            send_sem=send_a.at[sem], recv_sem=recv_a.at[sem],
            device_id=dev, device_id_type=MESH,
        )

    def own(hf):
        return a_ref.at[pl.ds(hf * half, half)]

    a_copy(own(0), 0, col, 0, right).start()
    a_copy(own(1), 1, col, 3, left).start()
    a_copy(own(1), 1, col, 1, right).start()
    a_copy(own(0), 0, col, 2, left).start()

    def f_copy(src, hf, c, sem):
        return pltpu.make_async_remote_copy(
            src_ref=src, dst_ref=slot(all_a, hf, c),
            send_sem=send_f.at[sem], recv_sem=recv_f.at[sem],
            device_id=partner, device_id_type=MESH,
        )

    for hf in range(2):
        f_copy(own(hf), hf, col, 6 + hf).start()
    all_a[:, pl.ds(pl.multiple_of(col * COLS, COLS), COLS), :] = a_ref[...]

    par = y % 2

    def bias2(step, src_row):
        sz, sy = src_row // 4, src_row % 4
        ref = all_b.at[sy % 2, pl.ds(2 * sz, 2)]
        return pltpu.make_async_remote_copy(
            src_ref=ref, dst_ref=ref,
            send_sem=send_b2.at[step], recv_sem=recv_b2.at[sy % 2, sz],
            device_id={"row": (row + step) % 16, "col": col}, device_id_type=MESH,
        )

    @pl.when(is_relay)
    def _():
        for c in range(2):
            @pl.when(jnp.logical_not(jnp.logical_and(z == x, core == c)))
            def _():
                pltpu.make_async_remote_copy(
                    src_ref=b_ref, dst_ref=all_b.at[par, 2 * z + c],
                    send_sem=send_b1, recv_sem=recv_b1.at[c],
                    device_id={"row": swap_row, "col": swap_col}, device_id_type=MESH,
                ).wait_recv()
        for step in range(1, 16):
            bias2(step, row).start()

    cl, cr, co = ((x + 3) % 4) * 2 + core, ((x + 1) % 4) * 2 + core, ((x + 2) % 4) * 2 + core

    def arrived(hf, c, sem):
        a_copy(slot(all_a, hf, c), hf, c, sem, right).wait_recv()

    arrived(0, cl, 0)
    a_copy(slot(all_a, 0, cl), 0, cl, 4, right).start()
    f_copy(slot(all_a, 0, cl), 0, cl, 0).start()
    arrived(1, cr, 3)
    a_copy(slot(all_a, 1, cr), 1, cr, 5, left).start()
    f_copy(slot(all_a, 1, cr), 1, cr, 3).start()
    arrived(1, cl, 1)
    f_copy(slot(all_a, 1, cl), 1, cl, 1).start()
    arrived(0, cr, 2)
    f_copy(slot(all_a, 0, cr), 0, cr, 2).start()
    arrived(0, co, 4)
    f_copy(slot(all_a, 0, co), 0, co, 4).start()
    arrived(1, co, 5)
    f_copy(slot(all_a, 1, co), 1, co, 5).start()

    for sy in range(2):
        for sz in range(4):
            @pl.when(jnp.logical_not(row == sz * 4 + 2 * core + sy))
            def _():
                ref = all_b.at[sy, pl.ds(2 * sz, 2)]
                pltpu.make_async_remote_copy(
                    src_ref=ref, dst_ref=ref, send_sem=send_b2.at[1], recv_sem=recv_b2.at[sy, sz],
                    device_id=partner, device_id_type=MESH,
                ).wait_recv()

    def from_partner(hf, c, sem):
        f_copy(slot(all_a, hf, c), hf, c, sem).wait_recv()

    other = 1 - core
    pl_, pr_, po_ = ((x + 3) % 4) * 2 + other, ((x + 1) % 4) * 2 + other, ((x + 2) % 4) * 2 + other
    from_partner(0, 2 * x + other, 6)
    from_partner(1, 2 * x + other, 7)
    from_partner(0, pl_, 0)
    from_partner(1, pr_, 3)
    from_partner(1, pl_, 1)
    from_partner(0, pr_, 2)
    from_partner(0, po_, 4)
    from_partner(1, po_, 5)

    for c in range(2):
        @pl.when(jnp.logical_and(core == c, jnp.logical_not(swap_self)))
        def _():
            bias1(c).wait_send()

    @pl.when(is_relay)
    def _():
        for step in range(1, 16):
            bias2(step, row).wait_send()

    for sem in range(6):
        a_copy(own(0), 0, col, sem, right).wait_send()
    for sem in range(8):
        f_copy(own(0), 0, col, sem).wait_send()


def exchange_call(a, b):
    dma = pltpu.SemaphoreType.DMA
    return pl.pallas_call(
        exchange_kernel,
        out_shape=(
            jax.ShapeDtypeStruct((PAIRS, KEYS, 2 * CH), BF16),
            jax.ShapeDtypeStruct((2, 8, 144, 128), BF16),
        ),
        in_specs=[pl.BlockSpec(memory_space=pltpu.VMEM)] * 2,
        out_specs=(pl.BlockSpec(memory_space=pltpu.VMEM),) * 2,
        scratch_shapes=[
            dma(()), dma((2,)), dma((16,)), dma((2, 4)), dma((6,)), dma((6,)), dma((8,)), dma((8,)),
        ],
        compiler_params=pltpu.CompilerParams(collective_id=0, has_side_effects=True, vmem_limit_bytes=16 * 2**20),
        cost_estimate=pl.CostEstimate(flops=10**11, bytes_accessed=10**9, transcendentals=0),
        name="exchange",
    )(a, b)


TILE_ROWS = ((0, 48), (32, 96), (80, 128))


def attention_kernel(
    a_ref, own_ref, b_ref, z_hbm, mask_hbm, gamma_hbm, beta_hbm, wb_hbm,
    wq_hbm, wk_hbm, wv_hbm, wg_hbm, wo_hbm,
    out_ref,
    z_ref, mask_ref, gamma_ref, beta_ref, wb_ref, wq_ref, wk_ref, wv_ref, wg_ref, wo_ref, sems,
    bias_s, w_s, kk0, kk1, vt0, vt1, qm0, qm1, p0, p1, sum0, sum1, o0, o1, l_s, bad_s,
):
    copies = load([
        (mask_hbm, mask_ref), (gamma_hbm, gamma_ref), (beta_hbm, beta_ref), (wb_hbm, wb_ref), (wq_hbm, wq_ref),
        (wk_hbm, wk_ref), (wv_hbm, wv_ref), (wg_hbm, wg_ref), (wo_hbm, wo_ref), (z_hbm, z_ref)], sems)
    kk_s, vt_s, qm_s, p_s, sum_s, o_s = (kk0, kk1), (vt0, vt1), (qm0, qm1), (p0, p1), (sum0, sum1), (o0, o1)

    for copy in copies:
        copy.wait()
    length = jnp.sum((mask_ref[...] > 0).astype(F32)).astype(jnp.int32)

    def top(ref):
        return jnp.max(jnp.abs(ref[...].astype(F32)))

    norm_max = 8.1 * top(gamma_ref) + 1.1 * top(beta_ref)
    q_max = CH * norm_max * top(wq_ref)
    k_max = CH * norm_max * top(wk_ref)
    limit = 4.2 * q_max * k_max + 1.1 * CH * norm_max * top(wb_ref)
    chunks = jnp.where(limit < 2e8, (length + 127) // 128, 6)
    bad_s[...] = jnp.zeros_like(bad_s)
    w_s[3] = block_diag(wk_ref[...])
    w_s[4] = jnp.transpose(block_diag(wv_ref[...]).astype(F32)).astype(BF16)
    w_s[0] = block_diag(wq_ref[...])
    w_s[1] = jnp.transpose(block_diag(wg_ref[...]).astype(F32)).astype(BF16)
    w_s[2] = jnp.transpose(block_diag(wo_ref[...]).astype(F32)).astype(BF16)
    for c in range(8):
        tiles = []
        for par in range(2):
            t = b_ref[par, c].astype(F32)
            tail = t[96:144]
            tiles.append(jnp.concatenate(
                [t[0:96], jnp.concatenate([tail[:, 0:64], tail[:, 64:128]], axis=0)], axis=1))
        full = jnp.concatenate(
            [tiles[par][:, 48 * h:48 * h + 48] for h in range(HEADS) for par in range(2)], axis=1)
        key = iota((COLS, 384), 0) + c * COLS
        bias_s[c * COLS:(c + 1) * COLS, :] = full + jnp.where(key < length, 0.0, NEG)

    def project(p, s, nk):
        kk_s[s][0:nk, :] = dot(a_ref[p, 0:nk, :], w_s[3]).astype(BF16)
        q = dot(own_ref[p], w_s[0]) * HEAD ** -0.5
        block = iota((COLS, 128), 1) // HEAD
        for b in range(BLOCKS):
            qm_s[s][b * COLS:(b + 1) * COLS, :] = jnp.where(block == b, q, 0.0).astype(BF16)

    def bias_of(t, k0, nk):
        lo = (2 * t) % 3
        if lo < 2:
            return bias_s[k0:k0 + nk, lo * 128:lo * 128 + 256]
        return jnp.concatenate([bias_s[k0:k0 + nk, 256:384], bias_s[k0:k0 + nk, 0:128]], axis=1)

    def logits(p, s, n_chunks):
        nk = n_chunks * 128
        vt_s[s][:, 0:nk] = dot(w_s[4], a_ref[p, 0:nk, :], 1, 1).astype(BF16)
        for t in range(3):
            lanes = slice(t * 256, t * 256 + 256)
            qm = qm_s[s][lanes, :]
            total = jnp.zeros((8, 256), F32)
            for kc in range(n_chunks):
                keys = slice(kc * 128, kc * 128 + 128)
                e = jnp.exp(dot(kk_s[s][keys, :], qm, 1, 1) + bias_of(t, kc * 128, 128))
                total = total + jnp.sum(e.reshape(16, 8, 256), axis=0)
                p_s[s][keys, lanes] = e.astype(BF16)
            sum_s[s][:, lanes] = total

    def assemble(o_tiles):
        parts = []
        for b in range(BLOCKS):
            pieces = []
            for t in range(3):
                lo, hi = max(b * 96, t * 256), min(b * 96 + 96, t * 256 + 256)
                if lo < hi:
                    r = b * HEAD - TILE_ROWS[t][0]
                    pieces.append(o_tiles[t][r:r + HEAD, lo - t * 256:hi - t * 256])
            parts.append(pieces[0] if len(pieces) == 1 else jnp.concatenate(pieces, axis=1))
        return jnp.concatenate(parts, axis=0)

    def combine(s, nk, live):
        outs = []
        for t in range(3):
            lanes = slice(t * 256, t * 256 + 256)
            r0, r1 = TILE_ROWS[t]
            o = dot(vt_s[s][r0:r1, 0:nk], p_s[s][0:nk, lanes])
            total = jnp.sum(sum_s[s][:, lanes], axis=0, keepdims=True)
            o_max = jnp.max(jnp.abs(o), axis=0, keepdims=True)
            good = (total > 1e-12) & (total < 1e25) & (o_max < 1e35)
            bad = jnp.where(good, 0.0, live)
            bad_s[0:1, lanes] = jnp.maximum(bad_s[0:1, lanes], bad)
            outs.append(o * (1.0 / total))
        o_s[s][...] = assemble(outs)

    def finish(p, s):
        gate = jax.nn.sigmoid(dot(w_s[1], own_ref[p], 1, 1))
        gated = (gate * o_s[s][...]).astype(BF16)
        update = dot(w_s[2], gated)
        for hf in range(2):
            res = z_ref[2 * p + hf].astype(F32) + update[hf * CH:(hf + 1) * CH]
            out_ref[2 * p + hf] = res.astype(BF16)

    def fast(n_chunks):
        nk = n_chunks * 128
        project(0, 0, nk)

        def body(m, carry):
            for s in range(2):
                i = 2 * m + s
                live = jnp.where((i >= 1) & (i <= PAIRS), 1.0, 0.0)
                finish(jnp.clip(i - 2, 0, PAIRS - 1), s)
                combine(1 - s, nk, live)
                logits(jnp.minimum(i, PAIRS - 1), s, n_chunks)
                project(jnp.minimum(i + 1, PAIRS - 1), 1 - s, nk)
            return carry

        lax.fori_loop(0, PAIRS // 2 + 1, body, 0)

    for n_chunks in range(2, 7):
        @pl.when(chunks == n_chunks)
        def _():
            fast(n_chunks)

    @pl.when(jnp.max(bad_s[...]) > 0.0)
    def _():
        def body(p, carry):
            project(p, 0, KEYS)
            vt0[...] = dot(w_s[4], a_ref[p], 1, 1).astype(BF16)
            outs = []
            for t in range(3):
                lanes = slice(t * 256, t * 256 + 256)
                qm = qm0[lanes, :]
                peak = jnp.full((1, 256), -jnp.inf, F32)
                for kc in range(6):
                    keys = slice(kc * 128, kc * 128 + 128)
                    s = dot(kk0[keys, :], qm, 1, 1) + bias_of(t, kc * 128, 128)
                    l_s[keys, :] = s
                    peak = jnp.maximum(peak, jnp.max(s, axis=0, keepdims=True))
                total = jnp.zeros((1, 256), F32)
                for kc in range(6):
                    keys = slice(kc * 128, kc * 128 + 128)
                    e = jnp.exp(l_s[keys, :] - peak)
                    total = total + jnp.sum(e, axis=0, keepdims=True)
                    p0[keys, lanes] = e.astype(BF16)
                r0, r1 = TILE_ROWS[t]
                outs.append(dot(vt0[r0:r1, :], p0[:, lanes]) * (1.0 / total))
            o0[...] = assemble(outs)
            finish(p, 0)
            return carry

        lax.fori_loop(0, PAIRS, body, 0)


def attention_call(all_a, a, z_t, all_b, mask, gamma, beta, wb_t, wq, wk, wv, wg, wo):
    hbm = (z_t, mask, gamma, beta, wb_t, wq, wk, wv, wg, wo)
    two = lambda *spec: [pltpu.VMEM(*spec)] * 2
    return pl.pallas_call(
        attention_kernel,
        out_shape=jax.ShapeDtypeStruct(z_t.shape, BF16),
        in_specs=[pl.BlockSpec(memory_space=pltpu.VMEM)] * 3 + [pl.BlockSpec(memory_space=pltpu.HBM)] * len(hbm),
        out_specs=pl.BlockSpec(memory_space=pltpu.VMEM),
        scratch_shapes=[
            *[pltpu.VMEM(s.shape, s.dtype) for s in hbm],
            pltpu.SemaphoreType.DMA((len(hbm),)),
            pltpu.VMEM((KEYS, 384), F32),
            pltpu.VMEM((5, 128, 128), BF16),
            *two((KEYS, 128), BF16),
            *two((128, KEYS), BF16),
            *two((KEYS, 128), BF16),
            *two((KEYS, KEYS), BF16),
            *two((8, KEYS), F32),
            *two((128, COLS), F32),
            pltpu.VMEM((KEYS, 256), F32),
            pltpu.VMEM((8, KEYS), F32),
        ],
        compiler_params=pltpu.CompilerParams(vmem_limit_bytes=24 * 2**20),
        cost_estimate=pl.CostEstimate(flops=10**10, bytes_accessed=8 * 10**6, transcendentals=14 * 10**6),
        name="attention",
    )(all_a, a, all_b, *hbm)


def solution(mesh):
    tile_spec = P(("dp", "row"), "col", None)

    def per_device(pair_tile, res_mask, ln_gamma, ln_beta, w_q, w_k, w_v, w_b, w_g, w_o):
        z_t = jnp.transpose(pair_tile, (0, 2, 1))
        gamma = ln_gamma.reshape(1, CH)
        beta = ln_beta.reshape(1, CH)
        wb_t = jnp.transpose(w_b)
        a, b = norm_call(z_t, gamma, beta, wb_t)
        all_a, all_b = exchange_call(a, b)
        out_t = attention_call(
            all_a, a, z_t, all_b, res_mask.reshape(6, 128), gamma, beta, wb_t, w_q, w_k, w_v, w_g, w_o
        )
        return jnp.transpose(out_t, (0, 2, 1))

    return jax.shard_map(
        per_device, mesh=mesh,
        in_specs=(tile_spec, P("dp"), P(), P(), P(), P(), P(), P(), P(), P()),
        out_specs=tile_spec, check_vma=False,
    )
```

```python
import functools

import jax
import jax.numpy as jnp
from jax import lax
from jax.experimental import pallas as pl
from jax.experimental.pallas import tpu as pltpu
from jax.sharding import PartitionSpec as P

LN_EPS = 1e-5
NEG = -1e9
MESH = pl.DeviceIdType.MESH
F32 = jnp.float32
BF16 = jnp.bfloat16

PAIRS, COLS, CH = 24, 96, 64
HEADS, HEAD = 4, 16
KEYS = 768
BLOCKS = 8
GROUPS, GP = 6, 4
LIVE = 672
CHUNK = 112
TILE_ROWS = ((0, 48), (32, 96), (80, 128))


def dot(a, b, ca=1, cb=0):
    return lax.dot_general(a, b, (((ca,), (cb,)), ((), ())), preferred_element_type=F32)


def iota(shape, dim):
    return lax.broadcasted_iota(jnp.int32, shape, dim)


def column(row_ref, n):
    eye = iota((n, n), 0) == iota((n, n), 1)
    return jnp.sum(jnp.where(eye, jnp.broadcast_to(row_ref[...], (n, n)), 0.0), axis=1, keepdims=True)


def block_diag(w):
    zero = jnp.zeros_like(w)
    return jnp.concatenate(
        [jnp.concatenate([w, zero], axis=1), jnp.concatenate([zero, w], axis=1)], axis=0
    )


def load(pairs, sems):
    copies = [pltpu.make_async_copy(src, dst, sems.at[i]) for i, (src, dst) in enumerate(pairs)]
    for copy in copies:
        copy.start()
    return copies


def fill_weights(w_s, wq_ref, wk_ref, wv_ref, wg_ref, wo_ref):
    w_s[0] = block_diag(wq_ref[...])
    w_s[1] = jnp.transpose(block_diag(wg_ref[...]).astype(F32)).astype(BF16)
    w_s[2] = jnp.transpose(block_diag(wo_ref[...]).astype(F32)).astype(BF16)
    w_s[3] = block_diag(wk_ref[...])
    w_s[4] = jnp.transpose(block_diag(wv_ref[...]).astype(F32)).astype(BF16)


def fill_bias(bias_s, all_b, mask_ref):
    length = jnp.sum((mask_ref[...] > 0).astype(F32), axis=1, keepdims=True)
    length = jnp.sum(length, axis=0, keepdims=True)
    for c in range(8):
        tiles = []
        for par in range(2):
            t = all_b[par, c].astype(F32)
            tail = t[96:144]
            tiles.append(jnp.concatenate(
                [t[0:96], jnp.concatenate([tail[:, 0:64], tail[:, 64:128]], axis=0)], axis=1))
        full = jnp.concatenate(
            [tiles[par][:, 48 * h:48 * h + 48] for h in range(HEADS) for par in range(2)], axis=1)
        key = (iota((COLS, 384), 0) + c * COLS).astype(F32)
        bias_s[c * COLS:(c + 1) * COLS, :] = full + jnp.where(key < length, 0.0, NEG)


def bias_of(bias_s, t, k0, nk):
    lo = (2 * t) % 3
    if lo < 2:
        return bias_s[k0:k0 + nk, lo * 128:lo * 128 + 256]
    return jnp.concatenate([bias_s[k0:k0 + nk, 256:384], bias_s[k0:k0 + nk, 0:128]], axis=1)


def fill_queries(qm, own, wq):
    q = dot(own, wq) * HEAD ** -0.5
    block = iota((COLS, 128), 1) // HEAD
    for b in range(BLOCKS):
        qm[b * COLS:(b + 1) * COLS, :] = jnp.where(block == b, q, 0.0).astype(BF16)


def assemble(o_tiles):
    parts = []
    for b in range(BLOCKS):
        pieces = []
        for t in range(3):
            lo, hi = max(b * 96, t * 256), min(b * 96 + 96, t * 256 + 256)
            if lo < hi:
                r = b * HEAD - TILE_ROWS[t][0]
                pieces.append(o_tiles[t][r:r + HEAD, lo - t * 256:hi - t * 256])
        parts.append(pieces[0] if len(pieces) == 1 else jnp.concatenate(pieces, axis=1))
    return jnp.concatenate(parts, axis=0)


def write_rows(p, own, o, w_s, z_ref, out_ref):
    gate = jax.nn.sigmoid(dot(w_s[1], own, 1, 1))
    update = dot(w_s[2], (gate * o).astype(BF16))
    for hf in range(2):
        res = z_ref[2 * p + hf].astype(F32) + update[hf * CH:(hf + 1) * CH]
        out_ref[2 * p + hf] = res.astype(BF16)


def fused_kernel(
    z_hbm, gamma_hbm, beta_hbm, wb_hbm, mask_hbm, wq_hbm, wk_hbm, wv_hbm, wg_hbm, wo_hbm,
    out_hbm, all_a_hbm, all_b_hbm, bad_hbm,
    z_ref, gamma_ref, beta_ref, wb_ref, mask_ref, wq_ref, wk_ref, wv_ref, wg_ref, wo_ref, in_sems,
    own_a, own_b, all_a, all_b, out_ref, bias_acc, bias_s, w_s,
    kk0, kk1, vt0, vt1, qm0, qm1, p0, p1, sum0, sum1, o0, o1, bad_s,
    send_b1, recv_b1, send_b2, recv_b2, send_d, recv_d, send_r, recv_r, send_f, recv_f, out_sems,
):
    kk_s, vt_s, qm_s, p_s, sum_s, o_s = (kk0, kk1), (vt0, vt1), (qm0, qm1), (p0, p1), (sum0, sum1), (o0, o1)
    row = lax.axis_index("row")
    col = lax.axis_index("col")
    z, y = row // 4, row % 4
    x, core = col // 2, col % 2

    copies = load(
        [(gamma_hbm, gamma_ref), (beta_hbm, beta_ref), (wb_hbm, wb_ref)]
        + [(z_hbm.at[pl.ds(12 * n, 12)], z_ref.at[pl.ds(12 * n, 12)]) for n in range(4)]
        + [(mask_hbm, mask_ref), (wq_hbm, wq_ref), (wk_hbm, wk_ref), (wv_hbm, wv_ref), (wg_hbm, wg_ref),
           (wo_hbm, wo_ref)], in_sems)

    right = {"row": row, "col": ((x + 1) % 4) * 2 + core}
    left = {"row": row, "col": ((x + 3) % 4) * 2 + core}
    partner = {"row": row, "col": x * 2 + (1 - core)}
    swap = {"row": 4 * x + y, "col": 2 * z + y // 2}
    is_relay = core == y // 2
    swap_self = jnp.logical_and(z == x, is_relay)

    barrier = pltpu.get_barrier_semaphore()

    def hello(dev):
        pl.semaphore_signal(barrier, inc=1, device_id=dev, device_id_type=MESH)

    for step in range(1, 16):
        hello({"row": (row + step) % 16, "col": col})
    hello(right)
    hello(left)
    hello(partner)

    @pl.when(jnp.logical_not(swap_self))
    def _():
        hello(swap)

    for c in range(2):
        @pl.when(jnp.logical_and(is_relay, jnp.logical_not(jnp.logical_and(z == x, core == c))))
        def _():
            hello({"row": 4 * x + y, "col": 2 * z + c})

    for copy in copies[:3]:
        copy.wait()
    gamma = column(gamma_ref, CH)
    beta = column(beta_ref, CH)
    pick = (iota((192, HEADS), 0) // 48 == iota((192, HEADS), 1)).astype(F32).astype(BF16)
    per_head = dot(pick, wb_ref[...]).astype(BF16)
    wide = jnp.concatenate([per_head, per_head], axis=1)
    keep = iota((192, 128), 0) % 2 == iota((192, 128), 1) // CH
    wide = jnp.where(keep, wide.astype(F32), 0.0).astype(BF16)
    lane_pair = (iota((COLS, 192), 1) % 48) // 2

    def norm_pair(p, carry):
        halves = []
        for half in range(2):
            v = z_ref[2 * p + half].astype(F32)
            mean = jnp.sum(v, axis=0, keepdims=True) * (1.0 / CH)
            centered = v - mean
            var = jnp.sum(centered * centered, axis=0, keepdims=True) * (1.0 / CH)
            halves.append(centered * lax.rsqrt(var + LN_EPS) * gamma + beta)
        a = jnp.transpose(jnp.concatenate(halves, axis=0)).astype(BF16)
        own_a[p] = a
        bias_acc[...] = jnp.where(lane_pair == p, dot(a, wide, 1, 1), bias_acc[...])
        return carry

    for n in range(4):
        copies[3 + n].wait()
        lax.fori_loop(6 * n, 6 * n + 6, norm_pair, 0, unroll=6)
    bias = bias_acc[...]
    own_b[0:96, :] = bias[:, 0:128].astype(BF16)
    own_b[96:144, :] = jnp.concatenate([bias[0:48, 128:192], bias[48:96, 128:192]], axis=1).astype(BF16)

    from_dest = jnp.where(swap_self, 0, 1)
    from_sources = jnp.where(is_relay, jnp.where(z == x, 1, 2), 0)
    pl.semaphore_wait(barrier, 18 + from_dest + from_sources)

    def bias1(c):
        return pltpu.make_async_remote_copy(
            src_ref=own_b, dst_ref=all_b.at[y % 2, 2 * x + c], send_sem=send_b1, recv_sem=recv_b1.at[c],
            device_id=swap, device_id_type=MESH,
        )

    for c in range(2):
        @pl.when(jnp.logical_and(core == c, jnp.logical_not(swap_self)))
        def _():
            bias1(c).start()

    def slot(g, c):
        return all_a.at[pl.ds(g * GP, GP), pl.ds(pl.multiple_of(c * COLS, COLS), COLS)]

    def own(g):
        return own_a.at[pl.ds(g * GP, GP)]

    def direct(src, g, c, way):
        return pltpu.make_async_remote_copy(
            src_ref=src, dst_ref=slot(g, c), send_sem=send_d.at[way, g], recv_sem=recv_d.at[way, g],
            device_id=left if way else right, device_id_type=MESH,
        )

    def relay(g, c, way):
        return pltpu.make_async_remote_copy(
            src_ref=slot(g, c), dst_ref=slot(g, c), send_sem=send_r.at[g], recv_sem=recv_r.at[g],
            device_id=left if way else right, device_id_type=MESH,
        )

    def forward(src, g, c, kind):
        return pltpu.make_async_remote_copy(
            src_ref=src, dst_ref=slot(g, c), send_sem=send_f.at[kind, g], recv_sem=recv_f.at[kind, g],
            device_id=partner, device_id_type=MESH,
        )

    for g in range(GROUPS):
        direct(own(g), g, col, 0).start()
        direct(own(g), g, col, 1).start()
        forward(own(g), g, col, 0).start()

    @pl.when(swap_self)
    def _():
        all_b[y % 2, col] = own_b[...]

    all_a[:, pl.ds(pl.multiple_of(col * COLS, COLS), COLS), :] = own_a[...]
    for copy in copies[7:]:
        copy.wait()
    fill_weights(w_s, wq_ref, wk_ref, wv_ref, wg_ref, wo_ref)

    def peak(ref):
        return jnp.max(jnp.max(jnp.abs(ref[...].astype(F32)), axis=1, keepdims=True), axis=0, keepdims=True)

    norm_max = 8.1 * peak(gamma_ref) + 1.1 * peak(beta_ref)
    limit = 4.2 * (CH * norm_max * peak(wq_ref)) * (CH * norm_max * peak(wk_ref)) + 1.1 * CH * norm_max * peak(wb_ref)
    bad_s[...] = jnp.broadcast_to(jnp.where(limit < 2e8, 0.0, 1.0), bad_s.shape)

    def bias2(step, src_row):
        sz, sy = src_row // 4, src_row % 4
        ref = all_b.at[sy % 2, pl.ds(2 * sz, 2)]
        return pltpu.make_async_remote_copy(
            src_ref=ref, dst_ref=ref, send_sem=send_b2.at[step], recv_sem=recv_b2.at[sy % 2, sz],
            device_id={"row": (row + step) % 16, "col": col}, device_id_type=MESH,
        )

    @pl.when(is_relay)
    def _():
        for c in range(2):
            @pl.when(jnp.logical_not(jnp.logical_and(z == x, core == c)))
            def _():
                pltpu.make_async_remote_copy(
                    src_ref=own_b, dst_ref=all_b.at[y % 2, 2 * z + c], send_sem=send_b1, recv_sem=recv_b1.at[c],
                    device_id=swap, device_id_type=MESH,
                ).wait_recv()
        for step in range(1, 16):
            bias2(step, row).start()

    cl, cr, co = ((x + 3) % 4) * 2 + core, ((x + 1) % 4) * 2 + core, ((x + 2) % 4) * 2 + core
    for g in range(GROUPS):
        direct(slot(g, cl), g, cl, 0).wait_recv()
        if g % 2 == 0:
            relay(g, cl, 0).start()
        forward(slot(g, cl), g, cl, 1).start()
        direct(slot(g, cr), g, cr, 1).wait_recv()
        if g % 2 == 1:
            relay(g, cr, 1).start()
        forward(slot(g, cr), g, cr, 2).start()

    for sy in range(2):
        for sz in range(4):
            @pl.when(jnp.logical_not(row == sz * 4 + 2 * core + sy))
            def _():
                ref = all_b.at[sy, pl.ds(2 * sz, 2)]
                pltpu.make_async_remote_copy(
                    src_ref=ref, dst_ref=ref, send_sem=send_b2.at[1], recv_sem=recv_b2.at[sy, sz],
                    device_id=partner, device_id_type=MESH,
                ).wait_recv()
    fill_bias(bias_s, all_b, mask_ref)
    b_out = pltpu.make_async_copy(all_b, all_b_hbm, out_sems.at[0])
    b_out.start()

    def relayed(g):
        relay(g, co, 0).wait_recv()
        forward(slot(g, co), g, co, 3).start()

    def complete(g):
        for kind, dc in ((0, 0), (1, 3), (2, 1), (3, 2)):
            c = ((x + dc) % 4) * 2 + 1 - core
            forward(slot(g, c), g, c, kind).wait_recv()

    def project(p, s):
        kk_s[s][...] = dot(all_a[p, 0:LIVE, :], w_s[3]).astype(BF16)
        fill_queries(qm_s[s], own_a[p], w_s[0])

    def logits(p, s):
        vt_s[s][...] = dot(w_s[4], all_a[p, 0:LIVE, :], 1, 1).astype(BF16)
        for t in range(3):
            lanes = slice(t * 256, t * 256 + 256)
            qm = qm_s[s][lanes, :]
            total = jnp.zeros((8, 256), F32)
            for k0 in range(0, LIVE, CHUNK):
                keys = slice(k0, k0 + CHUNK)
                e = jnp.exp(dot(kk_s[s][keys, :], qm, 1, 1) + bias_of(bias_s, t, k0, CHUNK))
                total = total + jnp.sum(e.reshape(CHUNK // 8, 8, 256), axis=0)
                p_s[s][keys, lanes] = e.astype(BF16)
            sum_s[s][:, lanes] = total

    def combine(s, live):
        outs = []
        for t in range(3):
            lanes = slice(t * 256, t * 256 + 256)
            r0, r1 = TILE_ROWS[t]
            o = dot(vt_s[s][r0:r1, :], p_s[s][:, lanes])
            total = jnp.sum(sum_s[s][:, lanes], axis=0, keepdims=True)
            o_max = jnp.max(jnp.abs(o), axis=0, keepdims=True)
            good = (total > 1e-12) & (total < 1e25) & (o_max < 1e35)
            bad_s[0:1, lanes] = jnp.maximum(bad_s[0:1, lanes], jnp.where(good, 0.0, live))
            outs.append(o * (1.0 / total))
        o_s[s][...] = assemble(outs)

    relayed(0)
    relayed(1)
    complete(0)
    project(0, 0)

    def body(m, carry):
        @pl.when(jnp.logical_and(m % 2 == 0, jnp.logical_and(m >= 2, m <= 8)))
        def _():
            relayed(m // 2 + 1)

        @pl.when(jnp.logical_and(m % 2 == 1, m <= 9))
        def _():
            complete((m + 1) // 2)

        for s in range(2):
            i = 2 * m + s
            live = jnp.where((i >= 1) & (i <= PAIRS), 1.0, 0.0)
            done = jnp.clip(i - 2, 0, PAIRS - 1)
            write_rows(done, own_a[done], o_s[s][...], w_s, z_ref, out_ref)
            combine(1 - s, live)
            logits(jnp.minimum(i, PAIRS - 1), s)
            project(jnp.minimum(i + 1, PAIRS - 1), 1 - s)
        return carry

    lax.fori_loop(0, PAIRS // 2 + 1, body, 0)
    outs = [
        pltpu.make_async_copy(out_ref, out_hbm, out_sems.at[1]),
        pltpu.make_async_copy(all_a, all_a_hbm, out_sems.at[2]),
        pltpu.make_async_copy(bad_s, bad_hbm, out_sems.at[3]),
    ]
    for copy in outs:
        copy.start()

    for c in range(2):
        @pl.when(jnp.logical_and(core == c, jnp.logical_not(swap_self)))
        def _():
            bias1(c).wait_send()

    @pl.when(is_relay)
    def _():
        for step in range(1, 16):
            bias2(step, row).wait_send()

    for g in range(GROUPS):
        direct(own(g), g, col, 0).wait_send()
        direct(own(g), g, col, 1).wait_send()
        relay(g, co, 0).wait_send()
        for kind in range(4):
            forward(own(g), g, col, kind).wait_send()
    for copy in outs:
        copy.wait()
    b_out.wait()


def fused_call(z_t, gamma, beta, wb_t, mask, wq, wk, wv, wg, wo):
    dma = pltpu.SemaphoreType.DMA
    args = (z_t, gamma, beta, wb_t, mask, wq, wk, wv, wg, wo)
    two = lambda *spec: [pltpu.VMEM(*spec)] * 2
    return pl.pallas_call(
        fused_kernel,
        out_shape=(
            jax.ShapeDtypeStruct(z_t.shape, BF16),
            jax.ShapeDtypeStruct((PAIRS, KEYS, 128), BF16),
            jax.ShapeDtypeStruct((2, 8, 144, 128), BF16),
            jax.ShapeDtypeStruct((8, KEYS), F32),
        ),
        in_specs=[pl.BlockSpec(memory_space=pl.ANY)] * len(args),
        out_specs=(pl.BlockSpec(memory_space=pl.ANY),) * 4,
        scratch_shapes=[
            *[pltpu.VMEM(s.shape, s.dtype) for s in args],
            dma((13,)),
            pltpu.VMEM((PAIRS, COLS, 128), BF16),
            pltpu.VMEM((144, 128), BF16),
            pltpu.VMEM((PAIRS, KEYS, 128), BF16),
            pltpu.VMEM((2, 8, 144, 128), BF16),
            pltpu.VMEM(z_t.shape, BF16),
            pltpu.VMEM((COLS, 192), F32),
            pltpu.VMEM((KEYS, 384), F32),
            pltpu.VMEM((5, 128, 128), BF16),
            *two((LIVE, 128), BF16),
            *two((128, LIVE), BF16),
            *two((KEYS, 128), BF16),
            *two((LIVE, KEYS), BF16),
            *two((8, KEYS), F32),
            *two((128, COLS), F32),
            pltpu.VMEM((8, KEYS), F32),
            dma(()), dma((2,)), dma((16,)), dma((2, 4)),
            dma((2, GROUPS)), dma((2, GROUPS)), dma((GROUPS,)), dma((GROUPS,)), dma((4, GROUPS)), dma((4, GROUPS)),
            dma((4,)),
        ],
        compiler_params=pltpu.CompilerParams(collective_id=0, has_side_effects=True),
        cost_estimate=pl.CostEstimate(flops=10**11, bytes_accessed=10**9, transcendentals=14 * 10**6),
        name="fused",
    )(*args)


def shifted_kernel(
    bad_ref, y_in, all_a_hbm, all_b_hbm, z_hbm, mask_hbm, wq_hbm, wk_hbm, wv_hbm, wg_hbm, wo_hbm,
    y_out,
    all_a, all_b, z_ref, mask_ref, wq_ref, wk_ref, wv_ref, wg_ref, wo_ref, sems,
    bias_s, w_s, kk, vt, qm, p_s, l_s, out_ref,
):
    @pl.when(jnp.max(bad_ref[...]) > 0.0)
    def _():
        col = lax.axis_index("col")
        for copy in load([
            (all_a_hbm, all_a), (all_b_hbm, all_b), (z_hbm, z_ref), (mask_hbm, mask_ref), (wq_hbm, wq_ref),
            (wk_hbm, wk_ref), (wv_hbm, wv_ref), (wg_hbm, wg_ref), (wo_hbm, wo_ref)], sems):
            copy.wait()
        fill_weights(w_s, wq_ref, wk_ref, wv_ref, wg_ref, wo_ref)
        fill_bias(bias_s, all_b, mask_ref)

        def body(p, carry):
            own = all_a[p, pl.ds(pl.multiple_of(col * COLS, COLS), COLS), :]
            kk[...] = dot(all_a[p], w_s[3]).astype(BF16)
            vt[...] = dot(w_s[4], all_a[p], 1, 1).astype(BF16)
            fill_queries(qm, own, w_s[0])
            outs = []
            for t in range(3):
                lanes = slice(t * 256, t * 256 + 256)
                peak = jnp.full((1, 256), -jnp.inf, F32)
                for k0 in range(0, KEYS, 128):
                    keys = slice(k0, k0 + 128)
                    s = dot(kk[keys, :], qm[lanes, :], 1, 1) + bias_of(bias_s, t, k0, 128)
                    l_s[keys, :] = s
                    peak = jnp.maximum(peak, jnp.max(s, axis=0, keepdims=True))
                total = jnp.zeros((1, 256), F32)
                for k0 in range(0, KEYS, 128):
                    keys = slice(k0, k0 + 128)
                    e = jnp.exp(l_s[keys, :] - peak)
                    total = total + jnp.sum(e, axis=0, keepdims=True)
                    p_s[keys, :] = e.astype(BF16)
                r0, r1 = TILE_ROWS[t]
                outs.append(dot(vt[r0:r1, :], p_s[...]) * (1.0 / total))
            write_rows(p, own, assemble(outs), w_s, z_ref, out_ref)
            return carry

        lax.fori_loop(0, PAIRS, body, 0)
        copy = pltpu.make_async_copy(out_ref, y_out, sems.at[0])
        copy.start()
        copy.wait()


def shifted_call(bad, y, all_a, all_b, z_t, mask, wq, wk, wv, wg, wo):
    args = (all_a, all_b, z_t, mask, wq, wk, wv, wg, wo)
    return pl.pallas_call(
        shifted_kernel,
        out_shape=jax.ShapeDtypeStruct(z_t.shape, BF16),
        in_specs=[pl.BlockSpec(memory_space=pltpu.VMEM)] + [pl.BlockSpec(memory_space=pl.ANY)] * (len(args) + 1),
        out_specs=pl.BlockSpec(memory_space=pl.ANY),
        input_output_aliases={1: 0},
        scratch_shapes=[
            *[pltpu.VMEM(s.shape, s.dtype) for s in args],
            pltpu.SemaphoreType.DMA((len(args),)),
            pltpu.VMEM((KEYS, 384), F32),
            pltpu.VMEM((5, 128, 128), BF16),
            pltpu.VMEM((KEYS, 128), BF16),
            pltpu.VMEM((128, KEYS), BF16),
            pltpu.VMEM((KEYS, 128), BF16),
            pltpu.VMEM((KEYS, 256), BF16),
            pltpu.VMEM((KEYS, 256), F32),
            pltpu.VMEM(z_t.shape, BF16),
        ],
        name="shifted",
    )(bad, y, *args)


def solution(mesh):
    tile_spec = P(("dp", "row"), "col", None)

    def per_device(pair_tile, res_mask, ln_gamma, ln_beta, w_q, w_k, w_v, w_b, w_g, w_o):
        z_t = jnp.transpose(pair_tile, (0, 2, 1))
        mask = res_mask.reshape(6, 128)
        y, all_a, all_b, bad = fused_call(
            z_t, ln_gamma.reshape(1, CH), ln_beta.reshape(1, CH), jnp.transpose(w_b), mask, w_q, w_k, w_v, w_g, w_o
        )
        y = shifted_call(bad, y, all_a, all_b, z_t, mask, w_q, w_k, w_v, w_g, w_o)
        return jnp.transpose(y, (0, 2, 1))

    return jax.shard_map(
        per_device, mesh=mesh,
        in_specs=(tile_spec, P("dp"), P(), P(), P(), P(), P(), P(), P(), P()),
        out_specs=tile_spec, check_vma=False,
    )
```

```python
import functools

import jax
import jax.numpy as jnp
from jax import lax
from jax.experimental import pallas as pl
from jax.experimental.pallas import tpu as pltpu
from jax.sharding import PartitionSpec as P

LN_EPS = 1e-5
NEG = -1e9
MESH = pl.DeviceIdType.MESH
F32 = jnp.float32
BF16 = jnp.bfloat16

PAIRS, COLS, CH = 24, 96, 64
HEADS, HEAD = 4, 16
KEYS = 768
BLOCKS = 8
GROUPS, GP = 12, 2
LEAD = 4
LIVE = 672
CHUNK = 336
TILE_ROWS = ((0, 48), (32, 96), (80, 128))


def dot(a, b, ca=1, cb=0):
    return lax.dot_general(a, b, (((ca,), (cb,)), ((), ())), preferred_element_type=F32)


def iota(shape, dim):
    return lax.broadcasted_iota(jnp.int32, shape, dim)


def column(row_ref, n):
    eye = iota((n, n), 0) == iota((n, n), 1)
    return jnp.sum(jnp.where(eye, jnp.broadcast_to(row_ref[...], (n, n)), 0.0), axis=1, keepdims=True)


def block_diag(w):
    zero = jnp.zeros_like(w)
    return jnp.concatenate(
        [jnp.concatenate([w, zero], axis=1), jnp.concatenate([zero, w], axis=1)], axis=0
    )


def load(pairs, sems):
    copies = [pltpu.make_async_copy(src, dst, sems.at[i]) for i, (src, dst) in enumerate(pairs)]
    for copy in copies:
        copy.start()
    return copies


def fill_weights(w_s, wq_ref, wk_ref, wv_ref, wg_ref, wo_ref):
    w_s[0] = jnp.transpose(block_diag(wq_ref[...]).astype(F32)).astype(BF16)
    w_s[1] = jnp.transpose(block_diag(wg_ref[...]).astype(F32)).astype(BF16)
    w_s[2] = jnp.transpose(block_diag(wo_ref[...]).astype(F32)).astype(BF16)
    w_s[3] = block_diag(wk_ref[...])
    w_s[4] = jnp.transpose(block_diag(wv_ref[...]).astype(F32)).astype(BF16)


def fill_bias(bias_s, all_b, mask_ref, blocks=range(8)):
    length = jnp.sum((mask_ref[...] > 0).astype(F32), axis=1, keepdims=True)
    length = jnp.sum(length, axis=0, keepdims=True)
    for c in blocks:
        tiles = []
        for par in range(2):
            t = all_b[par, c].astype(F32)
            tail = t[96:144]
            tiles.append(jnp.concatenate(
                [t[0:96], jnp.concatenate([tail[:, 0:64], tail[:, 64:128]], axis=0)], axis=1))
        full = jnp.concatenate(
            [tiles[par][:, 48 * h:48 * h + 48] for h in range(HEADS) for par in range(2)], axis=1)
        key = (iota((COLS, 384), 0) + c * COLS).astype(F32)
        bias_s[c * COLS:(c + 1) * COLS, :] = full + jnp.where(key < length, 0.0, NEG)


def bias_of(bias_s, t, k0, nk):
    lo = (2 * t) % 3
    if lo < 2:
        return bias_s[k0:k0 + nk, lo * 128:lo * 128 + 256]
    return jnp.concatenate([bias_s[k0:k0 + nk, 256:384], bias_s[k0:k0 + nk, 0:128]], axis=1)


def fill_queries(qm, own, wq_t):
    q = (dot(wq_t, own, 1, 1) * HEAD ** -0.5).astype(BF16)
    for b in range(BLOCKS):
        qm[b * HEAD:(b + 1) * HEAD, b * COLS:(b + 1) * COLS] = q[b * HEAD:(b + 1) * HEAD, :]


def assemble(o_tiles):
    parts = []
    for b in range(BLOCKS):
        pieces = []
        for t in range(3):
            lo, hi = max(b * 96, t * 256), min(b * 96 + 96, t * 256 + 256)
            if lo < hi:
                r = b * HEAD - TILE_ROWS[t][0]
                pieces.append(o_tiles[t][r:r + HEAD, lo - t * 256:hi - t * 256])
        parts.append(pieces[0] if len(pieces) == 1 else jnp.concatenate(pieces, axis=1))
    return jnp.concatenate(parts, axis=0)


def write_rows(p, own, o, w_s, z_ref, out_ref):
    gate = jax.nn.sigmoid(dot(w_s[1], own, 1, 1))
    update = dot(w_s[2], (gate * o).astype(BF16))
    for hf in range(2):
        res = z_ref[2 * p + hf].astype(F32) + update[hf * CH:(hf + 1) * CH]
        out_ref[2 * p + hf] = res.astype(BF16)


def fused_kernel(
    z_hbm, gamma_hbm, beta_hbm, wb_hbm, mask_hbm, wq_hbm, wk_hbm, wv_hbm, wg_hbm, wo_hbm,
    out_hbm, all_a_hbm, all_b_hbm, bad_hbm,
    z_ref, gamma_ref, beta_ref, wb_ref, mask_ref, wq_ref, wk_ref, wv_ref, wg_ref, wo_ref, in_sems,
    own_a, own_b, all_a, all_b, out_ref, bias_acc, bias_s, w_s,
    kk0, kk1, vt0, vt1, qm0, qm1, p0, p1, sum0, sum1, o0, o1, bad_s,
    send_b1, recv_b1, send_b2, recv_b2, send_d, recv_d, send_r, recv_r, send_f, recv_f, out_sems,
):
    kk_s, vt_s, qm_s, p_s, sum_s, o_s = (kk0, kk1), (vt0, vt1), (qm0, qm1), (p0, p1), (sum0, sum1), (o0, o1)
    row = lax.axis_index("row")
    col = lax.axis_index("col")
    z, y = row // 4, row % 4
    x, core = col // 2, col % 2

    copies = load(
        [(gamma_hbm, gamma_ref), (beta_hbm, beta_ref), (wb_hbm, wb_ref)]
        + [(z_hbm.at[pl.ds(12 * n, 12)], z_ref.at[pl.ds(12 * n, 12)]) for n in range(4)]
        + [(mask_hbm, mask_ref), (wq_hbm, wq_ref), (wk_hbm, wk_ref), (wv_hbm, wv_ref), (wg_hbm, wg_ref),
           (wo_hbm, wo_ref)], in_sems)

    right = {"row": row, "col": ((x + 1) % 4) * 2 + core}
    left = {"row": row, "col": ((x + 3) % 4) * 2 + core}
    partner = {"row": row, "col": x * 2 + (1 - core)}
    swap = {"row": 4 * x + y, "col": 2 * z + y // 2}
    is_relay = core == y // 2
    swap_self = jnp.logical_and(z == x, is_relay)

    barrier = pltpu.get_barrier_semaphore()

    def hello(dev):
        pl.semaphore_signal(barrier, inc=1, device_id=dev, device_id_type=MESH)

    for step in range(1, 16):
        hello({"row": (row + step) % 16, "col": col})
    hello(right)
    hello(left)
    hello(partner)

    @pl.when(jnp.logical_not(swap_self))
    def _():
        hello(swap)

    for c in range(2):
        @pl.when(jnp.logical_and(is_relay, jnp.logical_not(jnp.logical_and(z == x, core == c))))
        def _():
            hello({"row": 4 * x + y, "col": 2 * z + c})

    for copy in copies[:3]:
        copy.wait()
    gamma = column(gamma_ref, CH)
    beta = column(beta_ref, CH)
    pick = (iota((192, HEADS), 0) // 48 == iota((192, HEADS), 1)).astype(F32).astype(BF16)
    per_head = dot(pick, wb_ref[...]).astype(BF16)
    wide = jnp.concatenate([per_head, per_head], axis=1)
    keep = iota((192, 128), 0) % 2 == iota((192, 128), 1) // CH
    wide = jnp.where(keep, wide.astype(F32), 0.0).astype(BF16)
    lane_pair = (iota((COLS, 192), 1) % 48) // 2

    def norm_pair(p, carry):
        halves = []
        for half in range(2):
            v = z_ref[2 * p + half].astype(F32)
            mean = jnp.sum(v, axis=0, keepdims=True) * (1.0 / CH)
            centered = v - mean
            var = jnp.sum(centered * centered, axis=0, keepdims=True) * (1.0 / CH)
            halves.append(centered * lax.rsqrt(var + LN_EPS) * gamma + beta)
        a = jnp.transpose(jnp.concatenate(halves, axis=0)).astype(BF16)
        own_a[p] = a
        bias_acc[...] = jnp.where(lane_pair == p, dot(a, wide, 1, 1), bias_acc[...])
        return carry

    for n in range(4):
        copies[3 + n].wait()
        lax.fori_loop(6 * n, 6 * n + 6, norm_pair, 0, unroll=6)
    bias = bias_acc[...]
    own_b[0:96, :] = bias[:, 0:128].astype(BF16)
    own_b[96:144, :] = jnp.concatenate([bias[0:48, 128:192], bias[48:96, 128:192]], axis=1).astype(BF16)

    from_dest = jnp.where(swap_self, 0, 1)
    from_sources = jnp.where(is_relay, jnp.where(z == x, 1, 2), 0)
    pl.semaphore_wait(barrier, 18 + from_dest + from_sources)

    def bias1(c):
        return pltpu.make_async_remote_copy(
            src_ref=own_b, dst_ref=all_b.at[y % 2, 2 * x + c], send_sem=send_b1, recv_sem=recv_b1.at[c],
            device_id=swap, device_id_type=MESH,
        )

    for c in range(2):
        @pl.when(jnp.logical_and(core == c, jnp.logical_not(swap_self)))
        def _():
            bias1(c).start()

    def slot(g, c):
        return all_a.at[pl.ds(g * GP, GP), pl.ds(pl.multiple_of(c * COLS, COLS), COLS)]

    def own(g):
        return own_a.at[pl.ds(g * GP, GP)]

    def direct(src, g, c, way):
        return pltpu.make_async_remote_copy(
            src_ref=src, dst_ref=slot(g, c), send_sem=send_d.at[way, g], recv_sem=recv_d.at[way, g],
            device_id=left if way else right, device_id_type=MESH,
        )

    def relay(g, c, way):
        return pltpu.make_async_remote_copy(
            src_ref=slot(g, c), dst_ref=slot(g, c), send_sem=send_r.at[g], recv_sem=recv_r.at[g],
            device_id=left if way else right, device_id_type=MESH,
        )

    def forward(src, g, c, kind):
        return pltpu.make_async_remote_copy(
            src_ref=src, dst_ref=slot(g, c), send_sem=send_f.at[kind, g], recv_sem=recv_f.at[kind, g],
            device_id=partner, device_id_type=MESH,
        )

    def send_direct(g):
        direct(own(g), g, col, 0).start()
        direct(own(g), g, col, 1).start()

    for g in range(LEAD):
        send_direct(g)
    for g in range(GROUPS):
        forward(own(g), g, col, 0).start()

    @pl.when(swap_self)
    def _():
        all_b[y % 2, col] = own_b[...]

    all_a[:, pl.ds(pl.multiple_of(col * COLS, COLS), COLS), :] = own_a[...]
    for copy in copies[7:]:
        copy.wait()
    fill_weights(w_s, wq_ref, wk_ref, wv_ref, wg_ref, wo_ref)
    for qm in qm_s:
        qm[...] = jnp.zeros_like(qm)

    def peak(ref):
        return jnp.max(jnp.max(jnp.abs(ref[...].astype(F32)), axis=1, keepdims=True), axis=0, keepdims=True)

    norm_max = 8.1 * peak(gamma_ref) + 1.1 * peak(beta_ref)
    limit = 4.2 * (CH * norm_max * peak(wq_ref)) * (CH * norm_max * peak(wk_ref)) + 1.1 * CH * norm_max * peak(wb_ref)
    bad_s[...] = jnp.broadcast_to(jnp.where(limit < 2e8, 0.0, 1.0), bad_s.shape)

    def bias2(step, src_row):
        sz, sy = src_row // 4, src_row % 4
        ref = all_b.at[sy % 2, pl.ds(2 * sz, 2)]
        return pltpu.make_async_remote_copy(
            src_ref=ref, dst_ref=ref, send_sem=send_b2.at[step], recv_sem=recv_b2.at[sy % 2, sz],
            device_id={"row": (row + step) % 16, "col": col}, device_id_type=MESH,
        )

    def bias_relay():
        @pl.when(is_relay)
        def _():
            for c in range(2):
                @pl.when(jnp.logical_not(jnp.logical_and(z == x, core == c)))
                def _():
                    pltpu.make_async_remote_copy(
                        src_ref=own_b, dst_ref=all_b.at[y % 2, 2 * z + c], send_sem=send_b1,
                        recv_sem=recv_b1.at[c], device_id=swap, device_id_type=MESH,
                    ).wait_recv()
            for step in range(1, 16):
                bias2(step, row).start()

    cl, cr, co = ((x + 3) % 4) * 2 + core, ((x + 1) % 4) * 2 + core, ((x + 2) % 4) * 2 + core

    def event(g):
        direct(slot(g, cl), g, cl, 0).wait_recv()

        @pl.when(g % 2 == 0)
        def _():
            relay(g, cl, 0).start()

        forward(slot(g, cl), g, cl, 1).start()
        direct(slot(g, cr), g, cr, 1).wait_recv()

        @pl.when(g % 2 == 1)
        def _():
            relay(g, cr, 1).start()

        forward(slot(g, cr), g, cr, 2).start()

        @pl.when(g < GROUPS - LEAD)
        def _():
            send_direct(g + LEAD)

    def relayed(g):
        relay(g, co, 0).wait_recv()
        forward(slot(g, co), g, co, 3).start()

    def complete(g):
        for kind, dc in ((0, 0), (1, 3), (2, 1), (3, 2)):
            c = ((x + dc) % 4) * 2 + 1 - core
            forward(slot(g, c), g, c, kind).wait_recv()

    def early(g, carry):
        event(g)

        @pl.when(g == 1)
        def _():
            bias_relay()

        @pl.when(g >= 2)
        def _():
            relayed(g - 2)

        return carry

    lax.fori_loop(0, 8, early, 0)

    def project(p, s):
        kk_s[s][...] = dot(all_a[p, 0:LIVE, :], w_s[3]).astype(BF16)
        fill_queries(qm_s[s], own_a[p], w_s[0])

    complete(0)
    project(0, 0)

    for sz in range(4):
        for sy in range(2):
            @pl.when(jnp.logical_not(row == sz * 4 + 2 * core + sy))
            def _():
                ref = all_b.at[sy, pl.ds(2 * sz, 2)]
                pltpu.make_async_remote_copy(
                    src_ref=ref, dst_ref=ref, send_sem=send_b2.at[1], recv_sem=recv_b2.at[sy, sz],
                    device_id=partner, device_id_type=MESH,
                ).wait_recv()
        fill_bias(bias_s, all_b, mask_ref, (2 * sz, 2 * sz + 1))
    b_out = pltpu.make_async_copy(all_b, all_b_hbm, out_sems.at[0])
    b_out.start()

    def values(p, s):
        vt_s[s][...] = dot(w_s[4], all_a[p, 0:LIVE, :], 1, 1).astype(BF16)

    def logits(s, t):
        lanes = slice(t * 256, t * 256 + 256)
        qm = qm_s[s][:, lanes]
        total = jnp.zeros((8, 256), F32)
        for k0 in range(0, LIVE, CHUNK):
            keys = slice(k0, k0 + CHUNK)
            e = jnp.exp(dot(kk_s[s][keys, :], qm) + bias_of(bias_s, t, k0, CHUNK))
            total = total + jnp.sum(e.reshape(CHUNK // 8, 8, 256), axis=0)
            p_s[s][keys, lanes] = e.astype(BF16)
        sum_s[s][:, lanes] = total

    def combine(s, t, live):
        lanes = slice(t * 256, t * 256 + 256)
        r0, r1 = TILE_ROWS[t]
        o = dot(vt_s[s][r0:r1, :], p_s[s][:, lanes])
        total = jnp.sum(sum_s[s][:, lanes], axis=0, keepdims=True)
        o_max = jnp.max(jnp.abs(o), axis=0, keepdims=True)
        good = (total > 1e-12) & (total < 1e25) & (o_max < 1e35)
        bad_s[0:1, lanes] = jnp.maximum(bad_s[0:1, lanes], jnp.where(good, 0.0, live))
        return o * (1.0 / total)


    a_out = pltpu.make_async_copy(all_a, all_a_hbm, out_sems.at[2])

    def body(m, carry):
        @pl.when(m <= 3)
        def _():
            event(8 + m)

        @pl.when(m <= 5)
        def _():
            relayed(6 + m)

        @pl.when(m <= 10)
        def _():
            complete(m + 1)

        @pl.when(m == 11)
        def _():
            a_out.start()

        for s in range(2):
            i = 2 * m + s
            live = jnp.where(i >= 1, 1.0, 0.0)
            done = jnp.maximum(i - 2, 0)
            logits(s, 0)
            o_0 = combine(1 - s, 0, live)
            values(i, s)
            logits(s, 1)
            o_1 = combine(1 - s, 1, live)
            project(jnp.minimum(i + 1, PAIRS - 1), 1 - s)
            logits(s, 2)
            o_2 = combine(1 - s, 2, live)
            o_s[1 - s][...] = assemble([o_0, o_1, o_2])
            write_rows(done, own_a[done], o_s[s][...], w_s, z_ref, out_ref)
        return carry

    lax.fori_loop(0, PAIRS // 2, body, 0)
    tail = 2 * PAIRS - 4
    head_out = pltpu.make_async_copy(out_ref.at[0:tail], out_hbm.at[0:tail], out_sems.at[4])
    head_out.start()
    write_rows(PAIRS - 2, own_a[PAIRS - 2], o_s[0][...], w_s, z_ref, out_ref)
    o_s[1][...] = assemble([combine(1, t, 1.0) for t in range(3)])
    write_rows(PAIRS - 1, own_a[PAIRS - 1], o_s[1][...], w_s, z_ref, out_ref)
    outs = [
        pltpu.make_async_copy(out_ref.at[tail:2 * PAIRS], out_hbm.at[tail:2 * PAIRS], out_sems.at[1]),
        pltpu.make_async_copy(bad_s, bad_hbm, out_sems.at[3]),
    ]
    for copy in outs:
        copy.start()

    for c in range(2):
        @pl.when(jnp.logical_and(core == c, jnp.logical_not(swap_self)))
        def _():
            bias1(c).wait_send()

    @pl.when(is_relay)
    def _():
        for step in range(1, 16):
            bias2(step, row).wait_send()

    for g in range(GROUPS):
        direct(own(g), g, col, 0).wait_send()
        direct(own(g), g, col, 1).wait_send()
        relay(g, co, 0).wait_send()
        for kind in range(4):
            forward(own(g), g, col, kind).wait_send()
    for copy in outs:
        copy.wait()
    a_out.wait()
    b_out.wait()
    head_out.wait()


def fused_call(z_t, gamma, beta, wb_t, mask, wq, wk, wv, wg, wo):
    dma = pltpu.SemaphoreType.DMA
    args = (z_t, gamma, beta, wb_t, mask, wq, wk, wv, wg, wo)
    two = lambda *spec: [pltpu.VMEM(*spec)] * 2
    return pl.pallas_call(
        fused_kernel,
        out_shape=(
            jax.ShapeDtypeStruct(z_t.shape, BF16),
            jax.ShapeDtypeStruct((PAIRS, KEYS, 128), BF16),
            jax.ShapeDtypeStruct((2, 8, 144, 128), BF16),
            jax.ShapeDtypeStruct((8, KEYS), F32),
        ),
        in_specs=[pl.BlockSpec(memory_space=pl.ANY)] * len(args),
        out_specs=(pl.BlockSpec(memory_space=pl.ANY),) * 4,
        scratch_shapes=[
            *[pltpu.VMEM(s.shape, s.dtype) for s in args],
            dma((13,)),
            pltpu.VMEM((PAIRS, COLS, 128), BF16),
            pltpu.VMEM((144, 128), BF16),
            pltpu.VMEM((PAIRS, KEYS, 128), BF16),
            pltpu.VMEM((2, 8, 144, 128), BF16),
            pltpu.VMEM(z_t.shape, BF16),
            pltpu.VMEM((COLS, 192), F32),
            pltpu.VMEM((KEYS, 384), F32),
            pltpu.VMEM((5, 128, 128), BF16),
            *two((LIVE, 128), BF16),
            *two((128, LIVE), BF16),
            *two((128, KEYS), BF16),
            *two((LIVE, KEYS), BF16),
            *two((8, KEYS), F32),
            *two((128, COLS), F32),
            pltpu.VMEM((8, KEYS), F32),
            dma(()), dma((2,)), dma((16,)), dma((2, 4)),
            dma((2, GROUPS)), dma((2, GROUPS)), dma((GROUPS,)), dma((GROUPS,)), dma((4, GROUPS)), dma((4, GROUPS)),
            dma((5,)),
        ],
        compiler_params=pltpu.CompilerParams(collective_id=0, has_side_effects=True),
        cost_estimate=pl.CostEstimate(flops=10**11, bytes_accessed=10**9, transcendentals=14 * 10**6),
        name="fused",
    )(*args)


def shifted_kernel(
    bad_ref, y_in, all_a_hbm, all_b_hbm, z_hbm, mask_hbm, wq_hbm, wk_hbm, wv_hbm, wg_hbm, wo_hbm,
    y_out,
    all_a, all_b, z_ref, mask_ref, wq_ref, wk_ref, wv_ref, wg_ref, wo_ref, sems,
    bias_s, w_s, kk, vt, qm, p_s, l_s, out_ref,
):
    @pl.when(jnp.max(bad_ref[...]) > 0.0)
    def _():
        col = lax.axis_index("col")
        for copy in load([
            (all_a_hbm, all_a), (all_b_hbm, all_b), (z_hbm, z_ref), (mask_hbm, mask_ref), (wq_hbm, wq_ref),
            (wk_hbm, wk_ref), (wv_hbm, wv_ref), (wg_hbm, wg_ref), (wo_hbm, wo_ref)], sems):
            copy.wait()
        fill_weights(w_s, wq_ref, wk_ref, wv_ref, wg_ref, wo_ref)
        fill_bias(bias_s, all_b, mask_ref)
        qm[...] = jnp.zeros_like(qm)

        def body(p, carry):
            own = all_a[p, pl.ds(pl.multiple_of(col * COLS, COLS), COLS), :]
            kk[...] = dot(all_a[p], w_s[3]).astype(BF16)
            vt[...] = dot(w_s[4], all_a[p], 1, 1).astype(BF16)
            fill_queries(qm, own, w_s[0])
            outs = []
            for t in range(3):
                lanes = slice(t * 256, t * 256 + 256)
                peak = jnp.full((1, 256), -jnp.inf, F32)
                for k0 in range(0, KEYS, 128):
                    keys = slice(k0, k0 + 128)
                    s = dot(kk[keys, :], qm[:, lanes]) + bias_of(bias_s, t, k0, 128)
                    l_s[keys, :] = s
                    peak = jnp.maximum(peak, jnp.max(s, axis=0, keepdims=True))
                total = jnp.zeros((1, 256), F32)
                for k0 in range(0, KEYS, 128):
                    keys = slice(k0, k0 + 128)
                    e = jnp.exp(l_s[keys, :] - peak)
                    total = total + jnp.sum(e, axis=0, keepdims=True)
                    p_s[keys, :] = e.astype(BF16)
                r0, r1 = TILE_ROWS[t]
                outs.append(dot(vt[r0:r1, :], p_s[...]) * (1.0 / total))
            write_rows(p, own, assemble(outs), w_s, z_ref, out_ref)
            return carry

        lax.fori_loop(0, PAIRS, body, 0)
        copy = pltpu.make_async_copy(out_ref, y_out, sems.at[0])
        copy.start()
        copy.wait()


def shifted_call(bad, y, all_a, all_b, z_t, mask, wq, wk, wv, wg, wo):
    args = (all_a, all_b, z_t, mask, wq, wk, wv, wg, wo)
    return pl.pallas_call(
        shifted_kernel,
        out_shape=jax.ShapeDtypeStruct(z_t.shape, BF16),
        in_specs=[pl.BlockSpec(memory_space=pltpu.VMEM)] + [pl.BlockSpec(memory_space=pl.ANY)] * (len(args) + 1),
        out_specs=pl.BlockSpec(memory_space=pl.ANY),
        input_output_aliases={1: 0},
        scratch_shapes=[
            *[pltpu.VMEM(s.shape, s.dtype) for s in args],
            pltpu.SemaphoreType.DMA((len(args),)),
            pltpu.VMEM((KEYS, 384), F32),
            pltpu.VMEM((5, 128, 128), BF16),
            pltpu.VMEM((KEYS, 128), BF16),
            pltpu.VMEM((128, KEYS), BF16),
            pltpu.VMEM((128, KEYS), BF16),
            pltpu.VMEM((KEYS, 256), BF16),
            pltpu.VMEM((KEYS, 256), F32),
            pltpu.VMEM(z_t.shape, BF16),
        ],
        name="shifted",
    )(bad, y, *args)


def solution(mesh):
    tile_spec = P(("dp", "row"), "col", None)

    def per_device(pair_tile, res_mask, ln_gamma, ln_beta, w_q, w_k, w_v, w_b, w_g, w_o):
        z_t = jnp.transpose(pair_tile, (0, 2, 1))
        mask = res_mask.reshape(6, 128)
        y, all_a, all_b, bad = fused_call(
            z_t, ln_gamma.reshape(1, CH), ln_beta.reshape(1, CH), jnp.transpose(w_b), mask, w_q, w_k, w_v, w_g, w_o
        )
        y = shifted_call(bad, y, all_a, all_b, z_t, mask, w_q, w_k, w_v, w_g, w_o)
        return jnp.transpose(y, (0, 2, 1))

    return jax.shard_map(
        per_device, mesh=mesh,
        in_specs=(tile_spec, P("dp"), P(), P(), P(), P(), P(), P(), P(), P()),
        out_specs=tile_spec, check_vma=False,
    )
```

```python
import functools

import jax
import jax.numpy as jnp
from jax import lax
from jax.experimental import pallas as pl
from jax.experimental.pallas import tpu as pltpu
from jax.sharding import PartitionSpec as P

LN_EPS = 1e-5
NEG = -1e9
MESH = pl.DeviceIdType.MESH
F32 = jnp.float32
BF16 = jnp.bfloat16

PAIRS, COLS, CH = 24, 96, 64
HEADS, HEAD = 4, 16
KEYS = 768
BLOCKS = 8
GROUPS, GP = 12, 2
LEAD = 4
LIVE = (384, 512, 672)
TILE_ROWS = ((0, 48), (32, 96), (80, 128))


def dot(a, b, ca=1, cb=0):
    return lax.dot_general(a, b, (((ca,), (cb,)), ((), ())), preferred_element_type=F32)


def iota(shape, dim):
    return lax.broadcasted_iota(jnp.int32, shape, dim)


def column(row_ref, n):
    eye = iota((n, n), 0) == iota((n, n), 1)
    return jnp.sum(jnp.where(eye, jnp.broadcast_to(row_ref[...], (n, n)), 0.0), axis=1, keepdims=True)


def block_diag(w):
    zero = jnp.zeros_like(w)
    return jnp.concatenate(
        [jnp.concatenate([w, zero], axis=1), jnp.concatenate([zero, w], axis=1)], axis=0
    )


def load(pairs, sems):
    copies = [pltpu.make_async_copy(src, dst, sems.at[i]) for i, (src, dst) in enumerate(pairs)]
    for copy in copies:
        copy.start()
    return copies


def fill_weights(w_s, wq_ref, wk_ref, wv_ref, wg_ref, wo_ref):
    w_s[0] = jnp.transpose(block_diag(wq_ref[...]).astype(F32)).astype(BF16)
    w_s[1] = jnp.transpose(block_diag(wg_ref[...]).astype(F32)).astype(BF16)
    w_s[2] = jnp.transpose(block_diag(wo_ref[...]).astype(F32)).astype(BF16)
    w_s[3] = block_diag(wk_ref[...])
    w_s[4] = jnp.transpose(block_diag(wv_ref[...]).astype(F32)).astype(BF16)


def fill_bias(bias_s, all_b, mask_ref, blocks=range(8)):
    length = jnp.sum((mask_ref[...] > 0).astype(F32), axis=1, keepdims=True)
    length = jnp.sum(length, axis=0, keepdims=True)
    for c in blocks:
        tiles = []
        for par in range(2):
            t = all_b[par, c].astype(F32)
            tail = t[96:144]
            tiles.append(jnp.concatenate(
                [t[0:96], jnp.concatenate([tail[:, 0:64], tail[:, 64:128]], axis=0)], axis=1))
        full = jnp.concatenate(
            [tiles[par][:, 48 * h:48 * h + 48] for h in range(HEADS) for par in range(2)], axis=1)
        key = (iota((COLS, 384), 0) + c * COLS).astype(F32)
        bias_s[c * COLS:(c + 1) * COLS, :] = full + jnp.where(key < length, 0.0, NEG)


def bias_of(bias_s, t, k0, nk):
    lo = (2 * t) % 3
    if lo < 2:
        return bias_s[k0:k0 + nk, lo * 128:lo * 128 + 256]
    return jnp.concatenate([bias_s[k0:k0 + nk, 256:384], bias_s[k0:k0 + nk, 0:128]], axis=1)


def fill_queries(qm, own, wq_t):
    q = (dot(wq_t, own, 1, 1) * HEAD ** -0.5).astype(BF16)
    for b in range(BLOCKS):
        qm[b * HEAD:(b + 1) * HEAD, b * COLS:(b + 1) * COLS] = q[b * HEAD:(b + 1) * HEAD, :]


def assemble(o_tiles):
    parts = []
    for b in range(BLOCKS):
        pieces = []
        for t in range(3):
            lo, hi = max(b * 96, t * 256), min(b * 96 + 96, t * 256 + 256)
            if lo < hi:
                r = b * HEAD - TILE_ROWS[t][0]
                pieces.append(o_tiles[t][r:r + HEAD, lo - t * 256:hi - t * 256])
        parts.append(pieces[0] if len(pieces) == 1 else jnp.concatenate(pieces, axis=1))
    return jnp.concatenate(parts, axis=0)


def write_rows(p, own, o, w_s, z_ref, out_ref):
    gate = jax.nn.sigmoid(dot(w_s[1], own, 1, 1))
    update = dot(w_s[2], (gate * o).astype(BF16))
    for hf in range(2):
        res = z_ref[2 * p + hf].astype(F32) + update[hf * CH:(hf + 1) * CH]
        out_ref[2 * p + hf] = res.astype(BF16)


def fused_kernel(
    live_keys,
    z_hbm, gamma_hbm, beta_hbm, wb_hbm, mask_hbm, wq_hbm, wk_hbm, wv_hbm, wg_hbm, wo_hbm,
    out_hbm, all_a_hbm, all_b_hbm, bad_hbm,
    z_ref, gamma_ref, beta_ref, wb_ref, mask_ref, wq_ref, wk_ref, wv_ref, wg_ref, wo_ref, in_sems,
    own_a, own_b, all_a, all_b, out_ref, bias_acc, bias_s, w_s,
    kk0, kk1, vt0, vt1, qm0, qm1, p0, p1, sum0, sum1, o0, o1, bad_s,
    send_b1, recv_b1, send_b2, recv_b2, send_d, recv_d, send_r, recv_r, send_f, recv_f, out_sems,
):
    chunk = live_keys // 2
    kk_s, vt_s, qm_s, p_s, sum_s, o_s = (kk0, kk1), (vt0, vt1), (qm0, qm1), (p0, p1), (sum0, sum1), (o0, o1)
    row = lax.axis_index("row")
    col = lax.axis_index("col")
    z, y = row // 4, row % 4
    x, core = col // 2, col % 2

    copies = load(
        [(gamma_hbm, gamma_ref), (beta_hbm, beta_ref), (wb_hbm, wb_ref)]
        + [(z_hbm.at[pl.ds(12 * n, 12)], z_ref.at[pl.ds(12 * n, 12)]) for n in range(4)]
        + [(mask_hbm, mask_ref), (wq_hbm, wq_ref), (wk_hbm, wk_ref), (wv_hbm, wv_ref), (wg_hbm, wg_ref),
           (wo_hbm, wo_ref)], in_sems)

    right = {"row": row, "col": ((x + 1) % 4) * 2 + core}
    left = {"row": row, "col": ((x + 3) % 4) * 2 + core}
    partner = {"row": row, "col": x * 2 + (1 - core)}
    swap = {"row": 4 * x + y, "col": 2 * z + y // 2}
    is_relay = core == y // 2
    swap_self = jnp.logical_and(z == x, is_relay)

    barrier = pltpu.get_barrier_semaphore()

    def hello(dev):
        pl.semaphore_signal(barrier, inc=1, device_id=dev, device_id_type=MESH)

    for step in range(1, 16):
        hello({"row": (row + step) % 16, "col": col})
    hello(right)
    hello(left)
    hello(partner)

    @pl.when(jnp.logical_not(swap_self))
    def _():
        hello(swap)

    for c in range(2):
        @pl.when(jnp.logical_and(is_relay, jnp.logical_not(jnp.logical_and(z == x, core == c))))
        def _():
            hello({"row": 4 * x + y, "col": 2 * z + c})

    for copy in copies[:3]:
        copy.wait()
    gamma = column(gamma_ref, CH)
    beta = column(beta_ref, CH)
    pick = (iota((192, HEADS), 0) // 48 == iota((192, HEADS), 1)).astype(F32).astype(BF16)
    per_head = dot(pick, wb_ref[...]).astype(BF16)
    wide = jnp.concatenate([per_head, per_head], axis=1)
    keep = iota((192, 128), 0) % 2 == iota((192, 128), 1) // CH
    wide = jnp.where(keep, wide.astype(F32), 0.0).astype(BF16)
    lane_pair = (iota((COLS, 192), 1) % 48) // 2

    def norm_pair(p, carry):
        halves = []
        for half in range(2):
            v = z_ref[2 * p + half].astype(F32)
            mean = jnp.sum(v, axis=0, keepdims=True) * (1.0 / CH)
            centered = v - mean
            var = jnp.sum(centered * centered, axis=0, keepdims=True) * (1.0 / CH)
            halves.append(centered * lax.rsqrt(var + LN_EPS) * gamma + beta)
        a = jnp.transpose(jnp.concatenate(halves, axis=0)).astype(BF16)
        own_a[p] = a
        bias_acc[...] = jnp.where(lane_pair == p, dot(a, wide, 1, 1), bias_acc[...])
        return carry

    for n in range(4):
        copies[3 + n].wait()
        lax.fori_loop(6 * n, 6 * n + 6, norm_pair, 0, unroll=6)
    bias = bias_acc[...]
    own_b[0:96, :] = bias[:, 0:128].astype(BF16)
    own_b[96:144, :] = jnp.concatenate([bias[0:48, 128:192], bias[48:96, 128:192]], axis=1).astype(BF16)

    from_dest = jnp.where(swap_self, 0, 1)
    from_sources = jnp.where(is_relay, jnp.where(z == x, 1, 2), 0)
    pl.semaphore_wait(barrier, 18 + from_dest + from_sources)

    def bias1(c):
        return pltpu.make_async_remote_copy(
            src_ref=own_b, dst_ref=all_b.at[y % 2, 2 * x + c], send_sem=send_b1, recv_sem=recv_b1.at[c],
            device_id=swap, device_id_type=MESH,
        )

    for c in range(2):
        @pl.when(jnp.logical_and(core == c, jnp.logical_not(swap_self)))
        def _():
            bias1(c).start()

    def slot(g, c):
        return all_a.at[pl.ds(g * GP, GP), pl.ds(pl.multiple_of(c * COLS, COLS), COLS)]

    def own(g):
        return own_a.at[pl.ds(g * GP, GP)]

    def direct(src, g, c, way):
        return pltpu.make_async_remote_copy(
            src_ref=src, dst_ref=slot(g, c), send_sem=send_d.at[way, g], recv_sem=recv_d.at[way, g],
            device_id=left if way else right, device_id_type=MESH,
        )

    def relay(g, c, way):
        return pltpu.make_async_remote_copy(
            src_ref=slot(g, c), dst_ref=slot(g, c), send_sem=send_r.at[g], recv_sem=recv_r.at[g],
            device_id=left if way else right, device_id_type=MESH,
        )

    def forward(src, g, c, kind):
        return pltpu.make_async_remote_copy(
            src_ref=src, dst_ref=slot(g, c), send_sem=send_f.at[kind, g], recv_sem=recv_f.at[kind, g],
            device_id=partner, device_id_type=MESH,
        )

    def send_direct(g):
        direct(own(g), g, col, 0).start()
        direct(own(g), g, col, 1).start()

    for g in range(LEAD):
        send_direct(g)
    for g in range(GROUPS):
        forward(own(g), g, col, 0).start()

    @pl.when(swap_self)
    def _():
        all_b[y % 2, col] = own_b[...]

    all_a[:, pl.ds(pl.multiple_of(col * COLS, COLS), COLS), :] = own_a[...]
    for copy in copies[7:]:
        copy.wait()
    fill_weights(w_s, wq_ref, wk_ref, wv_ref, wg_ref, wo_ref)
    for qm in qm_s:
        qm[...] = jnp.zeros_like(qm)

    def peak(ref):
        return jnp.max(jnp.max(jnp.abs(ref[...].astype(F32)), axis=1, keepdims=True), axis=0, keepdims=True)

    norm_max = 8.1 * peak(gamma_ref) + 1.1 * peak(beta_ref)
    limit = 4.2 * (CH * norm_max * peak(wq_ref)) * (CH * norm_max * peak(wk_ref)) + 1.1 * CH * norm_max * peak(wb_ref)
    bad_s[...] = jnp.broadcast_to(jnp.where(limit < 2e8, 0.0, 1.0), bad_s.shape)

    def bias2(step, src_row):
        sz, sy = src_row // 4, src_row % 4
        ref = all_b.at[sy % 2, pl.ds(2 * sz, 2)]
        return pltpu.make_async_remote_copy(
            src_ref=ref, dst_ref=ref, send_sem=send_b2.at[step], recv_sem=recv_b2.at[sy % 2, sz],
            device_id={"row": (row + step) % 16, "col": col}, device_id_type=MESH,
        )

    def bias_relay():
        @pl.when(is_relay)
        def _():
            for c in range(2):
                @pl.when(jnp.logical_not(jnp.logical_and(z == x, core == c)))
                def _():
                    pltpu.make_async_remote_copy(
                        src_ref=own_b, dst_ref=all_b.at[y % 2, 2 * z + c], send_sem=send_b1,
                        recv_sem=recv_b1.at[c], device_id=swap, device_id_type=MESH,
                    ).wait_recv()
            for step in range(1, 16):
                bias2(step, row).start()

    cl, cr, co = ((x + 3) % 4) * 2 + core, ((x + 1) % 4) * 2 + core, ((x + 2) % 4) * 2 + core

    def event(g):
        direct(slot(g, cl), g, cl, 0).wait_recv()

        @pl.when(g % 2 == 0)
        def _():
            relay(g, cl, 0).start()

        forward(slot(g, cl), g, cl, 1).start()
        direct(slot(g, cr), g, cr, 1).wait_recv()

        @pl.when(g % 2 == 1)
        def _():
            relay(g, cr, 1).start()

        forward(slot(g, cr), g, cr, 2).start()

        @pl.when(g < GROUPS - LEAD)
        def _():
            send_direct(g + LEAD)

    def relayed(g):
        relay(g, co, 0).wait_recv()
        forward(slot(g, co), g, co, 3).start()

    def complete(g):
        for kind, dc in ((0, 0), (1, 3), (2, 1), (3, 2)):
            c = ((x + dc) % 4) * 2 + 1 - core
            forward(slot(g, c), g, c, kind).wait_recv()

    def early(g, carry):
        event(g)

        @pl.when(g == 1)
        def _():
            bias_relay()

        @pl.when(g >= 2)
        def _():
            relayed(g - 2)

        return carry

    lax.fori_loop(0, 7, early, 0)

    def project(p, s):
        kk_s[s][...] = dot(all_a[p, 0:live_keys, :], w_s[3]).astype(BF16)
        fill_queries(qm_s[s], own_a[p], w_s[0])

    complete(0)
    project(0, 0)

    for sz in range(4):
        for sy in range(2):
            @pl.when(jnp.logical_not(row == sz * 4 + 2 * core + sy))
            def _():
                ref = all_b.at[sy, pl.ds(2 * sz, 2)]
                pltpu.make_async_remote_copy(
                    src_ref=ref, dst_ref=ref, send_sem=send_b2.at[1], recv_sem=recv_b2.at[sy, sz],
                    device_id=partner, device_id_type=MESH,
                ).wait_recv()
        fill_bias(bias_s, all_b, mask_ref, (2 * sz, 2 * sz + 1))
    b_out = pltpu.make_async_copy(all_b, all_b_hbm, out_sems.at[0])
    b_out.start()

    def values(p, s):
        vt_s[s][...] = dot(w_s[4], all_a[p, 0:live_keys, :], 1, 1).astype(BF16)

    def logits(s, t):
        lanes = slice(t * 256, t * 256 + 256)
        qm = qm_s[s][:, lanes]
        total = jnp.zeros((8, 256), F32)
        for k0 in range(0, live_keys, chunk):
            keys = slice(k0, k0 + chunk)
            e = jnp.exp(dot(kk_s[s][keys, :], qm) + bias_of(bias_s, t, k0, chunk))
            total = total + jnp.sum(e.reshape(chunk // 8, 8, 256), axis=0)
            p_s[s][keys, lanes] = e.astype(BF16)
        sum_s[s][:, lanes] = total

    def combine(s, t, live):
        lanes = slice(t * 256, t * 256 + 256)
        r0, r1 = TILE_ROWS[t]
        o = dot(vt_s[s][r0:r1, :], p_s[s][:, lanes])
        total = jnp.sum(sum_s[s][:, lanes], axis=0, keepdims=True)
        o_max = jnp.max(jnp.abs(o), axis=0, keepdims=True)
        good = (total > 1e-12) & (total < 1e25) & (o_max < 1e35)
        bad_s[0:1, lanes] = jnp.maximum(bad_s[0:1, lanes], jnp.where(good, 0.0, live))
        return o * (1.0 / total)


    a_out = pltpu.make_async_copy(all_a, all_a_hbm, out_sems.at[2])

    def body(m, carry):
        @pl.when((m >= 1) & (m <= 5))
        def _():
            event(m + 6)

        @pl.when((m >= 2) & (m <= 8))
        def _():
            relayed(m + 3)

        @pl.when(m <= 10)
        def _():
            complete(m + 1)

        @pl.when(m == 11)
        def _():
            a_out.start()

        for s in range(2):
            i = 2 * m + s
            live = jnp.where(i >= 1, 1.0, 0.0)
            done = jnp.maximum(i - 2, 0)
            logits(s, 0)
            o_0 = combine(1 - s, 0, live)
            values(i, s)
            logits(s, 1)
            o_1 = combine(1 - s, 1, live)
            project(jnp.minimum(i + 1, PAIRS - 1), 1 - s)
            logits(s, 2)
            o_2 = combine(1 - s, 2, live)
            o_s[1 - s][...] = assemble([o_0, o_1, o_2])
            write_rows(done, own_a[done], o_s[s][...], w_s, z_ref, out_ref)
        return carry

    lax.fori_loop(0, PAIRS // 2, body, 0)
    tail = 2 * PAIRS - 4
    head_out = pltpu.make_async_copy(out_ref.at[0:tail], out_hbm.at[0:tail], out_sems.at[4])
    head_out.start()
    write_rows(PAIRS - 2, own_a[PAIRS - 2], o_s[0][...], w_s, z_ref, out_ref)
    o_s[1][...] = assemble([combine(1, t, 1.0) for t in range(3)])
    write_rows(PAIRS - 1, own_a[PAIRS - 1], o_s[1][...], w_s, z_ref, out_ref)
    outs = [
        pltpu.make_async_copy(out_ref.at[tail:2 * PAIRS], out_hbm.at[tail:2 * PAIRS], out_sems.at[1]),
        pltpu.make_async_copy(bad_s, bad_hbm, out_sems.at[3]),
    ]
    for copy in outs:
        copy.start()

    for c in range(2):
        @pl.when(jnp.logical_and(core == c, jnp.logical_not(swap_self)))
        def _():
            bias1(c).wait_send()

    @pl.when(is_relay)
    def _():
        for step in range(1, 16):
            bias2(step, row).wait_send()

    for g in range(GROUPS):
        direct(own(g), g, col, 0).wait_send()
        direct(own(g), g, col, 1).wait_send()
        relay(g, co, 0).wait_send()
        for kind in range(4):
            forward(own(g), g, col, kind).wait_send()
    for copy in outs:
        copy.wait()
    a_out.wait()
    b_out.wait()
    head_out.wait()


def fused_call(variant, z_t, gamma, beta, wb_t, mask, wq, wk, wv, wg, wo):
    dma = pltpu.SemaphoreType.DMA
    live_keys = LIVE[variant]
    args = (z_t, gamma, beta, wb_t, mask, wq, wk, wv, wg, wo)
    two = lambda *spec: [pltpu.VMEM(*spec)] * 2
    return pl.pallas_call(
        functools.partial(fused_kernel, live_keys),
        out_shape=(
            jax.ShapeDtypeStruct(z_t.shape, BF16),
            jax.ShapeDtypeStruct((PAIRS, KEYS, 128), BF16),
            jax.ShapeDtypeStruct((2, 8, 144, 128), BF16),
            jax.ShapeDtypeStruct((8, KEYS), F32),
        ),
        in_specs=[pl.BlockSpec(memory_space=pl.ANY)] * len(args),
        out_specs=(pl.BlockSpec(memory_space=pl.ANY),) * 4,
        scratch_shapes=[
            *[pltpu.VMEM(s.shape, s.dtype) for s in args],
            dma((13,)),
            pltpu.VMEM((PAIRS, COLS, 128), BF16),
            pltpu.VMEM((144, 128), BF16),
            pltpu.VMEM((PAIRS, KEYS, 128), BF16),
            pltpu.VMEM((2, 8, 144, 128), BF16),
            pltpu.VMEM(z_t.shape, BF16),
            pltpu.VMEM((COLS, 192), F32),
            pltpu.VMEM((KEYS, 384), F32),
            pltpu.VMEM((5, 128, 128), BF16),
            *two((live_keys, 128), BF16),
            *two((128, live_keys), BF16),
            *two((128, KEYS), BF16),
            *two((live_keys, KEYS), BF16),
            *two((8, KEYS), F32),
            *two((128, COLS), F32),
            pltpu.VMEM((8, KEYS), F32),
            dma(()), dma((2,)), dma((16,)), dma((2, 4)),
            dma((2, GROUPS)), dma((2, GROUPS)), dma((GROUPS,)), dma((GROUPS,)), dma((4, GROUPS)), dma((4, GROUPS)),
            dma((5,)),
        ],
        compiler_params=pltpu.CompilerParams(collective_id=variant, has_side_effects=True),
        cost_estimate=pl.CostEstimate(flops=10**11, bytes_accessed=10**9, transcendentals=14 * 10**6),
        name=f"fused{live_keys}",
    )(*args)


def shifted_kernel(
    bad_ref, y_in, all_a_hbm, all_b_hbm, z_hbm, mask_hbm, wq_hbm, wk_hbm, wv_hbm, wg_hbm, wo_hbm,
    y_out,
    all_a, all_b, z_ref, mask_ref, wq_ref, wk_ref, wv_ref, wg_ref, wo_ref, sems,
    bias_s, w_s, kk, vt, qm, p_s, l_s, out_ref,
):
    @pl.when(jnp.max(bad_ref[...]) > 0.0)
    def _():
        col = lax.axis_index("col")
        for copy in load([
            (all_a_hbm, all_a), (all_b_hbm, all_b), (z_hbm, z_ref), (mask_hbm, mask_ref), (wq_hbm, wq_ref),
            (wk_hbm, wk_ref), (wv_hbm, wv_ref), (wg_hbm, wg_ref), (wo_hbm, wo_ref)], sems):
            copy.wait()
        fill_weights(w_s, wq_ref, wk_ref, wv_ref, wg_ref, wo_ref)
        fill_bias(bias_s, all_b, mask_ref)
        qm[...] = jnp.zeros_like(qm)

        def body(p, carry):
            own = all_a[p, pl.ds(pl.multiple_of(col * COLS, COLS), COLS), :]
            kk[...] = dot(all_a[p], w_s[3]).astype(BF16)
            vt[...] = dot(w_s[4], all_a[p], 1, 1).astype(BF16)
            fill_queries(qm, own, w_s[0])
            outs = []
            for t in range(3):
                lanes = slice(t * 256, t * 256 + 256)
                peak = jnp.full((1, 256), -jnp.inf, F32)
                for k0 in range(0, KEYS, 128):
                    keys = slice(k0, k0 + 128)
                    s = dot(kk[keys, :], qm[:, lanes]) + bias_of(bias_s, t, k0, 128)
                    l_s[keys, :] = s
                    peak = jnp.maximum(peak, jnp.max(s, axis=0, keepdims=True))
                total = jnp.zeros((1, 256), F32)
                for k0 in range(0, KEYS, 128):
                    keys = slice(k0, k0 + 128)
                    e = jnp.exp(l_s[keys, :] - peak)
                    total = total + jnp.sum(e, axis=0, keepdims=True)
                    p_s[keys, :] = e.astype(BF16)
                r0, r1 = TILE_ROWS[t]
                outs.append(dot(vt[r0:r1, :], p_s[...]) * (1.0 / total))
            write_rows(p, own, assemble(outs), w_s, z_ref, out_ref)
            return carry

        lax.fori_loop(0, PAIRS, body, 0)
        copy = pltpu.make_async_copy(out_ref, y_out, sems.at[0])
        copy.start()
        copy.wait()


def shifted_call(bad, y, all_a, all_b, z_t, mask, wq, wk, wv, wg, wo):
    args = (all_a, all_b, z_t, mask, wq, wk, wv, wg, wo)
    return pl.pallas_call(
        shifted_kernel,
        out_shape=jax.ShapeDtypeStruct(z_t.shape, BF16),
        in_specs=[pl.BlockSpec(memory_space=pltpu.VMEM)] + [pl.BlockSpec(memory_space=pl.ANY)] * (len(args) + 1),
        out_specs=pl.BlockSpec(memory_space=pl.ANY),
        input_output_aliases={1: 0},
        scratch_shapes=[
            *[pltpu.VMEM(s.shape, s.dtype) for s in args],
            pltpu.SemaphoreType.DMA((len(args),)),
            pltpu.VMEM((KEYS, 384), F32),
            pltpu.VMEM((5, 128, 128), BF16),
            pltpu.VMEM((KEYS, 128), BF16),
            pltpu.VMEM((128, KEYS), BF16),
            pltpu.VMEM((128, KEYS), BF16),
            pltpu.VMEM((KEYS, 256), BF16),
            pltpu.VMEM((KEYS, 256), F32),
            pltpu.VMEM(z_t.shape, BF16),
        ],
        name="shifted",
    )(bad, y, *args)


def solution(mesh):
    tile_spec = P(("dp", "row"), "col", None)

    def per_device(pair_tile, res_mask, ln_gamma, ln_beta, w_q, w_k, w_v, w_b, w_g, w_o):
        z_t = jnp.transpose(pair_tile, (0, 2, 1))
        mask = res_mask.reshape(6, 128)
        length = jnp.sum((res_mask > 0).astype(jnp.int32))
        variant = (length > LIVE[0]).astype(jnp.int32) + (length > LIVE[1]).astype(jnp.int32)
        y, all_a, all_b, bad = lax.switch(
            variant, [functools.partial(fused_call, n) for n in range(3)],
            z_t, ln_gamma.reshape(1, CH), ln_beta.reshape(1, CH), jnp.transpose(w_b), mask, w_q, w_k, w_v, w_g, w_o
        )
        y = shifted_call(bad, y, all_a, all_b, z_t, mask, w_q, w_k, w_v, w_g, w_o)
        return jnp.transpose(y, (0, 2, 1))

    return jax.shard_map(
        per_device, mesh=mesh,
        in_specs=(tile_spec, P("dp"), P(), P(), P(), P(), P(), P(), P(), P()),
        out_specs=tile_spec, check_vma=False,
    )
```

```python
import functools

import jax
import jax.numpy as jnp
from jax import lax
from jax.experimental import pallas as pl
from jax.experimental.pallas import tpu as pltpu
from jax.sharding import PartitionSpec as P

LN_EPS = 1e-5
NEG = -1e9
MESH = pl.DeviceIdType.MESH
F32 = jnp.float32
BF16 = jnp.bfloat16

PAIRS, COLS, CH = 24, 96, 64
HEADS, HEAD = 4, 16
KEYS = 768
BLOCKS = 8
GROUPS, GP = 12, 2
LEAD = 4
LIVE = (384, 480, 576, 672, 768)
TILE_ROWS = ((0, 48), (32, 96), (80, 128))


def dot(a, b, ca=1, cb=0):
    return lax.dot_general(a, b, (((ca,), (cb,)), ((), ())), preferred_element_type=F32)


def iota(shape, dim):
    return lax.broadcasted_iota(jnp.int32, shape, dim)


def column(row_ref, n):
    eye = iota((n, n), 0) == iota((n, n), 1)
    return jnp.sum(jnp.where(eye, jnp.broadcast_to(row_ref[...], (n, n)), 0.0), axis=1, keepdims=True)


def block_diag(w):
    zero = jnp.zeros_like(w)
    return jnp.concatenate(
        [jnp.concatenate([w, zero], axis=1), jnp.concatenate([zero, w], axis=1)], axis=0
    )


def load(pairs, sems):
    copies = [pltpu.make_async_copy(src, dst, sems.at[i]) for i, (src, dst) in enumerate(pairs)]
    for copy in copies:
        copy.start()
    return copies


def fill_weights(w_s, wq_ref, wk_ref, wv_ref, wg_ref, wo_ref):
    w_s[0] = jnp.transpose(block_diag(wq_ref[...]).astype(F32)).astype(BF16)
    w_s[1] = jnp.transpose(block_diag(wg_ref[...]).astype(F32)).astype(BF16)
    w_s[2] = jnp.transpose(block_diag(wo_ref[...]).astype(F32)).astype(BF16)
    w_s[3] = block_diag(wk_ref[...])
    w_s[4] = jnp.transpose(block_diag(wv_ref[...]).astype(F32)).astype(BF16)


def fill_bias(bias_s, all_b, mask_ref, blocks=range(8)):
    length = jnp.sum((mask_ref[...] > 0).astype(F32), axis=1, keepdims=True)
    length = jnp.sum(length, axis=0, keepdims=True)
    for c in blocks:
        tiles = []
        for par in range(2):
            t = all_b[par, c].astype(F32)
            tail = t[96:144]
            tiles.append(jnp.concatenate(
                [t[0:96], jnp.concatenate([tail[:, 0:64], tail[:, 64:128]], axis=0)], axis=1))
        full = jnp.concatenate(
            [tiles[par][:, 48 * h:48 * h + 48] for h in range(HEADS) for par in range(2)], axis=1)
        key = (iota((COLS, 384), 0) + c * COLS).astype(F32)
        bias_s[c * COLS:(c + 1) * COLS, :] = full + jnp.where(key < length, 0.0, NEG)


def bias_of(bias_s, t, k0, nk):
    lo = (2 * t) % 3
    if lo < 2:
        return bias_s[k0:k0 + nk, lo * 128:lo * 128 + 256]
    return jnp.concatenate([bias_s[k0:k0 + nk, 256:384], bias_s[k0:k0 + nk, 0:128]], axis=1)


def fill_queries(qm, own, wq_t):
    q = (dot(wq_t, own, 1, 1) * HEAD ** -0.5).astype(BF16)
    for b in range(BLOCKS):
        qm[b * HEAD:(b + 1) * HEAD, b * COLS:(b + 1) * COLS] = q[b * HEAD:(b + 1) * HEAD, :]


def assemble(o_tiles):
    parts = []
    for b in range(BLOCKS):
        pieces = []
        for t in range(3):
            lo, hi = max(b * 96, t * 256), min(b * 96 + 96, t * 256 + 256)
            if lo < hi:
                r = b * HEAD - TILE_ROWS[t][0]
                pieces.append(o_tiles[t][r:r + HEAD, lo - t * 256:hi - t * 256])
        parts.append(pieces[0] if len(pieces) == 1 else jnp.concatenate(pieces, axis=1))
    return jnp.concatenate(parts, axis=0)


def write_rows(p, own, o, w_s, z_ref, out_ref):
    gate = jax.nn.sigmoid(dot(w_s[1], own, 1, 1))
    update = dot(w_s[2], (gate * o).astype(BF16))
    for hf in range(2):
        res = z_ref[2 * p + hf].astype(F32) + update[hf * CH:(hf + 1) * CH]
        out_ref[2 * p + hf] = res.astype(BF16)


def pick_kernel(mask_hbm, gamma_hbm, beta_hbm, wq_hbm, wk_hbm, wb_hbm, out_ref,
                mask_ref, gamma_ref, beta_ref, wq_ref, wk_ref, wb_ref, sems):
    for copy in load([(mask_hbm, mask_ref), (gamma_hbm, gamma_ref), (beta_hbm, beta_ref), (wq_hbm, wq_ref),
                      (wk_hbm, wk_ref), (wb_hbm, wb_ref)], sems):
        copy.wait()
    length = jnp.sum((mask_ref[...] > 0).astype(F32))

    def peak(ref):
        return jnp.max(jnp.abs(ref[...].astype(F32)))

    norm_max = 8.1 * peak(gamma_ref) + 1.1 * peak(beta_ref)
    limit = 4.2 * (CH * norm_max * peak(wq_ref)) * (CH * norm_max * peak(wk_ref)) + 1.1 * CH * norm_max * peak(wb_ref)
    build = sum((length > n).astype(jnp.int32) for n in LIVE[:3])
    out_ref[0] = jnp.where(limit < 2e8, build, 4)


def pick_call(mask, gamma, beta, wq, wk, wb_t):
    args = (mask, gamma, beta, wq, wk, wb_t)
    return pl.pallas_call(
        pick_kernel,
        out_shape=jax.ShapeDtypeStruct((1,), jnp.int32),
        in_specs=[pl.BlockSpec(memory_space=pl.ANY)] * len(args),
        out_specs=pl.BlockSpec(memory_space=pltpu.SMEM),
        scratch_shapes=[*[pltpu.VMEM(s.shape, s.dtype) for s in args], pltpu.SemaphoreType.DMA((len(args),))],
        name="pick",
    )(*args)


def fused_kernel(
    live_keys,
    z_hbm, gamma_hbm, beta_hbm, wb_hbm, mask_hbm, wq_hbm, wk_hbm, wv_hbm, wg_hbm, wo_hbm,
    out_hbm, all_a_hbm, all_b_hbm, bad_hbm,
    z_ref, gamma_ref, beta_ref, wb_ref, mask_ref, wq_ref, wk_ref, wv_ref, wg_ref, wo_ref, in_sems,
    own_a, own_b, all_a, all_b, out_ref, bias_acc, bias_s, w_s,
    kk0, kk1, vt0, vt1, qm0, qm1, p0, p1, sum0, sum1, o0, o1, bad_s,
    send_b1, recv_b1, send_b2, recv_b2, send_d, recv_d, send_r, recv_r, send_f, recv_f, out_sems,
):
    chunk = live_keys // 2
    blocks = -(-live_keys // COLS)
    sources = -(-blocks // 2)
    lead = GROUPS if sources == 2 else LEAD
    kk_s, vt_s, qm_s, p_s, sum_s, o_s = (kk0, kk1), (vt0, vt1), (qm0, qm1), (p0, p1), (sum0, sum1), (o0, o1)
    row = lax.axis_index("row")
    col = lax.axis_index("col")
    z, y = row // 4, row % 4
    x, core = col // 2, col % 2

    copies = load(
        [(gamma_hbm, gamma_ref), (beta_hbm, beta_ref), (wb_hbm, wb_ref)]
        + [(z_hbm.at[pl.ds(12 * n, 12)], z_ref.at[pl.ds(12 * n, 12)]) for n in range(4)]
        + [(mask_hbm, mask_ref), (wq_hbm, wq_ref), (wk_hbm, wk_ref), (wv_hbm, wv_ref), (wg_hbm, wg_ref),
           (wo_hbm, wo_ref)], in_sems)

    right = {"row": row, "col": ((x + 1) % 4) * 2 + core}
    left = {"row": row, "col": ((x + 3) % 4) * 2 + core}
    partner = {"row": row, "col": x * 2 + (1 - core)}
    swap = {"row": 4 * x + y, "col": 2 * z + y // 2}
    is_relay = core == y // 2
    swap_self = jnp.logical_and(z == x, is_relay)

    barrier = pltpu.get_barrier_semaphore()

    def hello(dev):
        pl.semaphore_signal(barrier, inc=1, device_id=dev, device_id_type=MESH)

    for step in range(1, 16):
        hello({"row": (row + step) % 16, "col": col})
    hello(right)
    hello(left)
    hello(partner)

    @pl.when(jnp.logical_not(swap_self))
    def _():
        hello(swap)

    for c in range(2):
        @pl.when(jnp.logical_and(is_relay, jnp.logical_not(jnp.logical_and(z == x, core == c))))
        def _():
            hello({"row": 4 * x + y, "col": 2 * z + c})

    for copy in copies[:3]:
        copy.wait()
    gamma = column(gamma_ref, CH)
    beta = column(beta_ref, CH)
    pick = (iota((192, HEADS), 0) // 48 == iota((192, HEADS), 1)).astype(F32).astype(BF16)
    per_head = dot(pick, wb_ref[...]).astype(BF16)
    wide = jnp.concatenate([per_head, per_head], axis=1)
    keep = iota((192, 128), 0) % 2 == iota((192, 128), 1) // CH
    wide = jnp.where(keep, wide.astype(F32), 0.0).astype(BF16)
    lane_pair = (iota((COLS, 192), 1) % 48) // 2

    def norm_pair(p, carry):
        halves = []
        for half in range(2):
            v = z_ref[2 * p + half].astype(F32)
            mean = jnp.sum(v, axis=0, keepdims=True) * (1.0 / CH)
            centered = v - mean
            var = jnp.sum(centered * centered, axis=0, keepdims=True) * (1.0 / CH)
            halves.append(centered * lax.rsqrt(var + LN_EPS) * gamma + beta)
        a = jnp.transpose(jnp.concatenate(halves, axis=0)).astype(BF16)
        own_a[p] = a
        bias_acc[...] = jnp.where(lane_pair == p, dot(a, wide, 1, 1), bias_acc[...])
        return carry

    for n in range(4):
        copies[3 + n].wait()
        lax.fori_loop(6 * n, 6 * n + 6, norm_pair, 0, unroll=6)
    bias = bias_acc[...]
    own_b[0:96, :] = bias[:, 0:128].astype(BF16)
    own_b[96:144, :] = jnp.concatenate([bias[0:48, 128:192], bias[48:96, 128:192]], axis=1).astype(BF16)

    from_dest = jnp.where(swap_self, 0, 1)
    from_sources = jnp.where(is_relay, jnp.where(z == x, 1, 2), 0)
    pl.semaphore_wait(barrier, 18 + from_dest + from_sources)

    def bias1(c):
        return pltpu.make_async_remote_copy(
            src_ref=own_b, dst_ref=all_b.at[y % 2, 2 * x + c], send_sem=send_b1, recv_sem=recv_b1.at[c],
            device_id=swap, device_id_type=MESH,
        )

    for c in range(2):
        @pl.when((core == c) & (x < sources) & jnp.logical_not(swap_self))
        def _():
            bias1(c).start()

    def slot(g, c):
        return all_a.at[pl.ds(g * GP, GP), pl.ds(pl.multiple_of(c * COLS, COLS), COLS)]

    def own(g):
        return own_a.at[pl.ds(g * GP, GP)]

    def direct(src, g, c, way):
        return pltpu.make_async_remote_copy(
            src_ref=src, dst_ref=slot(g, c), send_sem=send_d.at[way, g], recv_sem=recv_d.at[way, g],
            device_id=left if way else right, device_id_type=MESH,
        )

    def relay(g, c, way):
        return pltpu.make_async_remote_copy(
            src_ref=slot(g, c), dst_ref=slot(g, c), send_sem=send_r.at[g], recv_sem=recv_r.at[g],
            device_id=left if way else right, device_id_type=MESH,
        )

    def forward(src, g, c, kind):
        return pltpu.make_async_remote_copy(
            src_ref=src, dst_ref=slot(g, c), send_sem=send_f.at[kind, g], recv_sem=recv_f.at[kind, g],
            device_id=partner, device_id_type=MESH,
        )

    cl, cr, co = ((x + 3) % 4) * 2 + core, ((x + 1) % 4) * 2 + core, ((x + 2) % 4) * 2 + core
    mine, has_left, has_right, has_opposite = col < blocks, cl < blocks, cr < blocks, co < blocks

    def to_right(g):
        return has_left & (x == 2 if sources == 2 else g % 2 == 0)

    def to_left(g):
        return has_right & (x == 3 if sources == 2 else g % 2 == 1)

    def send_direct(g):
        direct(own(g), g, col, 0).start()
        direct(own(g), g, col, 1).start()

    @pl.when(mine)
    def _():
        for g in range(lead):
            send_direct(g)
        for g in range(GROUPS):
            forward(own(g), g, col, 0).start()

    @pl.when(swap_self & (x < sources))
    def _():
        all_b[y % 2, col] = own_b[...]

    all_a[:, pl.ds(pl.multiple_of(col * COLS, COLS), COLS), :] = own_a[...]
    for copy in copies[7:]:
        copy.wait()
    fill_weights(w_s, wq_ref, wk_ref, wv_ref, wg_ref, wo_ref)
    for qm in qm_s:
        qm[...] = jnp.zeros_like(qm)

    bad_s[...] = jnp.where(iota(bad_s.shape, 0) == 1, float(live_keys), 0.0)

    def bias2(step, src_row):
        sz, sy = src_row // 4, src_row % 4
        ref = all_b.at[sy % 2, pl.ds(2 * sz, 2)]
        return pltpu.make_async_remote_copy(
            src_ref=ref, dst_ref=ref, send_sem=send_b2.at[step], recv_sem=recv_b2.at[sy % 2, sz],
            device_id={"row": (row + step) % 16, "col": col}, device_id_type=MESH,
        )

    def bias_relay():
        @pl.when(is_relay & (z < sources))
        def _():
            for c in range(2):
                @pl.when(jnp.logical_not(jnp.logical_and(z == x, core == c)))
                def _():
                    pltpu.make_async_remote_copy(
                        src_ref=own_b, dst_ref=all_b.at[y % 2, 2 * z + c], send_sem=send_b1,
                        recv_sem=recv_b1.at[c], device_id=swap, device_id_type=MESH,
                    ).wait_recv()
            for step in range(1, 16):
                bias2(step, row).start()

    def event(g):
        @pl.when(has_left)
        def _():
            direct(slot(g, cl), g, cl, 0).wait_recv()

            @pl.when(to_right(g))
            def _():
                relay(g, cl, 0).start()

            forward(slot(g, cl), g, cl, 1).start()

        @pl.when(has_right)
        def _():
            direct(slot(g, cr), g, cr, 1).wait_recv()

            @pl.when(to_left(g))
            def _():
                relay(g, cr, 1).start()

            forward(slot(g, cr), g, cr, 2).start()

        @pl.when(mine & (g < GROUPS - lead))
        def _():
            send_direct(g + lead)

    def relayed(g):
        @pl.when(has_opposite)
        def _():
            relay(g, co, 0).wait_recv()
            forward(slot(g, co), g, co, 3).start()

    def complete(g):
        for kind, dc in ((0, 0), (1, 3), (2, 1), (3, 2)):
            c = ((x + dc) % 4) * 2 + 1 - core

            @pl.when(c < blocks)
            def _():
                forward(slot(g, c), g, c, kind).wait_recv()

    def early(g, carry):
        event(g)

        @pl.when(g == 1)
        def _():
            bias_relay()

        @pl.when(g >= 2)
        def _():
            relayed(g - 2)

        return carry

    lax.fori_loop(0, 7, early, 0)

    def project(p, s):
        kk_s[s][...] = dot(all_a[p, 0:live_keys, :], w_s[3]).astype(BF16)
        fill_queries(qm_s[s], own_a[p], w_s[0])

    complete(0)
    project(0, 0)

    for sz in range(sources):
        for sy in range(2):
            @pl.when(jnp.logical_not(row == sz * 4 + 2 * core + sy))
            def _():
                ref = all_b.at[sy, pl.ds(2 * sz, 2)]
                pltpu.make_async_remote_copy(
                    src_ref=ref, dst_ref=ref, send_sem=send_b2.at[1], recv_sem=recv_b2.at[sy, sz],
                    device_id=partner, device_id_type=MESH,
                ).wait_recv()
        fill_bias(bias_s, all_b, mask_ref, (2 * sz, 2 * sz + 1))
    b_out = pltpu.make_async_copy(all_b, all_b_hbm, out_sems.at[0])
    b_out.start()

    def values(p, s):
        vt_s[s][...] = dot(w_s[4], all_a[p, 0:live_keys, :], 1, 1).astype(BF16)

    def logits(s, t):
        lanes = slice(t * 256, t * 256 + 256)
        qm = qm_s[s][:, lanes]
        total = jnp.zeros((8, 256), F32)
        for k0 in range(0, live_keys, chunk):
            keys = slice(k0, k0 + chunk)
            e = jnp.exp(dot(kk_s[s][keys, :], qm) + bias_of(bias_s, t, k0, chunk))
            total = total + jnp.sum(e.reshape(chunk // 8, 8, 256), axis=0)
            p_s[s][keys, lanes] = e.astype(BF16)
        sum_s[s][:, lanes] = total

    def combine(s, t, live):
        lanes = slice(t * 256, t * 256 + 256)
        r0, r1 = TILE_ROWS[t]
        o = dot(vt_s[s][r0:r1, :], p_s[s][:, lanes])
        total = jnp.sum(sum_s[s][:, lanes], axis=0, keepdims=True)
        o_max = jnp.max(jnp.abs(o), axis=0, keepdims=True)
        good = (total > 1e-12) & (total < 1e25) & (o_max < 1e35)
        bad_s[0:1, lanes] = jnp.maximum(bad_s[0:1, lanes], jnp.where(good, 0.0, live))
        return o * (1.0 / total)


    a_out = pltpu.make_async_copy(all_a, all_a_hbm, out_sems.at[2])

    def body(m, carry):
        @pl.when((m >= 1) & (m <= 5))
        def _():
            event(m + 6)

        @pl.when((m >= 2) & (m <= 8))
        def _():
            relayed(m + 3)

        @pl.when(m <= 10)
        def _():
            complete(m + 1)

        @pl.when(m == 11)
        def _():
            a_out.start()

        for s in range(2):
            i = 2 * m + s
            live = jnp.where(i >= 1, 1.0, 0.0)
            done = jnp.maximum(i - 2, 0)
            logits(s, 0)
            o_0 = combine(1 - s, 0, live)
            values(i, s)
            logits(s, 1)
            o_1 = combine(1 - s, 1, live)
            project(jnp.minimum(i + 1, PAIRS - 1), 1 - s)
            logits(s, 2)
            o_2 = combine(1 - s, 2, live)
            o_s[1 - s][...] = assemble([o_0, o_1, o_2])
            write_rows(done, own_a[done], o_s[s][...], w_s, z_ref, out_ref)
        return carry

    lax.fori_loop(0, PAIRS // 2, body, 0)
    tail = 2 * PAIRS - 4
    head_out = pltpu.make_async_copy(out_ref.at[0:tail], out_hbm.at[0:tail], out_sems.at[4])
    head_out.start()
    write_rows(PAIRS - 2, own_a[PAIRS - 2], o_s[0][...], w_s, z_ref, out_ref)
    o_s[1][...] = assemble([combine(1, t, 1.0) for t in range(3)])
    write_rows(PAIRS - 1, own_a[PAIRS - 1], o_s[1][...], w_s, z_ref, out_ref)
    outs = [
        pltpu.make_async_copy(out_ref.at[tail:2 * PAIRS], out_hbm.at[tail:2 * PAIRS], out_sems.at[1]),
        pltpu.make_async_copy(bad_s, bad_hbm, out_sems.at[3]),
    ]
    for copy in outs:
        copy.start()

    for c in range(2):
        @pl.when((core == c) & (x < sources) & jnp.logical_not(swap_self))
        def _():
            bias1(c).wait_send()

    @pl.when(is_relay & (z < sources))
    def _():
        for step in range(1, 16):
            bias2(step, row).wait_send()

    def sent(g, carry):
        @pl.when(mine)
        def _():
            direct(own(g), g, col, 0).wait_send()
            direct(own(g), g, col, 1).wait_send()

        @pl.when(to_right(g))
        def _():
            relay(g, cl, 0).wait_send()

        @pl.when(to_left(g))
        def _():
            relay(g, cr, 1).wait_send()

        for kind, there in enumerate((mine, has_left, has_right, has_opposite)):
            @pl.when(there)
            def _():
                forward(own(g), g, col, kind).wait_send()

        return carry

    lax.fori_loop(0, GROUPS, sent, 0)
    for copy in outs:
        copy.wait()
    a_out.wait()
    b_out.wait()
    head_out.wait()


def fused_call(variant, z_t, gamma, beta, wb_t, mask, wq, wk, wv, wg, wo):
    dma = pltpu.SemaphoreType.DMA
    live_keys = LIVE[variant]
    args = (z_t, gamma, beta, wb_t, mask, wq, wk, wv, wg, wo)
    two = lambda *spec: [pltpu.VMEM(*spec)] * 2
    return pl.pallas_call(
        functools.partial(fused_kernel, live_keys),
        out_shape=(
            jax.ShapeDtypeStruct(z_t.shape, BF16),
            jax.ShapeDtypeStruct((PAIRS, KEYS, 128), BF16),
            jax.ShapeDtypeStruct((2, 8, 144, 128), BF16),
            jax.ShapeDtypeStruct((8, KEYS), F32),
        ),
        in_specs=[pl.BlockSpec(memory_space=pl.ANY)] * len(args),
        out_specs=(pl.BlockSpec(memory_space=pl.ANY),) * 4,
        scratch_shapes=[
            *[pltpu.VMEM(s.shape, s.dtype) for s in args],
            dma((13,)),
            pltpu.VMEM((PAIRS, COLS, 128), BF16),
            pltpu.VMEM((144, 128), BF16),
            pltpu.VMEM((PAIRS, KEYS, 128), BF16),
            pltpu.VMEM((2, 8, 144, 128), BF16),
            pltpu.VMEM(z_t.shape, BF16),
            pltpu.VMEM((COLS, 192), F32),
            pltpu.VMEM((KEYS, 384), F32),
            pltpu.VMEM((5, 128, 128), BF16),
            *two((live_keys, 128), BF16),
            *two((128, live_keys), BF16),
            *two((128, KEYS), BF16),
            *two((live_keys, KEYS), BF16),
            *two((8, KEYS), F32),
            *two((128, COLS), F32),
            pltpu.VMEM((8, KEYS), F32),
            dma(()), dma((2,)), dma((16,)), dma((2, 4)),
            dma((2, GROUPS)), dma((2, GROUPS)), dma((GROUPS,)), dma((GROUPS,)), dma((4, GROUPS)), dma((4, GROUPS)),
            dma((5,)),
        ],
        compiler_params=pltpu.CompilerParams(collective_id=variant, has_side_effects=True),
        cost_estimate=pl.CostEstimate(flops=10**11, bytes_accessed=10**9, transcendentals=14 * 10**6),
        name=f"fused{live_keys}",
    )(*args)


def shifted_kernel(
    bad_ref, y_in, all_a_hbm, all_b_hbm, z_hbm, mask_hbm, wq_hbm, wk_hbm, wv_hbm, wg_hbm, wo_hbm,
    y_out,
    all_a, all_b, z_ref, mask_ref, wq_ref, wk_ref, wv_ref, wg_ref, wo_ref, sems,
    bias_s, w_s, kk, vt, qm, p_s, l_s, out_ref,
):
    @pl.when(jnp.max(bad_ref[0:1, :]) > 0.0)
    def _():
        col = lax.axis_index("col")
        for copy in load([
            (all_a_hbm, all_a), (all_b_hbm, all_b), (z_hbm, z_ref), (mask_hbm, mask_ref), (wq_hbm, wq_ref),
            (wk_hbm, wk_ref), (wv_hbm, wv_ref), (wg_hbm, wg_ref), (wo_hbm, wo_ref)], sems):
            copy.wait()
        fill_weights(w_s, wq_ref, wk_ref, wv_ref, wg_ref, wo_ref)
        fill_bias(bias_s, all_b, mask_ref)
        live_keys = bad_ref[1:2, 0:128]
        there = iota((KEYS, 128), 0).astype(F32) < live_keys
        for lanes in range(0, 384, 128):
            bias_s[:, lanes:lanes + 128] = jnp.where(there, bias_s[:, lanes:lanes + 128], NEG)
        qm[...] = jnp.zeros_like(qm)

        def body(p, carry):
            own = all_a[p, pl.ds(pl.multiple_of(col * COLS, COLS), COLS), :]
            keys_a = jnp.where(there, all_a[p].astype(F32), 0.0).astype(BF16)
            kk[...] = dot(keys_a, w_s[3]).astype(BF16)
            vt[...] = dot(w_s[4], keys_a, 1, 1).astype(BF16)
            fill_queries(qm, own, w_s[0])
            outs = []
            for t in range(3):
                lanes = slice(t * 256, t * 256 + 256)
                peak = jnp.full((1, 256), -jnp.inf, F32)
                for k0 in range(0, KEYS, 128):
                    keys = slice(k0, k0 + 128)
                    s = dot(kk[keys, :], qm[:, lanes]) + bias_of(bias_s, t, k0, 128)
                    l_s[keys, :] = s
                    peak = jnp.maximum(peak, jnp.max(s, axis=0, keepdims=True))
                total = jnp.zeros((1, 256), F32)
                for k0 in range(0, KEYS, 128):
                    keys = slice(k0, k0 + 128)
                    e = jnp.exp(l_s[keys, :] - peak)
                    total = total + jnp.sum(e, axis=0, keepdims=True)
                    p_s[keys, :] = e.astype(BF16)
                r0, r1 = TILE_ROWS[t]
                outs.append(dot(vt[r0:r1, :], p_s[...]) * (1.0 / total))
            write_rows(p, own, assemble(outs), w_s, z_ref, out_ref)
            return carry

        lax.fori_loop(0, PAIRS, body, 0)
        copy = pltpu.make_async_copy(out_ref, y_out, sems.at[0])
        copy.start()
        copy.wait()


def shifted_call(bad, y, all_a, all_b, z_t, mask, wq, wk, wv, wg, wo):
    args = (all_a, all_b, z_t, mask, wq, wk, wv, wg, wo)
    return pl.pallas_call(
        shifted_kernel,
        out_shape=jax.ShapeDtypeStruct(z_t.shape, BF16),
        in_specs=[pl.BlockSpec(memory_space=pltpu.VMEM)] + [pl.BlockSpec(memory_space=pl.ANY)] * (len(args) + 1),
        out_specs=pl.BlockSpec(memory_space=pl.ANY),
        input_output_aliases={1: 0},
        scratch_shapes=[
            *[pltpu.VMEM(s.shape, s.dtype) for s in args],
            pltpu.SemaphoreType.DMA((len(args),)),
            pltpu.VMEM((KEYS, 384), F32),
            pltpu.VMEM((5, 128, 128), BF16),
            pltpu.VMEM((KEYS, 128), BF16),
            pltpu.VMEM((128, KEYS), BF16),
            pltpu.VMEM((128, KEYS), BF16),
            pltpu.VMEM((KEYS, 256), BF16),
            pltpu.VMEM((KEYS, 256), F32),
            pltpu.VMEM(z_t.shape, BF16),
        ],
        name="shifted",
    )(bad, y, *args)


def solution(mesh):
    tile_spec = P(("dp", "row"), "col", None)

    def per_device(pair_tile, res_mask, ln_gamma, ln_beta, w_q, w_k, w_v, w_b, w_g, w_o):
        z_t = jnp.transpose(pair_tile, (0, 2, 1))
        mask = res_mask.reshape(6, 128)
        gamma, beta, wb_t = ln_gamma.reshape(1, CH), ln_beta.reshape(1, CH), jnp.transpose(w_b)
        build = pick_call(mask, gamma, beta, w_q, w_k, wb_t)
        y, all_a, all_b, bad = lax.switch(
            build[0], [functools.partial(fused_call, n) for n in range(len(LIVE))],
            z_t, gamma, beta, wb_t, mask, w_q, w_k, w_v, w_g, w_o
        )
        y = shifted_call(bad, y, all_a, all_b, z_t, mask, w_q, w_k, w_v, w_g, w_o)
        return jnp.transpose(y, (0, 2, 1))

    return jax.shard_map(
        per_device, mesh=mesh,
        in_specs=(tile_spec, P("dp"), P(), P(), P(), P(), P(), P(), P(), P()),
        out_specs=tile_spec, check_vma=False,
    )
```

```python
import functools

import jax
import jax.numpy as jnp
from jax import lax
from jax.experimental import pallas as pl
from jax.experimental.pallas import tpu as pltpu
from jax.sharding import PartitionSpec as P

LN_EPS = 1e-5
NEG = -1e9
MESH = pl.DeviceIdType.MESH
F32 = jnp.float32
BF16 = jnp.bfloat16

PAIRS, COLS, CH = 24, 96, 64
HEADS, HEAD = 4, 16
KEYS = 768
LANES, TILE = 128, 256
BLOCKS = 8
GROUPS, GP = 12, 2
EARLY, EARLY_KEYS = 8, 480
LEAD = 4
LIVE = (384, 480, 544, 672, 768)
TILE_ROWS = ((0, 48), (32, 96), (80, 128))


def dot(a, b, ca=1, cb=0):
    return lax.dot_general(a, b, (((ca,), (cb,)), ((), ())), preferred_element_type=F32)


def iota(shape, dim):
    return lax.broadcasted_iota(jnp.int32, shape, dim)


def column(row_ref, n):
    eye = iota((n, n), 0) == iota((n, n), 1)
    return jnp.sum(jnp.where(eye, jnp.broadcast_to(row_ref[...], (n, n)), 0.0), axis=1, keepdims=True)


def block_diag(w):
    zero = jnp.zeros_like(w)
    return jnp.concatenate(
        [jnp.concatenate([w, zero], axis=1), jnp.concatenate([zero, w], axis=1)], axis=0
    )


def load(pairs, sems):
    copies = [pltpu.make_async_copy(src, dst, sems.at[i]) for i, (src, dst) in enumerate(pairs)]
    for copy in copies:
        copy.start()
    return copies


def fill_weights(w_s, wq_ref, wk_ref, wv_ref, wg_ref, wo_ref):
    w_s[0] = jnp.transpose(block_diag(wq_ref[...]).astype(F32)).astype(BF16)
    w_s[1] = jnp.transpose(block_diag(wg_ref[...]).astype(F32)).astype(BF16)
    w_s[2] = jnp.transpose(block_diag(wo_ref[...]).astype(F32)).astype(BF16)
    w_s[3] = block_diag(wk_ref[...])
    w_s[4] = jnp.transpose(block_diag(wv_ref[...]).astype(F32)).astype(BF16)


def fill_bias(bias_s, all_b, mask_ref, blocks=range(8)):
    length = jnp.sum((mask_ref[...] > 0).astype(F32), axis=1, keepdims=True)
    length = jnp.sum(length, axis=0, keepdims=True)
    for c in blocks:
        tiles = []
        for par in range(2):
            t = all_b[par, c].astype(F32)
            tail = t[96:144]
            tiles.append(jnp.concatenate(
                [t[0:96], jnp.concatenate([tail[:, 0:64], tail[:, 64:LANES]], axis=0)], axis=1))
        full = jnp.concatenate(
            [tiles[par][:, 48 * h:48 * h + 48] for h in range(HEADS) for par in range(2)], axis=1)
        key = (iota((COLS, 384), 0) + c * COLS).astype(F32)
        bias_s[c * COLS:(c + 1) * COLS, :] = full + jnp.where(key < length, 0.0, NEG)


def bias_of(bias_s, t, k0, nk):
    lo = (2 * t) % 3
    if lo < 2:
        return bias_s[k0:k0 + nk, lo * LANES:lo * LANES + TILE]
    return jnp.concatenate([bias_s[k0:k0 + nk, TILE:384], bias_s[k0:k0 + nk, 0:LANES]], axis=1)


def fill_queries(qm, own, wq_t):
    q = (dot(wq_t, own, 1, 1) * HEAD ** -0.5).astype(BF16)
    for b in range(BLOCKS):
        qm[b * HEAD:(b + 1) * HEAD, b * COLS:(b + 1) * COLS] = q[b * HEAD:(b + 1) * HEAD, :]


def assemble(o_tiles):
    parts = []
    for b in range(BLOCKS):
        pieces = []
        for t in range(3):
            lo, hi = max(b * 96, t * TILE), min(b * 96 + 96, t * TILE + TILE)
            if lo < hi:
                r = b * HEAD - TILE_ROWS[t][0]
                pieces.append(o_tiles[t][r:r + HEAD, lo - t * TILE:hi - t * TILE])
        parts.append(pieces[0] if len(pieces) == 1 else jnp.concatenate(pieces, axis=1))
    return jnp.concatenate(parts, axis=0)


def write_rows(p, own, o, w_s, z_ref, out_ref):
    gate = jax.nn.sigmoid(dot(w_s[1], own, 1, 1))
    update = dot(w_s[2], (gate * o).astype(BF16))
    for hf in range(2):
        res = z_ref[2 * p + hf].astype(F32) + update[hf * CH:(hf + 1) * CH]
        out_ref[2 * p + hf] = res.astype(BF16)


def pick_kernel(mask_hbm, gamma_hbm, beta_hbm, wq_hbm, wk_hbm, wb_hbm, out_ref,
                mask_ref, gamma_ref, beta_ref, wq_ref, wk_ref, wb_ref, sems):
    for copy in load([(mask_hbm, mask_ref), (gamma_hbm, gamma_ref), (beta_hbm, beta_ref), (wq_hbm, wq_ref),
                      (wk_hbm, wk_ref), (wb_hbm, wb_ref)], sems):
        copy.wait()
    length = jnp.sum((mask_ref[...] > 0).astype(F32))

    def peak(ref):
        return jnp.max(jnp.abs(ref[...].astype(F32)))

    norm_max = 8.1 * peak(gamma_ref) + 1.1 * peak(beta_ref)
    limit = 4.2 * (CH * norm_max * peak(wq_ref)) * (CH * norm_max * peak(wk_ref)) + 1.1 * CH * norm_max * peak(wb_ref)
    build = sum((length > n).astype(jnp.int32) for n in LIVE[:3])
    out_ref[0] = jnp.where(limit < 2e8, build, 4)


def pick_call(mask, gamma, beta, wq, wk, wb_t):
    args = (mask, gamma, beta, wq, wk, wb_t)
    return pl.pallas_call(
        pick_kernel,
        out_shape=jax.ShapeDtypeStruct((1,), jnp.int32),
        in_specs=[pl.BlockSpec(memory_space=pl.ANY)] * len(args),
        out_specs=pl.BlockSpec(memory_space=pltpu.SMEM),
        scratch_shapes=[*[pltpu.VMEM(s.shape, s.dtype) for s in args], pltpu.SemaphoreType.DMA((len(args),))],
        name="pick",
    )(*args)


def fused_kernel(
    live_keys,
    z_hbm, gamma_hbm, beta_hbm, wb_hbm, mask_hbm, wq_hbm, wk_hbm, wv_hbm, wg_hbm, wo_hbm,
    out_hbm, all_a_hbm, all_b_hbm, bad_hbm,
    z_ref, gamma_ref, beta_ref, wb_ref, mask_ref, wq_ref, wk_ref, wv_ref, wg_ref, wo_ref, in_sems,
    own_a, own_b, all_a, all_b, out_ref, bias_acc, bias_s, w_s,
    kk0, kk1, vt0, vt1, kk_e, vt_e, qm0, qm1, p0, p1, sum0, sum1, o0, o1, bad_s,
    send_b1, recv_b1, send_b2, recv_b2, send_d, recv_d, send_r, recv_r, send_f, recv_f, out_sems,
):
    chunk = live_keys // 2
    blocks = -(-live_keys // COLS)
    sources = -(-blocks // 2)
    lead = GROUPS if sources == 2 else LEAD
    is_early = live_keys <= EARLY_KEYS
    kk_s, vt_s, qm_s, p_s, sum_s, o_s = (kk0, kk1), (vt0, vt1), (qm0, qm1), (p0, p1), (sum0, sum1), (o0, o1)
    row = lax.axis_index("row")
    col = lax.axis_index("col")
    z, y = row // 4, row % 4
    x, core = col // 2, col % 2

    copies = load(
        [(gamma_hbm, gamma_ref), (beta_hbm, beta_ref), (wb_hbm, wb_ref)]
        + [(z_hbm.at[pl.ds(12 * n, 12)], z_ref.at[pl.ds(12 * n, 12)]) for n in range(4)]
        + [(mask_hbm, mask_ref), (wq_hbm, wq_ref), (wk_hbm, wk_ref), (wv_hbm, wv_ref), (wg_hbm, wg_ref),
           (wo_hbm, wo_ref)], in_sems)

    right = {"row": row, "col": ((x + 1) % 4) * 2 + core}
    left = {"row": row, "col": ((x + 3) % 4) * 2 + core}
    partner = {"row": row, "col": x * 2 + (1 - core)}
    swap = {"row": 4 * x + y, "col": 2 * z + y // 2}
    is_relay = core == y // 2
    swap_self = jnp.logical_and(z == x, is_relay)

    barrier = pltpu.get_barrier_semaphore()

    def hello(dev):
        pl.semaphore_signal(barrier, inc=1, device_id=dev, device_id_type=MESH)

    for step in range(1, 16):
        hello({"row": (row + step) % 16, "col": col})
    hello(right)
    hello(left)
    hello(partner)

    @pl.when(jnp.logical_not(swap_self))
    def _():
        hello(swap)

    for c in range(2):
        @pl.when(jnp.logical_and(is_relay, jnp.logical_not(jnp.logical_and(z == x, core == c))))
        def _():
            hello({"row": 4 * x + y, "col": 2 * z + c})

    for copy in copies[:3]:
        copy.wait()
    gamma = column(gamma_ref, CH)
    beta = column(beta_ref, CH)
    pick = (iota((192, HEADS), 0) // 48 == iota((192, HEADS), 1)).astype(F32).astype(BF16)
    per_head = dot(pick, wb_ref[...]).astype(BF16)
    wide = jnp.concatenate([per_head, per_head], axis=1)
    keep = iota((192, LANES), 0) % 2 == iota((192, LANES), 1) // CH
    wide = jnp.where(keep, wide.astype(F32), 0.0).astype(BF16)
    lane_pair = (iota((COLS, 192), 1) % 48) // 2

    def norm_pair(p, carry):
        halves = []
        for half in range(2):
            v = z_ref[2 * p + half].astype(F32)
            mean = jnp.sum(v, axis=0, keepdims=True) * (1.0 / CH)
            centered = v - mean
            var = jnp.sum(centered * centered, axis=0, keepdims=True) * (1.0 / CH)
            halves.append(centered * lax.rsqrt(var + LN_EPS) * gamma + beta)
        a = jnp.transpose(jnp.concatenate(halves, axis=0)).astype(BF16)
        own_a[p] = a
        bias_acc[...] = jnp.where(lane_pair == p, dot(a, wide, 1, 1), bias_acc[...])
        return carry

    for n in range(4):
        copies[3 + n].wait()
        lax.fori_loop(6 * n, 6 * n + 6, norm_pair, 0, unroll=6)
    bias = bias_acc[...]
    own_b[0:96, :] = bias[:, 0:LANES].astype(BF16)
    own_b[96:144, :] = jnp.concatenate([bias[0:48, LANES:192], bias[48:96, LANES:192]], axis=1).astype(BF16)

    from_dest = jnp.where(swap_self, 0, 1)
    from_sources = jnp.where(is_relay, jnp.where(z == x, 1, 2), 0)
    pl.semaphore_wait(barrier, 18 + from_dest + from_sources)

    def bias1(c):
        return pltpu.make_async_remote_copy(
            src_ref=own_b, dst_ref=all_b.at[y % 2, 2 * x + c], send_sem=send_b1, recv_sem=recv_b1.at[c],
            device_id=swap, device_id_type=MESH,
        )

    for c in range(2):
        @pl.when((core == c) & (x < sources) & jnp.logical_not(swap_self))
        def _():
            bias1(c).start()

    def slot(g, c):
        return all_a.at[pl.ds(g * GP, GP), pl.ds(pl.multiple_of(c * COLS, COLS), COLS)]

    def own(g):
        return own_a.at[pl.ds(g * GP, GP)]

    def direct(src, g, c, way):
        return pltpu.make_async_remote_copy(
            src_ref=src, dst_ref=slot(g, c), send_sem=send_d.at[way, g], recv_sem=recv_d.at[way, g],
            device_id=left if way else right, device_id_type=MESH,
        )

    def relay(g, c, way):
        return pltpu.make_async_remote_copy(
            src_ref=slot(g, c), dst_ref=slot(g, c), send_sem=send_r.at[g], recv_sem=recv_r.at[g],
            device_id=left if way else right, device_id_type=MESH,
        )

    def forward(src, g, c, kind):
        return pltpu.make_async_remote_copy(
            src_ref=src, dst_ref=slot(g, c), send_sem=send_f.at[kind, g], recv_sem=recv_f.at[kind, g],
            device_id=partner, device_id_type=MESH,
        )

    cl, cr, co = ((x + 3) % 4) * 2 + core, ((x + 1) % 4) * 2 + core, ((x + 2) % 4) * 2 + core
    mine, has_left, has_right, has_opposite = col < blocks, cl < blocks, cr < blocks, co < blocks

    def to_right(g):
        return has_left & (x == 2 if sources == 2 else g % 2 == 0)

    def to_left(g):
        return has_right & (x == 3 if sources == 2 else g % 2 == 1)

    def send_direct(g):
        direct(own(g), g, col, 0).start()
        direct(own(g), g, col, 1).start()

    @pl.when(mine)
    def _():
        for g in range(lead):
            send_direct(g)
        for g in range(GROUPS):
            forward(own(g), g, col, 0).start()

    @pl.when(swap_self & (x < sources))
    def _():
        all_b[y % 2, col] = own_b[...]

    all_a[:, pl.ds(pl.multiple_of(col * COLS, COLS), COLS), :] = own_a[...]
    for copy in copies[7:]:
        copy.wait()
    fill_weights(w_s, wq_ref, wk_ref, wv_ref, wg_ref, wo_ref)
    for qm in qm_s:
        qm[...] = jnp.zeros_like(qm)

    bad_s[...] = jnp.where(iota(bad_s.shape, 0) == 1, float(live_keys), 0.0)

    def bias2(step, src_row):
        sz, sy = src_row // 4, src_row % 4
        ref = all_b.at[sy % 2, pl.ds(2 * sz, 2)]
        return pltpu.make_async_remote_copy(
            src_ref=ref, dst_ref=ref, send_sem=send_b2.at[step], recv_sem=recv_b2.at[sy % 2, sz],
            device_id={"row": (row + step) % 16, "col": col}, device_id_type=MESH,
        )

    def bias_relay():
        @pl.when(is_relay & (z < sources))
        def _():
            for c in range(2):
                @pl.when(jnp.logical_not(jnp.logical_and(z == x, core == c)))
                def _():
                    pltpu.make_async_remote_copy(
                        src_ref=own_b, dst_ref=all_b.at[y % 2, 2 * z + c], send_sem=send_b1,
                        recv_sem=recv_b1.at[c], device_id=swap, device_id_type=MESH,
                    ).wait_recv()
            for step in range(1, 16):
                bias2(step, row).start()

    def event(g):
        @pl.when(has_left)
        def _():
            direct(slot(g, cl), g, cl, 0).wait_recv()

            @pl.when(to_right(g))
            def _():
                relay(g, cl, 0).start()

            forward(slot(g, cl), g, cl, 1).start()

        @pl.when(has_right)
        def _():
            direct(slot(g, cr), g, cr, 1).wait_recv()

            @pl.when(to_left(g))
            def _():
                relay(g, cr, 1).start()

            forward(slot(g, cr), g, cr, 2).start()

        @pl.when(mine & (g < GROUPS - lead))
        def _():
            send_direct(g + lead)

    def relayed(g):
        @pl.when(has_opposite)
        def _():
            relay(g, co, 0).wait_recv()
            forward(slot(g, co), g, co, 3).start()

    def complete(g):
        for kind, dc in ((0, 0), (1, 3), (2, 1), (3, 2)):
            c = ((x + dc) % 4) * 2 + 1 - core

            @pl.when(c < blocks)
            def _():
                forward(slot(g, c), g, c, kind).wait_recv()

    def project(p, s):
        kk_s[s][...] = dot(all_a[p, 0:live_keys, :], w_s[3]).astype(BF16)
        fill_queries(qm_s[s], own_a[p], w_s[0])

    def key_of(p):
        return dot(all_a[p, 0:live_keys, :], w_s[3]).astype(BF16)

    def value_of(p):
        return dot(w_s[4], all_a[p, 0:live_keys, :], 1, 1).astype(BF16)

    def ahead(g):
        complete(g)
        for n in range(GP):
            kk_e[GP * g + n] = key_of(GP * g + n)
            vt_e[GP * g + n] = value_of(GP * g + n)

    def early(g, carry):
        event(g)

        @pl.when(g == 1)
        def _():
            bias_relay()

        @pl.when(g >= 2)
        def _():
            relayed(g - 2)

        if is_early:
            @pl.when(g >= 4)
            def _():
                ahead(g - 4)

        return carry

    lax.fori_loop(0, 7, early, 0)

    if is_early:
        ahead(3)
        complete(4)
        kk0[...] = key_of(EARLY)
        vt1[...] = vt_e[EARLY - 1]
        fill_queries(qm0, own_a[0], w_s[0])
    else:
        complete(0)
        project(0, 0)

    for sz in range(sources):
        for sy in range(2):
            @pl.when(jnp.logical_not(row == sz * 4 + 2 * core + sy))
            def _():
                ref = all_b.at[sy, pl.ds(2 * sz, 2)]
                pltpu.make_async_remote_copy(
                    src_ref=ref, dst_ref=ref, send_sem=send_b2.at[1], recv_sem=recv_b2.at[sy, sz],
                    device_id=partner, device_id_type=MESH,
                ).wait_recv()
        fill_bias(bias_s, all_b, mask_ref, (2 * sz, 2 * sz + 1))
    b_out = pltpu.make_async_copy(all_b, all_b_hbm, out_sems.at[0])
    b_out.start()

    def logits(kk, s, t):
        lanes = slice(t * TILE, t * TILE + TILE)
        qm = qm_s[s][:, lanes]
        total = jnp.zeros((8, TILE), F32)
        for k0 in range(0, live_keys, chunk):
            keys = slice(k0, k0 + chunk)
            e = jnp.exp(dot(kk[keys, :], qm) + bias_of(bias_s, t, k0, chunk))
            total = total + jnp.sum(e.reshape(chunk // 8, 8, TILE), axis=0)
            p_s[s][keys, lanes] = e.astype(BF16)
        sum_s[s][:, lanes] = total

    def combine(vt, s, t, live):
        lanes = slice(t * TILE, t * TILE + TILE)
        r0, r1 = TILE_ROWS[t]
        o = dot(vt[r0:r1, :], p_s[s][:, lanes])
        total = jnp.sum(sum_s[s][:, lanes], axis=0, keepdims=True)
        o_max = jnp.max(jnp.abs(o), axis=0, keepdims=True)
        good = (total > 1e-12) & (total < 1e25) & (o_max < 1e35)
        bad_s[0:1, lanes] = jnp.maximum(bad_s[0:1, lanes], jnp.where(good, 0.0, live))
        return o * (1.0 / total)


    a_out = pltpu.make_async_copy(all_a, all_a_hbm, out_sems.at[2])

    def polls(m):
        @pl.when((m >= 1) & (m <= 5))
        def _():
            event(m + 6)

        @pl.when((m >= 2) & (m <= 8))
        def _():
            relayed(m + 3)

        @pl.when((m >= (4 if is_early else 0)) & (m <= 10))
        def _():
            complete(m + 1)

        @pl.when(m == 11)
        def _():
            a_out.start()

    def step(m, s, ahead_of_time):
        i = 2 * m + s
        live = jnp.where(i >= 1, 1.0, 0.0)
        done = jnp.maximum(i - 2, 0)
        kk = kk_e.at[i] if ahead_of_time else kk_s[s]
        vt = vt_e.at[jnp.maximum(i - 1, 0)] if ahead_of_time else vt_s[1 - s]
        logits(kk, s, 0)
        o_0 = combine(vt, 1 - s, 0, live)
        if not ahead_of_time:
            vt_s[s][...] = value_of(i)
        logits(kk, s, 1)
        o_1 = combine(vt, 1 - s, 1, live)
        following = jnp.minimum(i + 1, PAIRS - 1)
        if ahead_of_time:
            fill_queries(qm_s[1 - s], own_a[following], w_s[0])
        else:
            project(following, 1 - s)
        logits(kk, s, 2)
        o_2 = combine(vt, 1 - s, 2, live)
        o_s[1 - s][...] = assemble([o_0, o_1, o_2])
        write_rows(done, own_a[done], o_s[s][...], w_s, z_ref, out_ref)

    def body(ahead_of_time, m, carry):
        polls(m)
        for s in range(2):
            step(m, s, ahead_of_time)
        return carry

    if is_early:
        lax.fori_loop(0, EARLY // 2, functools.partial(body, True), 0)
    lax.fori_loop(EARLY // 2 if is_early else 0, PAIRS // 2, functools.partial(body, False), 0)
    tail = 2 * PAIRS - 4
    head_out = pltpu.make_async_copy(out_ref.at[0:tail], out_hbm.at[0:tail], out_sems.at[4])
    head_out.start()
    write_rows(PAIRS - 2, own_a[PAIRS - 2], o_s[0][...], w_s, z_ref, out_ref)
    o_s[1][...] = assemble([combine(vt1, 1, t, 1.0) for t in range(3)])
    write_rows(PAIRS - 1, own_a[PAIRS - 1], o_s[1][...], w_s, z_ref, out_ref)
    outs = [
        pltpu.make_async_copy(out_ref.at[tail:2 * PAIRS], out_hbm.at[tail:2 * PAIRS], out_sems.at[1]),
        pltpu.make_async_copy(bad_s, bad_hbm, out_sems.at[3]),
    ]
    for copy in outs:
        copy.start()

    for c in range(2):
        @pl.when((core == c) & (x < sources) & jnp.logical_not(swap_self))
        def _():
            bias1(c).wait_send()

    @pl.when(is_relay & (z < sources))
    def _():
        for step in range(1, 16):
            bias2(step, row).wait_send()

    def sent(g, carry):
        @pl.when(mine)
        def _():
            direct(own(g), g, col, 0).wait_send()
            direct(own(g), g, col, 1).wait_send()

        @pl.when(to_right(g))
        def _():
            relay(g, cl, 0).wait_send()

        @pl.when(to_left(g))
        def _():
            relay(g, cr, 1).wait_send()

        for kind, there in enumerate((mine, has_left, has_right, has_opposite)):
            @pl.when(there)
            def _():
                forward(own(g), g, col, kind).wait_send()

        return carry

    lax.fori_loop(0, GROUPS, sent, 0)
    for copy in outs:
        copy.wait()
    a_out.wait()
    b_out.wait()
    head_out.wait()


def fused_call(variant, z_t, gamma, beta, wb_t, mask, wq, wk, wv, wg, wo):
    dma = pltpu.SemaphoreType.DMA
    live_keys = LIVE[variant]
    args = (z_t, gamma, beta, wb_t, mask, wq, wk, wv, wg, wo)
    two = lambda *spec: [pltpu.VMEM(*spec)] * 2
    return pl.pallas_call(
        functools.partial(fused_kernel, live_keys),
        out_shape=(
            jax.ShapeDtypeStruct(z_t.shape, BF16),
            jax.ShapeDtypeStruct((PAIRS, KEYS, LANES), BF16),
            jax.ShapeDtypeStruct((2, 8, 144, LANES), BF16),
            jax.ShapeDtypeStruct((8, KEYS), F32),
        ),
        in_specs=[pl.BlockSpec(memory_space=pl.ANY)] * len(args),
        out_specs=(pl.BlockSpec(memory_space=pl.ANY),) * 4,
        scratch_shapes=[
            *[pltpu.VMEM(s.shape, s.dtype) for s in args],
            dma((13,)),
            pltpu.VMEM((PAIRS, COLS, LANES), BF16),
            pltpu.VMEM((144, LANES), BF16),
            pltpu.VMEM((PAIRS, KEYS, LANES), BF16),
            pltpu.VMEM((2, 8, 144, LANES), BF16),
            pltpu.VMEM(z_t.shape, BF16),
            pltpu.VMEM((COLS, 192), F32),
            pltpu.VMEM((KEYS, 384), F32),
            pltpu.VMEM((5, LANES, LANES), BF16),
            *two((live_keys, LANES), BF16),
            *two((LANES, live_keys), BF16),
            pltpu.VMEM((EARLY, min(live_keys, EARLY_KEYS), LANES), BF16),
            pltpu.VMEM((EARLY, LANES, min(live_keys, EARLY_KEYS)), BF16),
            *two((LANES, KEYS), BF16),
            *two((live_keys, KEYS), BF16),
            *two((8, KEYS), F32),
            *two((LANES, COLS), F32),
            pltpu.VMEM((8, KEYS), F32),
            dma(()), dma((2,)), dma((16,)), dma((2, 4)),
            dma((2, GROUPS)), dma((2, GROUPS)), dma((GROUPS,)), dma((GROUPS,)), dma((4, GROUPS)), dma((4, GROUPS)),
            dma((5,)),
        ],
        compiler_params=pltpu.CompilerParams(collective_id=variant, has_side_effects=True),
        cost_estimate=pl.CostEstimate(flops=10**11, bytes_accessed=10**9, transcendentals=14 * 10**6),
        name=f"fused{live_keys}",
    )(*args)


def shifted_kernel(
    bad_ref, y_in, all_a_hbm, all_b_hbm, z_hbm, mask_hbm, wq_hbm, wk_hbm, wv_hbm, wg_hbm, wo_hbm,
    y_out,
    all_a, all_b, z_ref, mask_ref, wq_ref, wk_ref, wv_ref, wg_ref, wo_ref, sems,
    bias_s, w_s, kk, vt, qm, p_s, l_s, out_ref,
):
    @pl.when(jnp.max(bad_ref[0:1, :]) > 0.0)
    def _():
        col = lax.axis_index("col")
        for copy in load([
            (all_a_hbm, all_a), (all_b_hbm, all_b), (z_hbm, z_ref), (mask_hbm, mask_ref), (wq_hbm, wq_ref),
            (wk_hbm, wk_ref), (wv_hbm, wv_ref), (wg_hbm, wg_ref), (wo_hbm, wo_ref)], sems):
            copy.wait()
        fill_weights(w_s, wq_ref, wk_ref, wv_ref, wg_ref, wo_ref)
        fill_bias(bias_s, all_b, mask_ref)
        live_keys = bad_ref[1:2, 0:LANES]
        there = iota((KEYS, LANES), 0).astype(F32) < live_keys
        for lanes in range(0, 384, LANES):
            bias_s[:, lanes:lanes + LANES] = jnp.where(there, bias_s[:, lanes:lanes + LANES], NEG)
        qm[...] = jnp.zeros_like(qm)

        def body(p, carry):
            own = all_a[p, pl.ds(pl.multiple_of(col * COLS, COLS), COLS), :]
            keys_a = jnp.where(there, all_a[p].astype(F32), 0.0).astype(BF16)
            kk[...] = dot(keys_a, w_s[3]).astype(BF16)
            vt[...] = dot(w_s[4], keys_a, 1, 1).astype(BF16)
            fill_queries(qm, own, w_s[0])
            outs = []
            for t in range(3):
                lanes = slice(t * TILE, t * TILE + TILE)
                peak = jnp.full((1, TILE), -jnp.inf, F32)
                for k0 in range(0, KEYS, LANES):
                    keys = slice(k0, k0 + LANES)
                    s = dot(kk[keys, :], qm[:, lanes]) + bias_of(bias_s, t, k0, LANES)
                    l_s[keys, :] = s
                    peak = jnp.maximum(peak, jnp.max(s, axis=0, keepdims=True))
                total = jnp.zeros((1, TILE), F32)
                for k0 in range(0, KEYS, LANES):
                    keys = slice(k0, k0 + LANES)
                    e = jnp.exp(l_s[keys, :] - peak)
                    total = total + jnp.sum(e, axis=0, keepdims=True)
                    p_s[keys, :] = e.astype(BF16)
                r0, r1 = TILE_ROWS[t]
                outs.append(dot(vt[r0:r1, :], p_s[...]) * (1.0 / total))
            write_rows(p, own, assemble(outs), w_s, z_ref, out_ref)
            return carry

        lax.fori_loop(0, PAIRS, body, 0)
        copy = pltpu.make_async_copy(out_ref, y_out, sems.at[0])
        copy.start()
        copy.wait()


def shifted_call(bad, y, all_a, all_b, z_t, mask, wq, wk, wv, wg, wo):
    args = (all_a, all_b, z_t, mask, wq, wk, wv, wg, wo)
    return pl.pallas_call(
        shifted_kernel,
        out_shape=jax.ShapeDtypeStruct(z_t.shape, BF16),
        in_specs=[pl.BlockSpec(memory_space=pltpu.VMEM)] + [pl.BlockSpec(memory_space=pl.ANY)] * (len(args) + 1),
        out_specs=pl.BlockSpec(memory_space=pl.ANY),
        input_output_aliases={1: 0},
        scratch_shapes=[
            *[pltpu.VMEM(s.shape, s.dtype) for s in args],
            pltpu.SemaphoreType.DMA((len(args),)),
            pltpu.VMEM((KEYS, 384), F32),
            pltpu.VMEM((5, LANES, LANES), BF16),
            pltpu.VMEM((KEYS, LANES), BF16),
            pltpu.VMEM((LANES, KEYS), BF16),
            pltpu.VMEM((LANES, KEYS), BF16),
            pltpu.VMEM((KEYS, TILE), BF16),
            pltpu.VMEM((KEYS, TILE), F32),
            pltpu.VMEM(z_t.shape, BF16),
        ],
        name="shifted",
    )(bad, y, *args)


def solution(mesh):
    tile_spec = P(("dp", "row"), "col", None)

    def per_device(pair_tile, res_mask, ln_gamma, ln_beta, w_q, w_k, w_v, w_b, w_g, w_o):
        z_t = jnp.transpose(pair_tile, (0, 2, 1))
        mask = res_mask.reshape(6, LANES)
        gamma, beta, wb_t = ln_gamma.reshape(1, CH), ln_beta.reshape(1, CH), jnp.transpose(w_b)
        build = pick_call(mask, gamma, beta, w_q, w_k, wb_t)
        y, all_a, all_b, bad = lax.switch(
            build[0], [functools.partial(fused_call, n) for n in range(len(LIVE))],
            z_t, gamma, beta, wb_t, mask, w_q, w_k, w_v, w_g, w_o
        )
        y = shifted_call(bad, y, all_a, all_b, z_t, mask, w_q, w_k, w_v, w_g, w_o)
        return jnp.transpose(y, (0, 2, 1))

    return jax.shard_map(
        per_device, mesh=mesh,
        in_specs=(tile_spec, P("dp"), P(), P(), P(), P(), P(), P(), P(), P()),
        out_specs=tile_spec, check_vma=False,
    )
```

```python
import functools

import jax
import jax.numpy as jnp
from jax import lax
from jax.experimental import pallas as pl
from jax.experimental.pallas import tpu as pltpu
from jax.sharding import PartitionSpec as P

LN_EPS = 1e-5
NEG = -1e9
MESH = pl.DeviceIdType.MESH
F32 = jnp.float32
BF16 = jnp.bfloat16

PAIRS, COLS, CH = 24, 96, 64
HEADS, HEAD = 4, 16
KEYS = 768
LANES, TILE = 128, 256
BLOCKS = 8
GROUPS, GP = 12, 2
EARLY, EARLY_KEYS = 8, 480
LEAD = 4
LIVE = (384, 480, 544, 672, 768)
TILE_ROWS = ((0, 48), (32, 96), (80, 128))


def dot(a, b, ca=1, cb=0):
    return lax.dot_general(a, b, (((ca,), (cb,)), ((), ())), preferred_element_type=F32)


def iota(shape, dim):
    return lax.broadcasted_iota(jnp.int32, shape, dim)


def column(row_ref, n):
    eye = iota((n, n), 0) == iota((n, n), 1)
    return jnp.sum(jnp.where(eye, jnp.broadcast_to(row_ref[...], (n, n)), 0.0), axis=1, keepdims=True)


def block_diag(w):
    zero = jnp.zeros_like(w)
    return jnp.concatenate(
        [jnp.concatenate([w, zero], axis=1), jnp.concatenate([zero, w], axis=1)], axis=0
    )


def load(pairs, sems):
    copies = [pltpu.make_async_copy(src, dst, sems.at[i]) for i, (src, dst) in enumerate(pairs)]
    for copy in copies:
        copy.start()
    return copies


def fill_weights(w_s, wq_ref, wk_ref, wv_ref, wg_ref, wo_ref):
    w_s[0] = jnp.transpose(block_diag(wq_ref[...]).astype(F32)).astype(BF16)
    w_s[1] = jnp.transpose(block_diag(wg_ref[...]).astype(F32)).astype(BF16)
    w_s[2] = jnp.transpose(block_diag(wo_ref[...]).astype(F32)).astype(BF16)
    w_s[3] = block_diag(wk_ref[...])
    w_s[4] = jnp.transpose(block_diag(wv_ref[...]).astype(F32)).astype(BF16)


def fill_bias(bias_s, all_b, mask_ref, blocks=range(8)):
    length = jnp.sum((mask_ref[...] > 0).astype(F32), axis=1, keepdims=True)
    length = jnp.sum(length, axis=0, keepdims=True)
    for c in blocks:
        tiles = []
        for par in range(2):
            t = all_b[par, c].astype(F32)
            tail = t[96:144]
            tiles.append(jnp.concatenate(
                [t[0:96], jnp.concatenate([tail[:, 0:64], tail[:, 64:LANES]], axis=0)], axis=1))
        full = jnp.concatenate(
            [tiles[par][:, 48 * h:48 * h + 48] for h in range(HEADS) for par in range(2)], axis=1)
        key = (iota((COLS, 384), 0) + c * COLS).astype(F32)
        bias_s[c * COLS:(c + 1) * COLS, :] = full + jnp.where(key < length, 0.0, NEG)


def bias_of(bias_s, t, k0, nk):
    lo = (2 * t) % 3
    if lo < 2:
        return bias_s[k0:k0 + nk, lo * LANES:lo * LANES + TILE]
    return jnp.concatenate([bias_s[k0:k0 + nk, TILE:384], bias_s[k0:k0 + nk, 0:LANES]], axis=1)


def fill_queries(qm, own, wq_t):
    q = (dot(wq_t, own, 1, 1) * HEAD ** -0.5).astype(BF16)
    for b in range(BLOCKS):
        qm[b * HEAD:(b + 1) * HEAD, b * COLS:(b + 1) * COLS] = q[b * HEAD:(b + 1) * HEAD, :]


def assemble(o_tiles):
    parts = []
    for b in range(BLOCKS):
        pieces = []
        for t in range(3):
            lo, hi = max(b * 96, t * TILE), min(b * 96 + 96, t * TILE + TILE)
            if lo < hi:
                r = b * HEAD - TILE_ROWS[t][0]
                pieces.append(o_tiles[t][r:r + HEAD, lo - t * TILE:hi - t * TILE])
        parts.append(pieces[0] if len(pieces) == 1 else jnp.concatenate(pieces, axis=1))
    return jnp.concatenate(parts, axis=0)


def write_rows(p, own, o, w_s, z_ref, out_ref):
    gate = jax.nn.sigmoid(dot(w_s[1], own, 1, 1))
    update = dot(w_s[2], (gate * o).astype(BF16))
    for hf in range(2):
        res = z_ref[2 * p + hf].astype(F32) + update[hf * CH:(hf + 1) * CH]
        out_ref[2 * p + hf] = res.astype(BF16)


def pick_kernel(mask_hbm, gamma_hbm, beta_hbm, wq_hbm, wk_hbm, wb_hbm, out_ref,
                mask_ref, gamma_ref, beta_ref, wq_ref, wk_ref, wb_ref, sems):
    for copy in load([(mask_hbm, mask_ref), (gamma_hbm, gamma_ref), (beta_hbm, beta_ref), (wq_hbm, wq_ref),
                      (wk_hbm, wk_ref), (wb_hbm, wb_ref)], sems):
        copy.wait()
    length = jnp.sum((mask_ref[...] > 0).astype(F32))

    def peak(ref):
        return jnp.max(jnp.abs(ref[...].astype(F32)))

    norm_max = 8.1 * peak(gamma_ref) + 1.1 * peak(beta_ref)
    limit = 4.2 * (CH * norm_max * peak(wq_ref)) * (CH * norm_max * peak(wk_ref)) + 1.1 * CH * norm_max * peak(wb_ref)
    build = sum((length > n).astype(jnp.int32) for n in LIVE[:3])
    out_ref[0] = jnp.where(limit < 2e8, build, 4)


def pick_call(mask, gamma, beta, wq, wk, wb_t):
    args = (mask, gamma, beta, wq, wk, wb_t)
    return pl.pallas_call(
        pick_kernel,
        out_shape=jax.ShapeDtypeStruct((1,), jnp.int32),
        in_specs=[pl.BlockSpec(memory_space=pl.ANY)] * len(args),
        out_specs=pl.BlockSpec(memory_space=pltpu.SMEM),
        scratch_shapes=[*[pltpu.VMEM(s.shape, s.dtype) for s in args], pltpu.SemaphoreType.DMA((len(args),))],
        name="pick",
    )(*args)


def fused_kernel(
    live_keys,
    z_hbm, gamma_hbm, beta_hbm, wb_hbm, mask_hbm, wq_hbm, wk_hbm, wv_hbm, wg_hbm, wo_hbm,
    out_hbm, all_a_hbm, all_b_hbm, bad_hbm,
    z_ref, gamma_ref, beta_ref, wb_ref, mask_ref, wq_ref, wk_ref, wv_ref, wg_ref, wo_ref, in_sems,
    own_a, own_b, all_a, all_b, out_ref, bias_acc, bias_s, w_s,
    kk0, kk1, vt0, vt1, kk_e, vt_e, qm0, qm1, p0, p1, sum0, sum1, o0, o1, bad_s,
    send_b1, recv_b1, send_b2, recv_b2, send_d, recv_d, send_r, recv_r, send_f, recv_f, out_sems,
):
    chunk = live_keys if live_keys == EARLY_KEYS else live_keys // 2
    blocks = -(-live_keys // COLS)
    sources = -(-blocks // 2)
    lead = GROUPS if sources == 2 else LEAD
    is_early = live_keys <= EARLY_KEYS
    kk_s, vt_s, qm_s, p_s, sum_s, o_s = (kk0, kk1), (vt0, vt1), (qm0, qm1), (p0, p1), (sum0, sum1), (o0, o1)
    row = lax.axis_index("row")
    col = lax.axis_index("col")
    z, y = row // 4, row % 4
    x, core = col // 2, col % 2

    copies = load(
        [(gamma_hbm, gamma_ref), (beta_hbm, beta_ref), (wb_hbm, wb_ref)]
        + [(z_hbm.at[pl.ds(12 * n, 12)], z_ref.at[pl.ds(12 * n, 12)]) for n in range(4)]
        + [(mask_hbm, mask_ref), (wq_hbm, wq_ref), (wk_hbm, wk_ref), (wv_hbm, wv_ref), (wg_hbm, wg_ref),
           (wo_hbm, wo_ref)], in_sems)

    right = {"row": row, "col": ((x + 1) % 4) * 2 + core}
    left = {"row": row, "col": ((x + 3) % 4) * 2 + core}
    partner = {"row": row, "col": x * 2 + (1 - core)}
    swap = {"row": 4 * x + y, "col": 2 * z + y // 2}
    is_relay = core == y // 2
    swap_self = jnp.logical_and(z == x, is_relay)

    barrier = pltpu.get_barrier_semaphore()

    def hello(dev):
        pl.semaphore_signal(barrier, inc=1, device_id=dev, device_id_type=MESH)

    for step in range(1, 16):
        hello({"row": (row + step) % 16, "col": col})
    hello(right)
    hello(left)
    hello(partner)

    @pl.when(jnp.logical_not(swap_self))
    def _():
        hello(swap)

    for c in range(2):
        @pl.when(jnp.logical_and(is_relay, jnp.logical_not(jnp.logical_and(z == x, core == c))))
        def _():
            hello({"row": 4 * x + y, "col": 2 * z + c})

    for copy in copies[:3]:
        copy.wait()
    gamma = column(gamma_ref, CH)
    beta = column(beta_ref, CH)
    pick = (iota((192, HEADS), 0) // 48 == iota((192, HEADS), 1)).astype(F32).astype(BF16)
    per_head = dot(pick, wb_ref[...]).astype(BF16)
    wide = jnp.concatenate([per_head, per_head], axis=1)
    keep = iota((192, LANES), 0) % 2 == iota((192, LANES), 1) // CH
    wide = jnp.where(keep, wide.astype(F32), 0.0).astype(BF16)
    lane_pair = (iota((COLS, 192), 1) % 48) // 2

    def norm_pair(p, carry):
        halves = []
        for half in range(2):
            v = z_ref[2 * p + half].astype(F32)
            mean = jnp.sum(v, axis=0, keepdims=True) * (1.0 / CH)
            centered = v - mean
            var = jnp.sum(centered * centered, axis=0, keepdims=True) * (1.0 / CH)
            halves.append(centered * lax.rsqrt(var + LN_EPS) * gamma + beta)
        a = jnp.transpose(jnp.concatenate(halves, axis=0)).astype(BF16)
        own_a[p] = a
        bias_acc[...] = jnp.where(lane_pair == p, dot(a, wide, 1, 1), bias_acc[...])
        return carry

    for n in range(4):
        copies[3 + n].wait()
        lax.fori_loop(6 * n, 6 * n + 6, norm_pair, 0, unroll=6)
    bias = bias_acc[...]
    own_b[0:96, :] = bias[:, 0:LANES].astype(BF16)
    own_b[96:144, :] = jnp.concatenate([bias[0:48, LANES:192], bias[48:96, LANES:192]], axis=1).astype(BF16)

    from_dest = jnp.where(swap_self, 0, 1)
    from_sources = jnp.where(is_relay, jnp.where(z == x, 1, 2), 0)
    pl.semaphore_wait(barrier, 18 + from_dest + from_sources)

    def bias1(c):
        return pltpu.make_async_remote_copy(
            src_ref=own_b, dst_ref=all_b.at[y % 2, 2 * x + c], send_sem=send_b1, recv_sem=recv_b1.at[c],
            device_id=swap, device_id_type=MESH,
        )

    for c in range(2):
        @pl.when((core == c) & (x < sources) & jnp.logical_not(swap_self))
        def _():
            bias1(c).start()

    def slot(g, c):
        return all_a.at[pl.ds(g * GP, GP), pl.ds(pl.multiple_of(c * COLS, COLS), COLS)]

    def own(g):
        return own_a.at[pl.ds(g * GP, GP)]

    def direct(src, g, c, way):
        return pltpu.make_async_remote_copy(
            src_ref=src, dst_ref=slot(g, c), send_sem=send_d.at[way, g], recv_sem=recv_d.at[way, g],
            device_id=left if way else right, device_id_type=MESH,
        )

    def relay(g, c, way):
        return pltpu.make_async_remote_copy(
            src_ref=slot(g, c), dst_ref=slot(g, c), send_sem=send_r.at[g], recv_sem=recv_r.at[g],
            device_id=left if way else right, device_id_type=MESH,
        )

    def forward(src, g, c, kind):
        return pltpu.make_async_remote_copy(
            src_ref=src, dst_ref=slot(g, c), send_sem=send_f.at[kind, g], recv_sem=recv_f.at[kind, g],
            device_id=partner, device_id_type=MESH,
        )

    cl, cr, co = ((x + 3) % 4) * 2 + core, ((x + 1) % 4) * 2 + core, ((x + 2) % 4) * 2 + core
    mine, has_left, has_right, has_opposite = col < blocks, cl < blocks, cr < blocks, co < blocks

    def to_right(g):
        return has_left & (x == 2 if sources == 2 else g % 2 == 0)

    def to_left(g):
        return has_right & (x == 3 if sources == 2 else g % 2 == 1)

    def send_direct(g):
        direct(own(g), g, col, 0).start()
        direct(own(g), g, col, 1).start()

    @pl.when(mine)
    def _():
        for g in range(lead):
            send_direct(g)
        for g in range(GROUPS):
            forward(own(g), g, col, 0).start()

    @pl.when(swap_self & (x < sources))
    def _():
        all_b[y % 2, col] = own_b[...]

    all_a[:, pl.ds(pl.multiple_of(col * COLS, COLS), COLS), :] = own_a[...]
    for copy in copies[7:]:
        copy.wait()
    fill_weights(w_s, wq_ref, wk_ref, wv_ref, wg_ref, wo_ref)
    for qm in qm_s:
        qm[...] = jnp.zeros_like(qm)

    bad_s[...] = jnp.where(iota(bad_s.shape, 0) == 1, float(live_keys), 0.0)

    def bias2(step, src_row):
        sz, sy = src_row // 4, src_row % 4
        ref = all_b.at[sy % 2, pl.ds(2 * sz, 2)]
        return pltpu.make_async_remote_copy(
            src_ref=ref, dst_ref=ref, send_sem=send_b2.at[step], recv_sem=recv_b2.at[sy % 2, sz],
            device_id={"row": (row + step) % 16, "col": col}, device_id_type=MESH,
        )

    def bias_relay():
        @pl.when(is_relay & (z < sources))
        def _():
            for c in range(2):
                @pl.when(jnp.logical_not(jnp.logical_and(z == x, core == c)))
                def _():
                    pltpu.make_async_remote_copy(
                        src_ref=own_b, dst_ref=all_b.at[y % 2, 2 * z + c], send_sem=send_b1,
                        recv_sem=recv_b1.at[c], device_id=swap, device_id_type=MESH,
                    ).wait_recv()
            for step in range(1, 16):
                bias2(step, row).start()

    def event(g):
        @pl.when(has_left)
        def _():
            direct(slot(g, cl), g, cl, 0).wait_recv()

            @pl.when(to_right(g))
            def _():
                relay(g, cl, 0).start()

            forward(slot(g, cl), g, cl, 1).start()

        @pl.when(has_right)
        def _():
            direct(slot(g, cr), g, cr, 1).wait_recv()

            @pl.when(to_left(g))
            def _():
                relay(g, cr, 1).start()

            forward(slot(g, cr), g, cr, 2).start()

        @pl.when(mine & (g < GROUPS - lead))
        def _():
            send_direct(g + lead)

    def relayed(g):
        @pl.when(has_opposite)
        def _():
            relay(g, co, 0).wait_recv()
            forward(slot(g, co), g, co, 3).start()

    def complete(g):
        for kind, dc in ((0, 0), (1, 3), (2, 1), (3, 2)):
            c = ((x + dc) % 4) * 2 + 1 - core

            @pl.when(c < blocks)
            def _():
                forward(slot(g, c), g, c, kind).wait_recv()

    def project(p, s):
        kk_s[s][...] = dot(all_a[p, 0:live_keys, :], w_s[3]).astype(BF16)
        fill_queries(qm_s[s], own_a[p], w_s[0])

    def key_of(p):
        return dot(all_a[p, 0:live_keys, :], w_s[3]).astype(BF16)

    def value_of(p):
        return dot(w_s[4], all_a[p, 0:live_keys, :], 1, 1).astype(BF16)

    def ahead(g):
        complete(g)
        for n in range(GP):
            kk_e[GP * g + n] = key_of(GP * g + n)
            vt_e[GP * g + n] = value_of(GP * g + n)

    def early(g, carry):
        event(g)

        @pl.when(g == 1)
        def _():
            bias_relay()

        @pl.when(g >= 2)
        def _():
            relayed(g - 2)

        if is_early:
            @pl.when(g >= 4)
            def _():
                ahead(g - 4)

        return carry

    lax.fori_loop(0, 7, early, 0)

    if is_early:
        ahead(3)
        complete(4)
        kk0[...] = key_of(EARLY)
        vt1[...] = vt_e[EARLY - 1]
        fill_queries(qm0, own_a[0], w_s[0])
    else:
        complete(0)
        project(0, 0)

    for sz in range(sources):
        for sy in range(2):
            @pl.when(jnp.logical_not(row == sz * 4 + 2 * core + sy))
            def _():
                ref = all_b.at[sy, pl.ds(2 * sz, 2)]
                pltpu.make_async_remote_copy(
                    src_ref=ref, dst_ref=ref, send_sem=send_b2.at[1], recv_sem=recv_b2.at[sy, sz],
                    device_id=partner, device_id_type=MESH,
                ).wait_recv()
        fill_bias(bias_s, all_b, mask_ref, (2 * sz, 2 * sz + 1))
    b_out = pltpu.make_async_copy(all_b, all_b_hbm, out_sems.at[0])
    b_out.start()

    def logits(kk, s, t):
        lanes = slice(t * TILE, t * TILE + TILE)
        qm = qm_s[s][:, lanes]
        total = jnp.zeros((8, TILE), F32)
        for k0 in range(0, live_keys, chunk):
            keys = slice(k0, k0 + chunk)
            e = jnp.exp(dot(kk[keys, :], qm) + bias_of(bias_s, t, k0, chunk))
            total = total + jnp.sum(e.reshape(chunk // 8, 8, TILE), axis=0)
            p_s[s][keys, lanes] = e.astype(BF16)
        sum_s[s][:, lanes] = total

    def combine(vt, s, t, live):
        lanes = slice(t * TILE, t * TILE + TILE)
        r0, r1 = TILE_ROWS[t]
        o = dot(vt[r0:r1, :], p_s[s][:, lanes])
        total = jnp.sum(sum_s[s][:, lanes], axis=0, keepdims=True)
        o_max = jnp.max(jnp.abs(o), axis=0, keepdims=True)
        good = (total > 1e-12) & (total < 1e25) & (o_max < 1e35)
        bad_s[0:1, lanes] = jnp.maximum(bad_s[0:1, lanes], jnp.where(good, 0.0, live))
        return o * (1.0 / total)


    a_out = pltpu.make_async_copy(all_a, all_a_hbm, out_sems.at[2])

    def polls(m):
        @pl.when((m >= 1) & (m <= 5))
        def _():
            event(m + 6)

        @pl.when((m >= 2) & (m <= 8))
        def _():
            relayed(m + 3)

        @pl.when((m >= (4 if is_early else 0)) & (m <= 10))
        def _():
            complete(m + 1)

        @pl.when(m == 11)
        def _():
            a_out.start()

    def step(m, s, ahead_of_time):
        i = 2 * m + s
        live = jnp.where(i >= 1, 1.0, 0.0)
        done = jnp.maximum(i - 2, 0)
        kk = kk_e.at[i] if ahead_of_time else kk_s[s]
        vt = vt_e.at[jnp.maximum(i - 1, 0)] if ahead_of_time else vt_s[1 - s]
        logits(kk, s, 0)
        o_0 = combine(vt, 1 - s, 0, live)
        if not ahead_of_time:
            vt_s[s][...] = value_of(i)
        logits(kk, s, 1)
        o_1 = combine(vt, 1 - s, 1, live)
        following = jnp.minimum(i + 1, PAIRS - 1)
        if ahead_of_time:
            fill_queries(qm_s[1 - s], own_a[following], w_s[0])
        else:
            project(following, 1 - s)
        logits(kk, s, 2)
        o_2 = combine(vt, 1 - s, 2, live)
        o_s[1 - s][...] = assemble([o_0, o_1, o_2])
        write_rows(done, own_a[done], o_s[s][...], w_s, z_ref, out_ref)

    def body(ahead_of_time, m, carry):
        polls(m)
        for s in range(2):
            step(m, s, ahead_of_time)
        return carry

    if is_early:
        lax.fori_loop(0, EARLY // 2, functools.partial(body, True), 0)
    lax.fori_loop(EARLY // 2 if is_early else 0, PAIRS // 2, functools.partial(body, False), 0)
    tail = 2 * PAIRS - 4
    head_out = pltpu.make_async_copy(out_ref.at[0:tail], out_hbm.at[0:tail], out_sems.at[4])
    head_out.start()
    write_rows(PAIRS - 2, own_a[PAIRS - 2], o_s[0][...], w_s, z_ref, out_ref)
    o_s[1][...] = assemble([combine(vt1, 1, t, 1.0) for t in range(3)])
    write_rows(PAIRS - 1, own_a[PAIRS - 1], o_s[1][...], w_s, z_ref, out_ref)
    outs = [
        pltpu.make_async_copy(out_ref.at[tail:2 * PAIRS], out_hbm.at[tail:2 * PAIRS], out_sems.at[1]),
        pltpu.make_async_copy(bad_s, bad_hbm, out_sems.at[3]),
    ]
    for copy in outs:
        copy.start()

    for c in range(2):
        @pl.when((core == c) & (x < sources) & jnp.logical_not(swap_self))
        def _():
            bias1(c).wait_send()

    @pl.when(is_relay & (z < sources))
    def _():
        for step in range(1, 16):
            bias2(step, row).wait_send()

    def sent(g, carry):
        @pl.when(mine)
        def _():
            direct(own(g), g, col, 0).wait_send()
            direct(own(g), g, col, 1).wait_send()

        @pl.when(to_right(g))
        def _():
            relay(g, cl, 0).wait_send()

        @pl.when(to_left(g))
        def _():
            relay(g, cr, 1).wait_send()

        for kind, there in enumerate((mine, has_left, has_right, has_opposite)):
            @pl.when(there)
            def _():
                forward(own(g), g, col, kind).wait_send()

        return carry

    lax.fori_loop(0, GROUPS, sent, 0)
    for copy in outs:
        copy.wait()
    a_out.wait()
    b_out.wait()
    head_out.wait()


def fused_call(variant, z_t, gamma, beta, wb_t, mask, wq, wk, wv, wg, wo):
    dma = pltpu.SemaphoreType.DMA
    live_keys = LIVE[variant]
    args = (z_t, gamma, beta, wb_t, mask, wq, wk, wv, wg, wo)
    two = lambda *spec: [pltpu.VMEM(*spec)] * 2
    return pl.pallas_call(
        functools.partial(fused_kernel, live_keys),
        out_shape=(
            jax.ShapeDtypeStruct(z_t.shape, BF16),
            jax.ShapeDtypeStruct((PAIRS, KEYS, LANES), BF16),
            jax.ShapeDtypeStruct((2, 8, 144, LANES), BF16),
            jax.ShapeDtypeStruct((8, KEYS), F32),
        ),
        in_specs=[pl.BlockSpec(memory_space=pl.ANY)] * len(args),
        out_specs=(pl.BlockSpec(memory_space=pl.ANY),) * 4,
        scratch_shapes=[
            *[pltpu.VMEM(s.shape, s.dtype) for s in args],
            dma((13,)),
            pltpu.VMEM((PAIRS, COLS, LANES), BF16),
            pltpu.VMEM((144, LANES), BF16),
            pltpu.VMEM((PAIRS, KEYS, LANES), BF16),
            pltpu.VMEM((2, 8, 144, LANES), BF16),
            pltpu.VMEM(z_t.shape, BF16),
            pltpu.VMEM((COLS, 192), F32),
            pltpu.VMEM((KEYS, 384), F32),
            pltpu.VMEM((5, LANES, LANES), BF16),
            *two((live_keys, LANES), BF16),
            *two((LANES, live_keys), BF16),
            pltpu.VMEM((EARLY, min(live_keys, EARLY_KEYS), LANES), BF16),
            pltpu.VMEM((EARLY, LANES, min(live_keys, EARLY_KEYS)), BF16),
            *two((LANES, KEYS), BF16),
            *two((live_keys, KEYS), BF16),
            *two((8, KEYS), F32),
            *two((LANES, COLS), F32),
            pltpu.VMEM((8, KEYS), F32),
            dma(()), dma((2,)), dma((16,)), dma((2, 4)),
            dma((2, GROUPS)), dma((2, GROUPS)), dma((GROUPS,)), dma((GROUPS,)), dma((4, GROUPS)), dma((4, GROUPS)),
            dma((5,)),
        ],
        compiler_params=pltpu.CompilerParams(collective_id=variant, has_side_effects=True),
        cost_estimate=pl.CostEstimate(flops=10**11, bytes_accessed=10**9, transcendentals=14 * 10**6),
        name=f"fused{live_keys}",
    )(*args)


def shifted_kernel(
    bad_ref, y_in, all_a_hbm, all_b_hbm, z_hbm, mask_hbm, wq_hbm, wk_hbm, wv_hbm, wg_hbm, wo_hbm,
    y_out,
    all_a, all_b, z_ref, mask_ref, wq_ref, wk_ref, wv_ref, wg_ref, wo_ref, sems,
    bias_s, w_s, kk, vt, qm, p_s, l_s, out_ref,
):
    @pl.when(jnp.max(bad_ref[0:1, :]) > 0.0)
    def _():
        col = lax.axis_index("col")
        for copy in load([
            (all_a_hbm, all_a), (all_b_hbm, all_b), (z_hbm, z_ref), (mask_hbm, mask_ref), (wq_hbm, wq_ref),
            (wk_hbm, wk_ref), (wv_hbm, wv_ref), (wg_hbm, wg_ref), (wo_hbm, wo_ref)], sems):
            copy.wait()
        fill_weights(w_s, wq_ref, wk_ref, wv_ref, wg_ref, wo_ref)
        fill_bias(bias_s, all_b, mask_ref)
        live_keys = bad_ref[1:2, 0:LANES]
        there = iota((KEYS, LANES), 0).astype(F32) < live_keys
        for lanes in range(0, 384, LANES):
            bias_s[:, lanes:lanes + LANES] = jnp.where(there, bias_s[:, lanes:lanes + LANES], NEG)
        qm[...] = jnp.zeros_like(qm)

        def body(p, carry):
            own = all_a[p, pl.ds(pl.multiple_of(col * COLS, COLS), COLS), :]
            keys_a = jnp.where(there, all_a[p].astype(F32), 0.0).astype(BF16)
            kk[...] = dot(keys_a, w_s[3]).astype(BF16)
            vt[...] = dot(w_s[4], keys_a, 1, 1).astype(BF16)
            fill_queries(qm, own, w_s[0])
            outs = []
            for t in range(3):
                lanes = slice(t * TILE, t * TILE + TILE)
                peak = jnp.full((1, TILE), -jnp.inf, F32)
                for k0 in range(0, KEYS, LANES):
                    keys = slice(k0, k0 + LANES)
                    s = dot(kk[keys, :], qm[:, lanes]) + bias_of(bias_s, t, k0, LANES)
                    l_s[keys, :] = s
                    peak = jnp.maximum(peak, jnp.max(s, axis=0, keepdims=True))
                total = jnp.zeros((1, TILE), F32)
                for k0 in range(0, KEYS, LANES):
                    keys = slice(k0, k0 + LANES)
                    e = jnp.exp(l_s[keys, :] - peak)
                    total = total + jnp.sum(e, axis=0, keepdims=True)
                    p_s[keys, :] = e.astype(BF16)
                r0, r1 = TILE_ROWS[t]
                outs.append(dot(vt[r0:r1, :], p_s[...]) * (1.0 / total))
            write_rows(p, own, assemble(outs), w_s, z_ref, out_ref)
            return carry

        lax.fori_loop(0, PAIRS, body, 0)
        copy = pltpu.make_async_copy(out_ref, y_out, sems.at[0])
        copy.start()
        copy.wait()


def shifted_call(bad, y, all_a, all_b, z_t, mask, wq, wk, wv, wg, wo):
    args = (all_a, all_b, z_t, mask, wq, wk, wv, wg, wo)
    return pl.pallas_call(
        shifted_kernel,
        out_shape=jax.ShapeDtypeStruct(z_t.shape, BF16),
        in_specs=[pl.BlockSpec(memory_space=pltpu.VMEM)] + [pl.BlockSpec(memory_space=pl.ANY)] * (len(args) + 1),
        out_specs=pl.BlockSpec(memory_space=pl.ANY),
        input_output_aliases={1: 0},
        scratch_shapes=[
            *[pltpu.VMEM(s.shape, s.dtype) for s in args],
            pltpu.SemaphoreType.DMA((len(args),)),
            pltpu.VMEM((KEYS, 384), F32),
            pltpu.VMEM((5, LANES, LANES), BF16),
            pltpu.VMEM((KEYS, LANES), BF16),
            pltpu.VMEM((LANES, KEYS), BF16),
            pltpu.VMEM((LANES, KEYS), BF16),
            pltpu.VMEM((KEYS, TILE), BF16),
            pltpu.VMEM((KEYS, TILE), F32),
            pltpu.VMEM(z_t.shape, BF16),
        ],
        name="shifted",
    )(bad, y, *args)


def solution(mesh):
    tile_spec = P(("dp", "row"), "col", None)

    def per_device(pair_tile, res_mask, ln_gamma, ln_beta, w_q, w_k, w_v, w_b, w_g, w_o):
        z_t = jnp.transpose(pair_tile, (0, 2, 1))
        mask = res_mask.reshape(6, LANES)
        gamma, beta, wb_t = ln_gamma.reshape(1, CH), ln_beta.reshape(1, CH), jnp.transpose(w_b)
        build = pick_call(mask, gamma, beta, w_q, w_k, wb_t)
        y, all_a, all_b, bad = lax.switch(
            build[0], [functools.partial(fused_call, n) for n in range(len(LIVE))],
            z_t, gamma, beta, wb_t, mask, w_q, w_k, w_v, w_g, w_o
        )
        y = shifted_call(bad, y, all_a, all_b, z_t, mask, w_q, w_k, w_v, w_g, w_o)
        return jnp.transpose(y, (0, 2, 1))

    return jax.shard_map(
        per_device, mesh=mesh,
        in_specs=(tile_spec, P("dp"), P(), P(), P(), P(), P(), P(), P(), P()),
        out_specs=tile_spec, check_vma=False,
    )
```
